8 devices in a mesh: data: 2 (over z, y), stage: 4 (over x, core).
Axes of the slice: x: 2, y: 2, z: 1, core: 2. Of those that a mesh axis runs over, the one named last changes fastest.
Arguments:
- master_up: float32 [4, 768, 3072], P('stage')
- master_down: float32 [4, 3072, 768], P('stage')
- mom1_up: float32 [4, 768, 3072], P('stage')
- mom1_down: float32 [4, 3072, 768], P('stage')
- mom2_up: float32 [4, 768, 3072], P('stage')
- mom2_down: float32 [4, 3072, 768], P('stage')
- grad_up: float32 [2, 4, 768, 3072], P('data', 'stage')
- grad_down: float32 [2, 4, 3072, 768], P('data', 'stage')
- stage_acts: bfloat16 [4, 8192, 768], P('stage', 'data')
- loss_grad: bfloat16 [8192, 768], P('data')
- next_batch: bfloat16 [2, 8192, 768], P(None, 'data')
- learn_rate: float32 [], replicated
- max_norm: float32 [], replicated
Outputs:
- output 1: float32 [4, 768, 3072], P('stage')
- output 2: float32 [4, 3072, 768], P('stage')
- output 3: float32 [4, 768, 3072], P('stage')
- output 4: float32 [4, 3072, 768], P('stage')
- output 5: float32 [4, 768, 3072], P('stage')
- output 6: float32 [4, 3072, 768], P('stage')
- output 7: bfloat16 [4, 2, 8192, 768], P('stage', None, 'data')
All inputs are finite; a program needn't handle non-finite values.
Results may differ from the reference program's by a relative error of at most 0.00896169.
Values are sent between devices in bfloat16 or wider.
A program may use at most 1 GiB of HBM per device.

```python
import jax
import jax.numpy as jnp
from jax import lax

STAGES = 4
REPLICAS = 2
D = 768
FF = 3072
TOKENS = 4096
MICROBATCHES = 2
ADAM_STEP = 8

ROWS = REPLICAS * TOKENS
BETA1 = 0.9
BETA2 = 0.95
ADAM_EPS = 1e-8
WEIGHT_DECAY = 0.1
NORM_EPS = 1e-6
SQRT_TWO_PI = 0.7978845608028654
GELU_CUBIC = 0.044715


def tanh_part(pre_act):
    return jnp.tanh(SQRT_TWO_PI * (pre_act + GELU_CUBIC * pre_act * pre_act * pre_act))


def gelu_tanh(pre_act):
    return 0.5 * pre_act * (1.0 + tanh_part(pre_act))


def gelu_pair(pre_act):
    tanh_val = tanh_part(pre_act)
    act_value = 0.5 * pre_act * (1.0 + tanh_val)
    act_slope = 0.5 * (1.0 + tanh_val) + 0.5 * pre_act * (1.0 - tanh_val * tanh_val) * SQRT_TWO_PI * (1.0 + 3.0 * GELU_CUBIC * pre_act * pre_act)
    return act_value, act_slope


def stage_backward(stage_in, master_up, master_down, loss_grad):
    up_bf = master_up.astype(jnp.bfloat16)
    down_bf = master_down.astype(jnp.bfloat16)

    def back_body(grad_in, stage_xs):
        rows_in, up_p, down_p = stage_xs
        pre_act = jnp.dot(rows_in, up_p, preferred_element_type=jnp.float32)
        act_value, act_slope = gelu_pair(pre_act)
        hidden = act_value.astype(jnp.bfloat16)
        d_hidden = jnp.dot(grad_in, down_p.T, preferred_element_type=jnp.float32)
        d_pre = (d_hidden * act_slope).astype(jnp.bfloat16)
        d_rows = (grad_in.astype(jnp.float32) + jnp.dot(d_pre, up_p.T, preferred_element_type=jnp.float32)).astype(jnp.bfloat16)
        dw_up = jnp.dot(rows_in.T, d_pre, preferred_element_type=jnp.float32)
        dw_down = jnp.dot(hidden.T, grad_in, preferred_element_type=jnp.float32)
        return d_rows, (dw_up, dw_down)

    _, (dw_up, dw_down) = lax.scan(back_body, loss_grad, (stage_in, up_bf, down_bf), reverse=True)
    return dw_up, dw_down


def mean_grads(grad_up, grad_down, stage_in, master_up, master_down, loss_grad):
    dw_up, dw_down = stage_backward(stage_in, master_up, master_down, loss_grad)
    gbar_up = (jnp.sum(grad_up, axis=0) + dw_up) / REPLICAS
    gbar_down = (jnp.sum(grad_down, axis=0) + dw_down) / REPLICAS
    return gbar_up, gbar_down


def adamw_update(master, first_mom, second_mom, grad_avg, clip_scale, learn_rate):
    scaled = clip_scale * grad_avg
    new_first = BETA1 * first_mom + (1.0 - BETA1) * scaled
    new_second = BETA2 * second_mom + (1.0 - BETA2) * scaled * scaled
    first_hat = new_first / (1.0 - BETA1 ** ADAM_STEP)
    second_hat = new_second / (1.0 - BETA2 ** ADAM_STEP)
    new_master = master - learn_rate * (first_hat / (jnp.sqrt(second_hat) + ADAM_EPS) + WEIGHT_DECAY * master)
    return new_master, new_first, new_second


def setup_inputs(seed: int = 0) -> dict:
    base_key = jax.random.key(seed)
    key_list = jax.random.split(base_key, 16)
    std_up = D ** -0.5
    std_down = 1.5 * (FF * STAGES) ** -0.5
    master_up = jax.random.normal(key_list[0], (STAGES, D, FF), jnp.float32) * std_up
    master_down = jax.random.normal(key_list[1], (STAGES, FF, D), jnp.float32) * std_down
    stage_acts = jax.random.normal(key_list[2], (STAGES, ROWS, D), jnp.float32).astype(jnp.bfloat16)
    loss_grad = jax.random.normal(key_list[3], (ROWS, D), jnp.float32).astype(jnp.bfloat16)
    next_batch = jax.random.normal(key_list[4], (MICROBATCHES, ROWS, D), jnp.float32).astype(jnp.bfloat16)
    grad_up = jax.random.normal(key_list[5], (REPLICAS, STAGES, D, FF), jnp.float32) * (0.4 * (TOKENS / STAGES) ** 0.5)
    grad_down = jax.random.normal(key_list[6], (REPLICAS, STAGES, FF, D), jnp.float32) * (0.6 * TOKENS ** 0.5)
    gbar_up, gbar_down = mean_grads(grad_up, grad_down, stage_acts, master_up, master_down, loss_grad)
    grad_norm = jnp.sqrt(jnp.sum(gbar_up * gbar_up) + jnp.sum(gbar_down * gbar_down))
    norm_frac = jax.random.uniform(key_list[7], (), jnp.float32, 0.35, 0.65)
    max_norm = norm_frac * grad_norm
    rms_up = norm_frac * jnp.sqrt(jnp.mean(gbar_up * gbar_up))
    rms_down = norm_frac * jnp.sqrt(jnp.mean(gbar_down * gbar_down))
    mom1_up = jax.random.normal(key_list[8], (STAGES, D, FF), jnp.float32) * (0.1 * rms_up)
    mom1_down = jax.random.normal(key_list[9], (STAGES, FF, D), jnp.float32) * (0.1 * rms_down)
    mom2_up = jax.random.uniform(key_list[10], (STAGES, D, FF), jnp.float32, 0.05, 0.15) * (rms_up * rms_up)
    mom2_down = jax.random.uniform(key_list[11], (STAGES, FF, D), jnp.float32, 0.05, 0.15) * (rms_down * rms_down)
    learn_rate = jax.random.uniform(key_list[12], (), jnp.float32, 0.1, 0.3) * std_down
    return dict(master_up=master_up, master_down=master_down, mom1_up=mom1_up, mom1_down=mom1_down, mom2_up=mom2_up, mom2_down=mom2_down, grad_up=grad_up, grad_down=grad_down, stage_acts=stage_acts, loss_grad=loss_grad, next_batch=next_batch, learn_rate=learn_rate, max_norm=max_norm)


def reference(master_up, master_down, mom1_up, mom1_down, mom2_up, mom2_down, grad_up, grad_down, stage_acts, loss_grad, next_batch, learn_rate, max_norm):
    gbar_up, gbar_down = mean_grads(grad_up, grad_down, stage_acts, master_up, master_down, loss_grad)
    grad_norm = jnp.sqrt(jnp.sum(gbar_up * gbar_up) + jnp.sum(gbar_down * gbar_down))
    clip_scale = jnp.minimum(1.0, max_norm / (grad_norm + NORM_EPS))
    new_up, new_mom1_up, new_mom2_up = adamw_update(master_up, mom1_up, mom2_up, gbar_up, clip_scale, learn_rate)
    new_down, new_mom1_down, new_mom2_down = adamw_update(master_down, mom1_down, mom2_down, gbar_down, clip_scale, learn_rate)
    up_bf = new_up.astype(jnp.bfloat16)
    down_bf = new_down.astype(jnp.bfloat16)

    def fwd_body(rows_in, weights):
        up_p, down_p = weights
        pre_act = jnp.dot(rows_in, up_p, preferred_element_type=jnp.float32)
        hidden = gelu_tanh(pre_act).astype(jnp.bfloat16)
        rows_out = (rows_in.astype(jnp.float32) + jnp.dot(hidden, down_p, preferred_element_type=jnp.float32)).astype(jnp.bfloat16)
        return rows_out, rows_out

    flat_batch = next_batch.reshape(MICROBATCHES * ROWS, D)
    _, stage_outs = lax.scan(fwd_body, flat_batch, (up_bf, down_bf))
    stage_outputs = stage_outs.reshape(STAGES, MICROBATCHES, ROWS, D)
    return (new_up, new_down, new_mom1_up, new_mom1_down, new_mom2_up, new_mom2_down, stage_outputs)
```

```python
import functools

import jax
import jax.numpy as jnp
from jax import lax
from jax.experimental import pallas as pl
from jax.experimental.pallas import tpu as pltpu
from jax.sharding import PartitionSpec as P

BETA1 = 0.9
BETA2 = 0.95
ADAM_EPS = 1e-8
WEIGHT_DECAY = 0.1
NORM_EPS = 1e-6
ADAM_STEP = 8
SQRT_TWO_PI = 0.7978845608028654
GELU_CUBIC = 0.044715

BACK_ROWS = 512
FWD_ROWS = 512
BACK_TILE = 512
FWD_TILE = 512
PIECES = 3
F32_FIRST = 1
STAGING = 4

BF16 = jnp.bfloat16
F32 = jnp.float32
MESH_ID = pl.DeviceIdType.MESH
ANY = pl.BlockSpec(memory_space=pl.ANY)
VMEM_LIMIT = 60 * 1024 * 1024


def dot_nn(left, right):
    return lax.dot_general(left, right, (((1,), (0,)), ((), ())), preferred_element_type=F32)


def dot_nt(left, right):
    return lax.dot_general(left, right, (((1,), (1,)), ((), ())), preferred_element_type=F32)


def dot_tn(left, right):
    return lax.dot_general(left, right, (((0,), (0,)), ((), ())), preferred_element_type=F32)


def span(index, size):
    return pl.ds(pl.multiple_of(index * size, size), size)


def tanh_part(x, sq):
    return jnp.tanh(x * (SQRT_TWO_PI + (SQRT_TWO_PI * GELU_CUBIC) * sq))


def gelu_value(x):
    return x * (0.5 + 0.5 * tanh_part(x, x * x))


def gelu_pair(x):
    sq = x * x
    th = tanh_part(x, sq)
    half = 0.5 + 0.5 * th
    value = x * half
    slope = half + value * (1.0 - th) * (SQRT_TWO_PI + (3.0 * SQRT_TWO_PI * GELU_CUBIC) * sq)
    return value, slope


def meet_neighbours(stage, n_stages):
    barrier = pltpu.get_barrier_semaphore()

    @pl.when(stage > 0)
    def _():
        pl.semaphore_signal(barrier, inc=1, device_id={"stage": stage - 1}, device_id_type=MESH_ID)

    @pl.when(stage < n_stages - 1)
    def _():
        pl.semaphore_signal(barrier, inc=1, device_id={"stage": stage + 1}, device_id_type=MESH_ID)

    pl.semaphore_wait(barrier, jnp.minimum(stage, 1) + jnp.minimum(n_stages - 1 - stage, 1))


def back_kernel(n_stages, acts_ref, dy_ref, up32_ref, down32_ref, hid_ref, dpre_ref, gown_ref,
                up_ref, down_ref, g_buf, h_buf, p_buf, dx_buf, acc_ref, stage_u, stage_v,
                u_sem, v_sem, recv_sem, send_sem, gown_sem, h_sem, p_sem):
    stage = lax.axis_index("stage")
    last = n_stages - 1
    rows_all, width = g_buf.shape
    hidden = up_ref.shape[1]
    n_chunks = rows_all // BACK_ROWS
    n_tiles = hidden // BACK_TILE
    u_rows = stage_u.shape[1]
    v_rows = stage_v.shape[1]
    n_cast = width // u_rows

    def u_copy(i, slot):
        return pltpu.make_async_copy(up32_ref.at[0, span(i, u_rows), :], stage_u.at[slot], u_sem.at[slot])

    def v_copy(i, slot):
        return pltpu.make_async_copy(down32_ref.at[0, span(i, v_rows), :], stage_v.at[slot], v_sem.at[slot])

    for i in range(STAGING):
        u_copy(i, i).start()
        v_copy(i, i).start()

    def rows_of(c):
        return span(c, BACK_ROWS)

    @pl.when(stage == last)
    def _():
        def load(c, carry):
            pltpu.make_async_copy(dy_ref.at[rows_of(c), :], g_buf.at[rows_of(c), :], recv_sem.at[c]).start()
            return carry
        lax.fori_loop(0, n_chunks, load, 0)

    meet_neighbours(stage, n_stages)

    def cast(i, carry):
        slot = lax.rem(i, STAGING)
        u_copy(i, slot).wait()
        up_ref[span(i, u_rows), :] = stage_u[slot].astype(BF16)
        v_copy(i, slot).wait()
        down_ref[span(i, v_rows), :] = stage_v[slot].astype(BF16)

        @pl.when(i + STAGING < n_cast)
        def _():
            u_copy(i + STAGING, slot).start()
            v_copy(i + STAGING, slot).start()
        return carry

    lax.fori_loop(0, n_cast, cast, 0)

    def send_of(c):
        return pltpu.make_async_remote_copy(
            src_ref=dx_buf.at[rows_of(c), :], dst_ref=g_buf.at[rows_of(c), :],
            send_sem=send_sem.at[c], recv_sem=recv_sem.at[c],
            device_id={"stage": stage - 1}, device_id_type=MESH_ID)

    def out_copies(c, slot):
        return (pltpu.make_async_copy(h_buf.at[slot], hid_ref.at[rows_of(c), :], h_sem.at[slot]),
                pltpu.make_async_copy(p_buf.at[slot], dpre_ref.at[rows_of(c), :], p_sem.at[slot]))

    def gown_copy(c):
        return pltpu.make_async_copy(g_buf.at[rows_of(c), :], gown_ref.at[rows_of(c), :], gown_sem.at[c])

    def chunk(c, carry):
        slot = lax.rem(c, 2)
        rows = rows_of(c)

        @pl.when(c >= 2)
        def _():
            for copy in out_copies(c - 2, slot):
                copy.wait()

        pltpu.make_async_copy(dy_ref.at[rows, :], g_buf.at[rows, :], recv_sem.at[c]).wait()
        gown_copy(c).start()

        def tile(j, inner):
            cols = span(j, BACK_TILE)
            pre = dot_nn(acts_ref[0, rows, :], up_ref[:, cols])
            d_hid = dot_nt(g_buf[rows, :], down_ref[cols, :])
            value, slope = gelu_pair(pre)
            h_buf[slot, :, cols] = value.astype(BF16)
            d_pre = (d_hid * slope).astype(BF16)
            p_buf[slot, :, cols] = d_pre

            @pl.when(stage > 0)
            def _():
                part = dot_nt(d_pre, up_ref[:, cols])
                acc_ref[...] = jnp.where(j == 0, part, acc_ref[...] + part)
            return inner

        lax.fori_loop(0, n_tiles, tile, 0)

        @pl.when(stage > 0)
        def _():
            dx_buf[rows, :] = (g_buf[rows, :].astype(F32) + acc_ref[...]).astype(BF16)
        for copy in out_copies(c, slot):
            copy.start()

        @pl.when(stage > 0)
        def _():
            send_of(c).start()
        return carry

    lax.fori_loop(0, n_chunks, chunk, 0)

    for c in (n_chunks - 2, n_chunks - 1):
        for copy in out_copies(c, c % 2):
            copy.wait()

    def finish(c, carry):
        gown_copy(c).wait()

        @pl.when(stage > 0)
        def _():
            send_of(c).wait_send()
        return carry

    lax.fori_loop(0, n_chunks, finish, 0)


def backward(n_stages, acts, loss_grad, up32, down32):
    _, rows, width = acts.shape
    hidden = up32.shape[2]
    n_chunks = rows // BACK_ROWS
    u_rows, v_rows = width // 12, hidden // 12
    wide = jax.ShapeDtypeStruct((rows, hidden), BF16)
    return pl.pallas_call(
        functools.partial(back_kernel, n_stages),
        name="backward",
        out_shape=(wide, wide, jax.ShapeDtypeStruct((rows, width), BF16)),
        in_specs=[pl.BlockSpec(memory_space=pltpu.VMEM), ANY, ANY, ANY],
        out_specs=(ANY, ANY, ANY),
        scratch_shapes=[
            pltpu.VMEM((width, hidden), BF16),
            pltpu.VMEM((hidden, width), BF16),
            pltpu.VMEM((rows, width), BF16),
            pltpu.VMEM((2, BACK_ROWS, hidden), BF16),
            pltpu.VMEM((2, BACK_ROWS, hidden), BF16),
            pltpu.VMEM((rows, width), BF16),
            pltpu.VMEM((BACK_ROWS, width), F32),
            pltpu.VMEM((STAGING, u_rows, hidden), F32),
            pltpu.VMEM((STAGING, v_rows, width), F32),
            pltpu.SemaphoreType.DMA((STAGING,)),
            pltpu.SemaphoreType.DMA((STAGING,)),
            pltpu.SemaphoreType.DMA((n_chunks,)),
            pltpu.SemaphoreType.DMA((n_chunks,)),
            pltpu.SemaphoreType.DMA((n_chunks,)),
            pltpu.SemaphoreType.DMA((2,)),
            pltpu.SemaphoreType.DMA((2,)),
        ],
        compiler_params=pltpu.CompilerParams(collective_id=0, has_side_effects=True, vmem_limit_bytes=VMEM_LIMIT),
        cost_estimate=pl.CostEstimate(flops=6 * rows * width * hidden, bytes_accessed=6 * rows * hidden, transcendentals=rows * hidden),
    )(acts, loss_grad, up32, down32)


def wgrad_kernel(own_ref, acts_ref, dpre_ref, gu_ref, hid_ref, gown_ref, gv_ref, su_ref, sv_ref):
    rows = acts_ref.shape[1]
    step = 1024

    def accumulate(left_ref, right_ref, init, left_index=None):
        acc = init
        for k in range(rows // step):
            part = pl.ds(k * step, step)
            left = left_ref[part, :] if left_index is None else left_ref[left_index, part, :]
            acc = acc + dot_tn(left, right_ref[part, :])
        return acc

    su_ref[...] = accumulate(acts_ref, dpre_ref, gu_ref[0, 0], 0)
    sv_ref[...] = accumulate(hid_ref, gown_ref, gv_ref[0, 0])


def wgrad_piece(k, owner, acts, d_pre, grad_up, hid, g_own, grad_down, name):
    _, rows, width = acts.shape
    hidden = hid.shape[1]
    half_w, piece_n = width // 2, hidden // PIECES
    half_h, piece_m = hidden // 2, hidden // 2 // PIECES
    steps = 2
    un, vm = piece_n // steps, piece_m // steps
    return pl.pallas_call(
        wgrad_kernel,
        name=name,
        out_shape=(jax.ShapeDtypeStruct((half_w, piece_n), F32), jax.ShapeDtypeStruct((piece_m, width), F32)),
        grid_spec=pltpu.PrefetchScalarGridSpec(
            num_scalar_prefetch=1,
            grid=(steps,),
            in_specs=[
                pl.BlockSpec((1, rows, half_w), lambda i, own: (0, 0, own[0])),
                pl.BlockSpec((rows, un), lambda i, own: (0, k * steps + i)),
                pl.BlockSpec((1, 1, half_w, un), lambda i, own: (0, 0, own[0], k * steps + i)),
                pl.BlockSpec((rows, vm), lambda i, own: (0, (own[0] * PIECES + k) * steps + i)),
                pl.BlockSpec((rows, width), lambda i, own: (0, 0)),
                pl.BlockSpec((1, 1, vm, width), lambda i, own: (0, 0, (own[0] * PIECES + k) * steps + i, 0)),
            ],
            out_specs=(
                pl.BlockSpec((half_w, un), lambda i, own: (0, i)),
                pl.BlockSpec((vm, width), lambda i, own: (i, 0)),
            ),
        ),
        compiler_params=pltpu.CompilerParams(vmem_limit_bytes=VMEM_LIMIT),
        cost_estimate=pl.CostEstimate(flops=4 * rows * half_w * piece_n, bytes_accessed=30 * 1024 * 1024, transcendentals=0),
    )(owner, acts, d_pre, grad_up, hid, g_own, grad_down)


def update_kernel(n_alias, own_ref, knobs_ref, wu, mu, vu, gu, wd, md, vd, gd, *rest):
    wu_o, mu_o, vu_o, wd_o, md_o, vd_o, bu_o, bd_o = rest[n_alias:]
    clip, lr = knobs_ref[0], knobs_ref[1]

    def adamw(w, m, v, g):
        q = clip * g
        m_new = BETA1 * m + (1.0 - BETA1) * q
        v_new = BETA2 * v + (1.0 - BETA2) * q * q
        m_hat = m_new * (1.0 / (1.0 - BETA1 ** ADAM_STEP))
        v_hat = v_new * (1.0 / (1.0 - BETA2 ** ADAM_STEP))
        w_new = w - lr * (m_hat / (jnp.sqrt(v_hat) + ADAM_EPS) + WEIGHT_DECAY * w)
        return w_new, m_new, v_new

    w, m, v = adamw(wu[0], mu[0], vu[0], gu[...])
    wu_o[0], mu_o[0], vu_o[0] = w, m, v
    bu_o[...] = w.astype(BF16)
    w, m, v = adamw(wd[0], md[0], vd[0], gd[...])
    wd_o[0], md_o[0], vd_o[0] = w, m, v
    bd_o[...] = w.astype(BF16)


def update_piece(k, owner, knobs, up_set, down_set, gbar_u, gbar_v, chain, name):
    _, width, hidden = up_set[0].shape
    half_w, piece_n = gbar_u.shape
    piece_m = gbar_v.shape[0]
    steps = 4
    um, vm = half_w // steps, piece_m // steps
    up_spec = pl.BlockSpec((1, um, piece_n), lambda i, own: (0, own[0] * steps + i, k))
    down_spec = pl.BlockSpec((1, vm, width), lambda i, own: (0, (own[0] * PIECES + k) * steps + i, 0))
    gu_spec = pl.BlockSpec((um, piece_n), lambda i, own: (i, 0))
    gd_spec = pl.BlockSpec((vm, width), lambda i, own: (i, 0))
    full_u = jax.ShapeDtypeStruct((1, width, hidden), F32)
    full_d = jax.ShapeDtypeStruct((1, hidden, width), F32)
    elements = half_w * piece_n + piece_m * width
    return pl.pallas_call(
        functools.partial(update_kernel, len(chain)),
        name=name,
        out_shape=(full_u,) * 3 + (full_d,) * 3 + (jax.ShapeDtypeStruct((half_w, piece_n), BF16), jax.ShapeDtypeStruct((piece_m, width), BF16)),
        grid_spec=pltpu.PrefetchScalarGridSpec(
            num_scalar_prefetch=1,
            grid=(steps,),
            in_specs=[pl.BlockSpec(memory_space=pltpu.SMEM)] + [up_spec] * 3 + [gu_spec] + [down_spec] * 3 + [gd_spec] + [ANY] * len(chain),
            out_specs=(up_spec,) * 3 + (down_spec,) * 3 + (gu_spec, gd_spec),
        ),
        input_output_aliases={10 + i: i for i in range(len(chain))},
        compiler_params=pltpu.CompilerParams(vmem_limit_bytes=VMEM_LIMIT),
        cost_estimate=pl.CostEstimate(flops=30 * elements, bytes_accessed=30 * elements, transcendentals=elements),
    )(owner, knobs, *up_set, gbar_u, *down_set, gbar_v, *chain)


def fwd_kernel(n_stages, n_rep, batch_ref, *refs):
    n_w = 2 * PIECES * n_rep
    w_refs = refs[:n_w]
    out_ref, up_ref, down_ref, x_buf, y_buf, acc_ref, w_sem, recv_sem, send_sem, out_sem = refs[n_w:]
    stage = lax.axis_index("stage")
    me = lax.axis_index("data")
    last = n_stages - 1
    n_chunks = x_buf.shape[0]
    hidden = up_ref.shape[1]
    n_tiles = hidden // FWD_TILE
    chunks_per_micro = n_chunks // batch_ref.shape[0]

    def batch_chunk(ref, c, lead):
        return ref.at[lead + (c // chunks_per_micro, span(lax.rem(c, chunks_per_micro), FWD_ROWS), slice(None))]

    copies = []
    for side in range(n_rep):
        owner = me if side == 0 else 1 - me
        for k in range(PIECES):
            u_src = w_refs[(2 * side) * PIECES + k]
            v_src = w_refs[(2 * side + 1) * PIECES + k]
            half_w, piece_n = u_src.shape
            piece_m = v_src.shape[0]
            u_dst = up_ref.at[span(owner, half_w), pl.ds(k * piece_n, piece_n)]
            v_dst = down_ref.at[span(owner * PIECES + k, piece_m), :]
            copies.append(pltpu.make_async_copy(u_src, u_dst, w_sem.at[len(copies)]))
            copies.append(pltpu.make_async_copy(v_src, v_dst, w_sem.at[len(copies)]))
    for copy in copies:
        copy.start()

    @pl.when(stage == 0)
    def _():
        def load(c, carry):
            pltpu.make_async_copy(batch_chunk(batch_ref, c, ()), x_buf.at[c], recv_sem.at[c]).start()
            return carry
        lax.fori_loop(0, n_chunks, load, 0)

    meet_neighbours(stage, n_stages)
    for copy in copies:
        copy.wait()

    def send_of(c):
        return pltpu.make_async_remote_copy(
            src_ref=y_buf.at[c], dst_ref=x_buf.at[c],
            send_sem=send_sem.at[c], recv_sem=recv_sem.at[c],
            device_id={"stage": stage + 1}, device_id_type=MESH_ID)

    def out_copy(c):
        return pltpu.make_async_copy(y_buf.at[c], batch_chunk(out_ref, c, (0,)), out_sem.at[c])

    def chunk(c, carry):
        pltpu.make_async_copy(batch_chunk(batch_ref, c, ()), x_buf.at[c], recv_sem.at[c]).wait()

        def tile(j, inner):
            cols = span(j, FWD_TILE)
            hid = gelu_value(dot_nn(x_buf[c], up_ref[:, cols])).astype(BF16)
            part = dot_nn(hid, down_ref[cols, :])
            acc_ref[...] = jnp.where(j == 0, part, acc_ref[...] + part)
            return inner

        lax.fori_loop(0, n_tiles, tile, 0)
        y_buf[c] = (x_buf[c].astype(F32) + acc_ref[...]).astype(BF16)
        out_copy(c).start()

        @pl.when(stage < last)
        def _():
            send_of(c).start()
        return carry

    lax.fori_loop(0, n_chunks, chunk, 0)

    def finish(c, carry):
        out_copy(c).wait()

        @pl.when(stage < last)
        def _():
            send_of(c).wait_send()
        return carry

    lax.fori_loop(0, n_chunks, finish, 0)


def forward(n_stages, n_rep, next_batch, weights):
    n_micro, rows, width = next_batch.shape
    hidden = PIECES * weights[0].shape[1]
    n_chunks = n_micro * rows // FWD_ROWS
    return pl.pallas_call(
        functools.partial(fwd_kernel, n_stages, n_rep),
        name="forward",
        out_shape=jax.ShapeDtypeStruct((1, n_micro, rows, width), BF16),
        in_specs=[ANY] * (1 + len(weights)),
        out_specs=ANY,
        scratch_shapes=[
            pltpu.VMEM((width, hidden), BF16),
            pltpu.VMEM((hidden, width), BF16),
            pltpu.VMEM((n_chunks, FWD_ROWS, width), BF16),
            pltpu.VMEM((n_chunks, FWD_ROWS, width), BF16),
            pltpu.VMEM((FWD_ROWS, width), F32),
            pltpu.SemaphoreType.DMA((len(weights),)),
            pltpu.SemaphoreType.DMA((n_chunks,)),
            pltpu.SemaphoreType.DMA((n_chunks,)),
            pltpu.SemaphoreType.DMA((n_chunks,)),
        ],
        compiler_params=pltpu.CompilerParams(collective_id=1, has_side_effects=True, vmem_limit_bytes=VMEM_LIMIT),
        cost_estimate=pl.CostEstimate(flops=4 * n_micro * rows * width * hidden, bytes_accessed=6 * rows * hidden, transcendentals=n_micro * rows * hidden),
    )(next_batch, *weights)


def solution(mesh):
    n_stages = mesh.shape["stage"]
    n_rep = mesh.shape["data"]
    swap = [(i, n_rep - 1 - i) for i in range(n_rep)]

    def exchange(x):
        return lax.ppermute(x, "data", swap)

    def local_step(master_up, master_down, mom1_up, mom1_down, mom2_up, mom2_down, grad_up, grad_down, stage_acts, loss_grad, next_batch, learn_rate, max_norm):
        me = lax.axis_index("data")
        mine = jnp.reshape(me, (1,)).astype(jnp.int32)
        other = 1 - mine
        hid, d_pre, g_own = backward(n_stages, stage_acts, loss_grad, master_up, master_down)

        def wgrad(k, owner, name):
            return wgrad_piece(k, owner, stage_acts, d_pre, grad_up, hid, g_own, grad_down, name)

        arrived, whose = [], other
        for k in range(PIECES):
            su, sv = wgrad(k, whose, "wgrad_peer")
            arrived.append((exchange(su), exchange(sv)))
            whose = lax.optimization_barrier((other, sv))[0]
        gbar, local_sq = [], jnp.zeros((), F32)
        for k in range(PIECES):
            su, sv = wgrad(k, mine, "wgrad_mine")
            bu = (su + arrived[k][0]) * (1.0 / n_rep)
            bv = (sv + arrived[k][1]) * (1.0 / n_rep)
            local_sq = local_sq + jnp.sum(bu * bu) + jnp.sum(bv * bv)
            gbar.append((bu, bv))
        gbar_other = [None] * PIECES
        for k in range(F32_FIRST):
            gbar_other[k] = (exchange(gbar[k][0]), exchange(gbar[k][1]))
        grad_norm = jnp.sqrt(lax.psum(local_sq, ("data", "stage")))
        clip_scale = jnp.minimum(1.0, max_norm / (grad_norm + NORM_EPS))
        knobs = jnp.stack([clip_scale, learn_rate])
        up_set = (master_up, mom1_up, mom2_up)
        down_set = (master_down, mom1_down, mom2_down)

        chain = ()
        own_w, other_w = [None] * PIECES, [None] * PIECES
        order = list(range(F32_FIRST, PIECES)) + list(range(F32_FIRST))
        for k in order:
            res = update_piece(k, mine, knobs, up_set, down_set, *gbar[k], chain, "update_mine")
            chain, own_w[k] = res[:6], res[6:]
            if k >= F32_FIRST:
                other_w[k] = (exchange(own_w[k][0]), exchange(own_w[k][1]))
        for k in range(F32_FIRST, PIECES):
            gbar_other[k] = (exchange(gbar[k][0]), exchange(gbar[k][1]))
        for k in range(F32_FIRST):
            res = update_piece(k, other, knobs, up_set, down_set, *gbar_other[k], chain, "update_peer")
            chain, other_w[k] = res[:6], res[6:]
        weights = []
        for side in (own_w, other_w):
            weights += [side[k][0] for k in range(PIECES)]
            weights += [side[k][1] for k in range(PIECES)]
        stage_outs = forward(n_stages, n_rep, next_batch, weights)
        for k in range(F32_FIRST, PIECES):
            res = update_piece(k, other, knobs, up_set, down_set, *gbar_other[k], chain, "update_peer")
            chain = res[:6]
        new_up, new_m1_up, new_m2_up, new_down, new_m1_down, new_m2_down = chain
        return (new_up, new_down, new_m1_up, new_m1_down, new_m2_up, new_m2_down, stage_outs)

    w_spec = P("stage", None, None)
    g_spec = P("data", "stage", None, None)
    in_specs = (w_spec,) * 6 + (g_spec, g_spec, P("stage", "data", None), P("data", None), P(None, "data", None), P(), P())
    out_specs = (w_spec,) * 6 + (P("stage", None, "data", None),)
    return jax.shard_map(local_step, mesh=mesh, in_specs=in_specs, out_specs=out_specs, check_vma=False)
```

```python
import functools

import jax
import jax.numpy as jnp
from jax import lax
from jax.experimental import pallas as pl
from jax.experimental.pallas import tpu as pltpu
from jax.sharding import PartitionSpec as P

BETA1 = 0.9
BETA2 = 0.95
ADAM_EPS = 1e-8
WEIGHT_DECAY = 0.1
NORM_EPS = 1e-6
ADAM_STEP = 8
SQRT_TWO_PI = 0.7978845608028654
GELU_CUBIC = 0.044715

BACK_ROWS = 256
FWD_ROWS = 256
BACK_TILE = 512
FWD_TILE = 512
PIECES = 3
F32_FIRST = ((0, 0),)
STAGING = 4
WGRAD_STEP = 1024
WGRAD_GRID = 2
UPDATE_GRID = 4

BF16 = jnp.bfloat16
F32 = jnp.float32
MESH_ID = pl.DeviceIdType.MESH
ANY = pl.BlockSpec(memory_space=pl.ANY)
VMEM_LIMIT = 60 * 1024 * 1024


def dot_nn(left, right):
    return lax.dot_general(left, right, (((1,), (0,)), ((), ())), preferred_element_type=F32)


def dot_nt(left, right):
    return lax.dot_general(left, right, (((1,), (1,)), ((), ())), preferred_element_type=F32)


def dot_tn(left, right):
    return lax.dot_general(left, right, (((0,), (0,)), ((), ())), preferred_element_type=F32)


def span(index, size):
    return pl.ds(pl.multiple_of(index * size, size), size)


def tanh_part(x, sq):
    return jnp.tanh(x * (SQRT_TWO_PI + (SQRT_TWO_PI * GELU_CUBIC) * sq))


def gelu_value(x):
    return x * (0.5 + 0.5 * tanh_part(x, x * x))


def gelu_pair(x):
    sq = x * x
    th = tanh_part(x, sq)
    half = 0.5 + 0.5 * th
    value = x * half
    slope = half + value * (1.0 - th) * (SQRT_TWO_PI + (3.0 * SQRT_TWO_PI * GELU_CUBIC) * sq)
    return value, slope


def meet_neighbours(stage, n_stages):
    barrier = pltpu.get_barrier_semaphore()

    @pl.when(stage > 0)
    def _():
        pl.semaphore_signal(barrier, inc=1, device_id={"stage": stage - 1}, device_id_type=MESH_ID)

    @pl.when(stage < n_stages - 1)
    def _():
        pl.semaphore_signal(barrier, inc=1, device_id={"stage": stage + 1}, device_id_type=MESH_ID)

    pl.semaphore_wait(barrier, jnp.minimum(stage, 1) + jnp.minimum(n_stages - 1 - stage, 1))


def back_kernel(n_stages, acts_ref, dy_ref, up32_ref, down32_ref, hid_ref, dpre_ref, gown_ref,
                up_ref, down_ref, g_buf, h_buf, p_buf, dx_buf, acc_ref, pre_buf, dh_buf, stage_u, stage_v,
                u_sem, v_sem, recv_sem, send_sem, gown_sem, h_sem, p_sem):
    stage = lax.axis_index("stage")
    last = n_stages - 1
    rows_all, width = g_buf.shape
    hidden = up_ref.shape[1]
    n_chunks = rows_all // BACK_ROWS
    n_tiles = hidden // BACK_TILE
    u_rows = stage_u.shape[1]
    v_rows = stage_v.shape[1]
    n_cast = width // u_rows

    def u_copy(i, slot):
        return pltpu.make_async_copy(up32_ref.at[0, span(i, u_rows), :], stage_u.at[slot], u_sem.at[slot])

    def v_copy(i, slot):
        return pltpu.make_async_copy(down32_ref.at[0, span(i, v_rows), :], stage_v.at[slot], v_sem.at[slot])

    for i in range(STAGING):
        u_copy(i, i).start()
        v_copy(i, i).start()

    def rows_of(c):
        return span(c, BACK_ROWS)

    @pl.when(stage == last)
    def _():
        def load(c, carry):
            pltpu.make_async_copy(dy_ref.at[rows_of(c), :], g_buf.at[rows_of(c), :], recv_sem.at[c]).start()
            return carry
        lax.fori_loop(0, n_chunks, load, 0)

    meet_neighbours(stage, n_stages)

    def cast(i, carry):
        slot = lax.rem(i, STAGING)
        u_copy(i, slot).wait()
        up_ref[span(i, u_rows), :] = stage_u[slot].astype(BF16)
        v_copy(i, slot).wait()
        down_ref[span(i, v_rows), :] = stage_v[slot].astype(BF16)

        @pl.when(i + STAGING < n_cast)
        def _():
            u_copy(i + STAGING, slot).start()
            v_copy(i + STAGING, slot).start()
        return carry

    lax.fori_loop(0, n_cast, cast, 0)

    def send_of(c):
        return pltpu.make_async_remote_copy(
            src_ref=dx_buf.at[rows_of(c), :], dst_ref=g_buf.at[rows_of(c), :],
            send_sem=send_sem.at[c], recv_sem=recv_sem.at[c],
            device_id={"stage": stage - 1}, device_id_type=MESH_ID)

    def out_copies(c, slot):
        return (pltpu.make_async_copy(h_buf.at[slot], hid_ref.at[rows_of(c), :], h_sem.at[slot]),
                pltpu.make_async_copy(p_buf.at[slot], dpre_ref.at[rows_of(c), :], p_sem.at[slot]))

    def gown_copy(c):
        return pltpu.make_async_copy(g_buf.at[rows_of(c), :], gown_ref.at[rows_of(c), :], gown_sem.at[c])

    def chunk(c, carry):
        slot = lax.rem(c, 2)
        rows = rows_of(c)

        @pl.when(c >= 2)
        def _():
            for copy in out_copies(c - 2, slot):
                copy.wait()

        pltpu.make_async_copy(dy_ref.at[rows, :], g_buf.at[rows, :], recv_sem.at[c]).wait()
        gown_copy(c).start()

        def products(j):
            cols = pl.ds(j * BACK_TILE, BACK_TILE)
            pre_buf[j % 2] = dot_nn(acts_ref[0, rows, :], up_ref[:, cols])
            dh_buf[j % 2] = dot_nt(g_buf[rows, :], down_ref[cols, :])

        def rest(j):
            cols = pl.ds(j * BACK_TILE, BACK_TILE)
            value, slope = gelu_pair(pre_buf[j % 2])
            h_buf[slot, :, cols] = value.astype(BF16)
            d_pre = (dh_buf[j % 2] * slope).astype(BF16)
            p_buf[slot, :, cols] = d_pre
            part = dot_nt(d_pre, up_ref[:, cols])
            if j == 0:
                acc_ref[...] = g_buf[rows, :].astype(F32) + part
            elif j < n_tiles - 1:
                acc_ref[...] += part
            else:
                dx_buf[rows, :] = (acc_ref[...] + part).astype(BF16)

        products(0)
        for j in range(n_tiles):
            if j + 1 < n_tiles:
                products(j + 1)
            rest(j)
        for copy in out_copies(c, slot):
            copy.start()

        @pl.when(stage > 0)
        def _():
            send_of(c).start()
        return carry

    lax.fori_loop(0, n_chunks, chunk, 0)

    for c in (n_chunks - 2, n_chunks - 1):
        for copy in out_copies(c, c % 2):
            copy.wait()

    def finish(c, carry):
        gown_copy(c).wait()

        @pl.when(stage > 0)
        def _():
            send_of(c).wait_send()
        return carry

    lax.fori_loop(0, n_chunks, finish, 0)


def backward(n_stages, acts, loss_grad, up32, down32):
    _, rows, width = acts.shape
    hidden = up32.shape[2]
    n_chunks = rows // BACK_ROWS
    u_rows, v_rows = width // 12, hidden // 12
    wide = jax.ShapeDtypeStruct((rows, hidden), BF16)
    return pl.pallas_call(
        functools.partial(back_kernel, n_stages),
        name="backward",
        out_shape=(wide, wide, jax.ShapeDtypeStruct((rows, width), BF16)),
        in_specs=[pl.BlockSpec(memory_space=pltpu.VMEM), ANY, ANY, ANY],
        out_specs=(ANY, ANY, ANY),
        scratch_shapes=[
            pltpu.VMEM((width, hidden), BF16),
            pltpu.VMEM((hidden, width), BF16),
            pltpu.VMEM((rows, width), BF16),
            pltpu.VMEM((2, BACK_ROWS, hidden), BF16),
            pltpu.VMEM((2, BACK_ROWS, hidden), BF16),
            pltpu.VMEM((rows, width), BF16),
            pltpu.VMEM((BACK_ROWS, width), F32),
            pltpu.VMEM((2, BACK_ROWS, BACK_TILE), F32),
            pltpu.VMEM((2, BACK_ROWS, BACK_TILE), F32),
            pltpu.VMEM((STAGING, u_rows, hidden), F32),
            pltpu.VMEM((STAGING, v_rows, width), F32),
            pltpu.SemaphoreType.DMA((STAGING,)),
            pltpu.SemaphoreType.DMA((STAGING,)),
            pltpu.SemaphoreType.DMA((n_chunks,)),
            pltpu.SemaphoreType.DMA((n_chunks,)),
            pltpu.SemaphoreType.DMA((n_chunks,)),
            pltpu.SemaphoreType.DMA((2,)),
            pltpu.SemaphoreType.DMA((2,)),
        ],
        compiler_params=pltpu.CompilerParams(collective_id=0, has_side_effects=True, vmem_limit_bytes=VMEM_LIMIT),
        cost_estimate=pl.CostEstimate(flops=6 * rows * width * hidden, bytes_accessed=6 * rows * hidden, transcendentals=rows * hidden),
    )(acts, loss_grad, up32, down32)


def wgrad_kernel(owner_ref, left_ref, right_ref, grad_ref, sum_ref):
    lead = len(left_ref.shape) - 2
    rows = right_ref.shape[0]
    acc = grad_ref[0, 0]
    for k in range(rows // WGRAD_STEP):
        part = pl.ds(k * WGRAD_STEP, WGRAD_STEP)
        acc = acc + dot_tn(left_ref[(0,) * lead + (part, slice(None))], right_ref[part, :])
    sum_ref[...] = acc


def wgrad_call(owner, operands, in_specs, out_spec, shape, steps, name):
    rows = operands[1].shape[0]
    return pl.pallas_call(
        wgrad_kernel,
        name=name,
        out_shape=jax.ShapeDtypeStruct(shape, F32),
        grid_spec=pltpu.PrefetchScalarGridSpec(num_scalar_prefetch=1, grid=(steps,), in_specs=in_specs, out_specs=out_spec),
        compiler_params=pltpu.CompilerParams(vmem_limit_bytes=VMEM_LIMIT),
        cost_estimate=pl.CostEstimate(flops=2 * rows * shape[0] * shape[1], bytes_accessed=15 * 1024 * 1024, transcendentals=0),
    )(owner, *operands)


def wgrad_up(k, owner, acts, d_pre, grad_up, name):
    _, rows, width = acts.shape
    half, piece = width // 2, d_pre.shape[1] // PIECES
    steps = WGRAD_GRID
    un = piece // steps
    in_specs = [
        pl.BlockSpec((1, rows, half), lambda i, own: (0, 0, own[0])),
        pl.BlockSpec((rows, un), lambda i, own: (0, k * steps + i)),
        pl.BlockSpec((1, 1, half, un), lambda i, own: (0, 0, own[0], k * steps + i)),
    ]
    return wgrad_call(owner, (acts, d_pre, grad_up), in_specs, pl.BlockSpec((half, un), lambda i, own: (0, i)), (half, piece), steps, name)


def wgrad_down(k, owner, hid, g_own, grad_down, name):
    rows, width = g_own.shape
    piece = hid.shape[1] // 2 // PIECES
    steps = 2
    vm = piece // steps
    in_specs = [
        pl.BlockSpec((rows, vm), lambda i, own: (0, (own[0] * PIECES + k) * steps + i)),
        pl.BlockSpec((rows, width), lambda i, own: (0, 0)),
        pl.BlockSpec((1, 1, vm, width), lambda i, own: (0, 0, (own[0] * PIECES + k) * steps + i, 0)),
    ]
    return wgrad_call(owner, (hid, g_own, grad_down), in_specs, pl.BlockSpec((vm, width), lambda i, own: (i, 0)), (piece, width), steps, name)


def update_kernel(n_alias, owner_ref, knobs_ref, w_ref, m_ref, v_ref, g_ref, *rest):
    w_out, m_out, v_out, b_out = rest[n_alias:]
    clip, lr = knobs_ref[0], knobs_ref[1]
    w = w_ref[0]
    q = clip * g_ref[...]
    m_new = BETA1 * m_ref[0] + (1.0 - BETA1) * q
    v_new = BETA2 * v_ref[0] + (1.0 - BETA2) * q * q
    m_hat = m_new * (1.0 / (1.0 - BETA1 ** ADAM_STEP))
    v_hat = v_new * (1.0 / (1.0 - BETA2 ** ADAM_STEP))
    w_new = w - lr * (m_hat / (jnp.sqrt(v_hat) + ADAM_EPS) + WEIGHT_DECAY * w)
    w_out[0], m_out[0], v_out[0] = w_new, m_new, v_new
    b_out[...] = w_new.astype(BF16)


def update_unit(kind, k, owner, knobs, state, gbar, chain, name):
    rows, cols = gbar.shape
    steps = UPDATE_GRID
    block = rows // steps
    if kind == 0:
        spec = pl.BlockSpec((1, block, cols), lambda i, own: (0, own[0] * steps + i, k))
    else:
        spec = pl.BlockSpec((1, block, cols), lambda i, own: (0, (own[0] * PIECES + k) * steps + i, 0))
    piece_spec = pl.BlockSpec((block, cols), lambda i, own: (i, 0))
    full = jax.ShapeDtypeStruct(state[0].shape, F32)
    return pl.pallas_call(
        functools.partial(update_kernel, len(chain)),
        name=name,
        out_shape=(full, full, full, jax.ShapeDtypeStruct((rows, cols), BF16)),
        grid_spec=pltpu.PrefetchScalarGridSpec(
            num_scalar_prefetch=1,
            grid=(steps,),
            in_specs=[pl.BlockSpec(memory_space=pltpu.SMEM)] + [spec] * 3 + [piece_spec] + [ANY] * len(chain),
            out_specs=(spec, spec, spec, piece_spec),
        ),
        input_output_aliases={6 + i: i for i in range(len(chain))},
        compiler_params=pltpu.CompilerParams(vmem_limit_bytes=VMEM_LIMIT),
        cost_estimate=pl.CostEstimate(flops=30 * rows * cols, bytes_accessed=30 * rows * cols, transcendentals=rows * cols),
    )(owner, knobs, *state, gbar, *chain)


def fwd_kernel(n_stages, n_rep, batch_ref, *refs):
    n_w = 2 * PIECES * n_rep
    w_refs = refs[:n_w]
    out_ref, up_ref, down_ref, x_buf, y_buf, acc_ref, pre_buf, w_sem, recv_sem, send_sem, out_sem = refs[n_w:]
    stage = lax.axis_index("stage")
    me = lax.axis_index("data")
    last = n_stages - 1
    n_chunks = x_buf.shape[0]
    hidden = up_ref.shape[1]
    n_tiles = hidden // FWD_TILE
    chunks_per_micro = n_chunks // batch_ref.shape[0]

    def batch_chunk(ref, c, lead):
        return ref.at[lead + (c // chunks_per_micro, span(lax.rem(c, chunks_per_micro), FWD_ROWS), slice(None))]

    copies = []
    for side in range(n_rep):
        owner = me if side == 0 else 1 - me
        for k in range(PIECES):
            u_src = w_refs[(2 * side) * PIECES + k]
            v_src = w_refs[(2 * side + 1) * PIECES + k]
            half_w, piece_n = u_src.shape
            piece_m = v_src.shape[0]
            u_dst = up_ref.at[span(owner, half_w), pl.ds(k * piece_n, piece_n)]
            v_dst = down_ref.at[span(owner * PIECES + k, piece_m), :]
            copies.append(pltpu.make_async_copy(u_src, u_dst, w_sem.at[len(copies)]))
            copies.append(pltpu.make_async_copy(v_src, v_dst, w_sem.at[len(copies)]))
    for copy in copies:
        copy.start()

    @pl.when(stage == 0)
    def _():
        def load(c, carry):
            pltpu.make_async_copy(batch_chunk(batch_ref, c, ()), x_buf.at[c], recv_sem.at[c]).start()
            return carry
        lax.fori_loop(0, n_chunks, load, 0)

    meet_neighbours(stage, n_stages)
    for copy in copies:
        copy.wait()

    def send_of(c):
        return pltpu.make_async_remote_copy(
            src_ref=y_buf.at[c], dst_ref=x_buf.at[c],
            send_sem=send_sem.at[c], recv_sem=recv_sem.at[c],
            device_id={"stage": stage + 1}, device_id_type=MESH_ID)

    def out_copy(c):
        return pltpu.make_async_copy(y_buf.at[c], batch_chunk(out_ref, c, (0,)), out_sem.at[c])

    def chunk(c, carry):
        pltpu.make_async_copy(batch_chunk(batch_ref, c, ()), x_buf.at[c], recv_sem.at[c]).wait()

        def products(j):
            pre_buf[j % 2] = dot_nn(x_buf[c], up_ref[:, pl.ds(j * FWD_TILE, FWD_TILE)])

        def rest(j):
            hid = gelu_value(pre_buf[j % 2]).astype(BF16)
            part = dot_nn(hid, down_ref[pl.ds(j * FWD_TILE, FWD_TILE), :])
            if j == 0:
                acc_ref[...] = x_buf[c].astype(F32) + part
            elif j < n_tiles - 1:
                acc_ref[...] += part
            else:
                y_buf[c] = (acc_ref[...] + part).astype(BF16)

        products(0)
        for j in range(n_tiles):
            if j + 1 < n_tiles:
                products(j + 1)
            rest(j)
        out_copy(c).start()

        @pl.when(stage < last)
        def _():
            send_of(c).start()
        return carry

    lax.fori_loop(0, n_chunks, chunk, 0)

    def finish(c, carry):
        out_copy(c).wait()

        @pl.when(stage < last)
        def _():
            send_of(c).wait_send()
        return carry

    lax.fori_loop(0, n_chunks, finish, 0)


def forward(n_stages, n_rep, next_batch, weights):
    n_micro, rows, width = next_batch.shape
    hidden = PIECES * weights[0].shape[1]
    n_chunks = n_micro * rows // FWD_ROWS
    return pl.pallas_call(
        functools.partial(fwd_kernel, n_stages, n_rep),
        name="forward",
        out_shape=jax.ShapeDtypeStruct((1, n_micro, rows, width), BF16),
        in_specs=[ANY] * (1 + len(weights)),
        out_specs=ANY,
        scratch_shapes=[
            pltpu.VMEM((width, hidden), BF16),
            pltpu.VMEM((hidden, width), BF16),
            pltpu.VMEM((n_chunks, FWD_ROWS, width), BF16),
            pltpu.VMEM((n_chunks, FWD_ROWS, width), BF16),
            pltpu.VMEM((FWD_ROWS, width), F32),
            pltpu.VMEM((2, FWD_ROWS, FWD_TILE), F32),
            pltpu.SemaphoreType.DMA((len(weights),)),
            pltpu.SemaphoreType.DMA((n_chunks,)),
            pltpu.SemaphoreType.DMA((n_chunks,)),
            pltpu.SemaphoreType.DMA((n_chunks,)),
        ],
        compiler_params=pltpu.CompilerParams(collective_id=1, has_side_effects=True, vmem_limit_bytes=VMEM_LIMIT),
        cost_estimate=pl.CostEstimate(flops=4 * n_micro * rows * width * hidden, bytes_accessed=6 * rows * hidden, transcendentals=n_micro * rows * hidden),
    )(next_batch, *weights)


def solution(mesh):
    n_stages = mesh.shape["stage"]
    n_rep = mesh.shape["data"]
    swap = [(i, n_rep - 1 - i) for i in range(n_rep)]

    def exchange(x):
        return lax.ppermute(x, "data", swap)

    def local_step(master_up, master_down, mom1_up, mom1_down, mom2_up, mom2_down, grad_up, grad_down, stage_acts, loss_grad, next_batch, learn_rate, max_norm):
        me = lax.axis_index("data")
        mine = jnp.reshape(me, (1,)).astype(jnp.int32)
        other = 1 - mine
        hid, d_pre, g_own = backward(n_stages, stage_acts, loss_grad, master_up, master_down)

        units = [(kind, k) for k in range(PIECES) for kind in (0, 1)]

        def wgrad(unit, owner, name):
            if unit[0] == 0:
                return wgrad_up(unit[1], owner, stage_acts, d_pre, grad_up, name)
            return wgrad_down(unit[1], owner, hid, g_own, grad_down, name)

        arrived, whose = {}, other
        for unit in units:
            part = wgrad(unit, whose, "wgrad_peer")
            arrived[unit] = exchange(part)
            whose = lax.optimization_barrier((other, part))[0]
        gbar, local_sq = {}, jnp.zeros((), F32)
        for unit in units:
            gbar[unit] = (wgrad(unit, mine, "wgrad_mine") + arrived[unit]) * (1.0 / n_rep)
            local_sq = local_sq + jnp.sum(gbar[unit] * gbar[unit])
        grad_norm = jnp.sqrt(lax.psum(local_sq, ("data", "stage")))
        clip_scale = jnp.minimum(1.0, max_norm / (grad_norm + NORM_EPS))
        knobs = jnp.stack([clip_scale, learn_rate])
        gbar_other = {}
        for unit in F32_FIRST:
            gbar_other[unit] = exchange(lax.optimization_barrier((gbar[unit], knobs))[0])
        state = ((master_up, mom1_up, mom2_up), (master_down, mom1_down, mom2_down))
        chain = [(), ()]

        def update(unit, owner, grad, name):
            res = update_unit(unit[0], unit[1], owner, knobs, state[unit[0]], grad, chain[unit[0]], name)
            chain[unit[0]] = res[:3]
            return res[3]

        late = [unit for unit in units if unit not in F32_FIRST]
        own_w, other_w = {}, {}
        for unit in late + list(F32_FIRST):
            own_w[unit] = update(unit, mine, gbar[unit], "update_mine")
            if unit in late:
                other_w[unit] = exchange(own_w[unit])
        for unit in late:
            gbar_other[unit] = exchange(lax.optimization_barrier((gbar[unit], own_w[late[-1]]))[0])
        for unit in F32_FIRST:
            other_w[unit] = update(unit, other, gbar_other[unit], "update_peer")
        weights = []
        for side in (own_w, other_w):
            for kind in (0, 1):
                weights += [side[kind, k] for k in range(PIECES)]
        stage_outs = forward(n_stages, n_rep, next_batch, weights)
        for unit in late:
            update(unit, other, gbar_other[unit], "update_peer")
        (new_up, new_m1_up, new_m2_up), (new_down, new_m1_down, new_m2_down) = chain
        return (new_up, new_down, new_m1_up, new_m1_down, new_m2_up, new_m2_down, stage_outs)

    w_spec = P("stage", None, None)
    g_spec = P("data", "stage", None, None)
    in_specs = (w_spec,) * 6 + (g_spec, g_spec, P("stage", "data", None), P("data", None), P(None, "data", None), P(), P())
    out_specs = (w_spec,) * 6 + (P("stage", None, "data", None),)
    return jax.shard_map(local_step, mesh=mesh, in_specs=in_specs, out_specs=out_specs, check_vma=False)
```

```python
import functools

import jax
import jax.numpy as jnp
from jax import lax
from jax.experimental import pallas as pl
from jax.experimental.pallas import tpu as pltpu
from jax.sharding import PartitionSpec as P


BETA1 = 0.9
BETA2 = 0.95
ADAM_EPS = 1e-8
WEIGHT_DECAY = 0.1
NORM_EPS = 1e-6
ADAM_STEP = 8
SQRT_TWO_PI = 0.7978845608028654
GELU_CUBIC = 0.044715

BACK_ROWS = 256
FWD_ROWS = 256
BACK_TILE = 512
FWD_TILE = 512
PIECES = 6
F32_FIRST = ((0, 0),)
TAIL = ((0, 1, 5), (1, 0, 5), (0, 5, 6), (1, 5, 6))
STAGING = 4
WGRAD_STEP = 1024
WGRAD_GRID = 2
UPDATE_GRID = 4

BF16 = jnp.bfloat16
F32 = jnp.float32
MESH_ID = pl.DeviceIdType.MESH
ANY = pl.BlockSpec(memory_space=pl.ANY)
VMEM_LIMIT = 60 * 1024 * 1024
FWD_VMEM = 54000000
STORE_VMEM = 4 * 1024 * 1024
UPDATE_VMEM = 60 * 1024 * 1024


def dot_nn(left, right):
    return lax.dot_general(left, right, (((1,), (0,)), ((), ())), preferred_element_type=F32)


def dot_nt(left, right):
    return lax.dot_general(left, right, (((1,), (1,)), ((), ())), preferred_element_type=F32)


def dot_tn(left, right):
    return lax.dot_general(left, right, (((0,), (0,)), ((), ())), preferred_element_type=F32)


def span(index, size):
    return pl.ds(pl.multiple_of(index * size, size), size)


def tanh_part(x, sq):
    return jnp.tanh(x * (SQRT_TWO_PI + (SQRT_TWO_PI * GELU_CUBIC) * sq))


def gelu_value(x):
    return x * (0.5 + 0.5 * tanh_part(x, x * x))


def gelu_pair(x):
    sq = x * x
    th = tanh_part(x, sq)
    half = 0.5 + 0.5 * th
    value = x * half
    slope = half + value * (1.0 - th) * (SQRT_TWO_PI + (3.0 * SQRT_TWO_PI * GELU_CUBIC) * sq)
    return value, slope


def meet_neighbours(stage, n_stages):
    barrier = pltpu.get_barrier_semaphore()

    @pl.when(stage > 0)
    def _():
        pl.semaphore_signal(barrier, inc=1, device_id={"stage": stage - 1}, device_id_type=MESH_ID)

    @pl.when(stage < n_stages - 1)
    def _():
        pl.semaphore_signal(barrier, inc=1, device_id={"stage": stage + 1}, device_id_type=MESH_ID)

    pl.semaphore_wait(barrier, jnp.minimum(stage, 1) + jnp.minimum(n_stages - 1 - stage, 1))


def back_kernel(n_stages, acts_ref, dy_ref, up32_ref, down32_ref, hid_ref, dpre_ref, gown_ref,
                up_ref, down_ref, g_buf, h_buf, p_buf, dx_buf, acc_ref, pre_buf, dh_buf, stage_u, stage_v,
                u_sem, v_sem, recv_sem, send_sem, gown_sem, h_sem, p_sem):
    stage = lax.axis_index("stage")
    last = n_stages - 1
    rows_all, width = g_buf.shape
    hidden = up_ref.shape[1]
    n_chunks = rows_all // BACK_ROWS
    n_tiles = hidden // BACK_TILE
    u_rows = stage_u.shape[1]
    v_rows = stage_v.shape[1]
    n_cast = width // u_rows

    def u_copy(i, slot):
        return pltpu.make_async_copy(up32_ref.at[0, span(i, u_rows), :], stage_u.at[slot], u_sem.at[slot])

    def v_copy(i, slot):
        return pltpu.make_async_copy(down32_ref.at[0, span(i, v_rows), :], stage_v.at[slot], v_sem.at[slot])

    for i in range(STAGING):
        u_copy(i, i).start()
        v_copy(i, i).start()

    def rows_of(c):
        return span(c, BACK_ROWS)

    @pl.when(stage == last)
    def _():
        def load(c, carry):
            pltpu.make_async_copy(dy_ref.at[rows_of(c), :], g_buf.at[rows_of(c), :], recv_sem.at[c]).start()
            return carry

        lax.fori_loop(0, n_chunks, load, 0)

    meet_neighbours(stage, n_stages)

    def cast(i, carry):
        slot = lax.rem(i, STAGING)
        u_copy(i, slot).wait()
        up_ref[span(i, u_rows), :] = stage_u[slot].astype(BF16)
        v_copy(i, slot).wait()
        down_ref[span(i, v_rows), :] = stage_v[slot].astype(BF16)

        @pl.when(i + STAGING < n_cast)
        def _():
            u_copy(i + STAGING, slot).start()
            v_copy(i + STAGING, slot).start()

        return carry

    lax.fori_loop(0, n_cast, cast, 0)

    def send_of(c):
        return pltpu.make_async_remote_copy(
            src_ref=dx_buf.at[rows_of(c), :], dst_ref=g_buf.at[rows_of(c), :],
            send_sem=send_sem.at[c], recv_sem=recv_sem.at[c],
            device_id={"stage": stage - 1}, device_id_type=MESH_ID)

    def out_copies(c, slot):
        return (pltpu.make_async_copy(h_buf.at[slot], hid_ref.at[rows_of(c), :], h_sem.at[slot]),
                pltpu.make_async_copy(p_buf.at[slot], dpre_ref.at[rows_of(c), :], p_sem.at[slot]))

    def gown_copy(c):
        return pltpu.make_async_copy(g_buf.at[rows_of(c), :], gown_ref.at[rows_of(c), :], gown_sem.at[c])

    def chunk(c, carry):
        slot = lax.rem(c, 2)
        rows = rows_of(c)

        @pl.when(c >= 2)
        def _():
            for copy in out_copies(c - 2, slot):
                copy.wait()

        pltpu.make_async_copy(dy_ref.at[rows, :], g_buf.at[rows, :], recv_sem.at[c]).wait()
        gown_copy(c).start()

        def products(j):
            cols = pl.ds(j * BACK_TILE, BACK_TILE)
            pre_buf[j % 2] = dot_nn(acts_ref[0, rows, :], up_ref[:, cols])
            dh_buf[j % 2] = dot_nt(g_buf[rows, :], down_ref[cols, :])

        def rest(j):
            cols = pl.ds(j * BACK_TILE, BACK_TILE)
            value, slope = gelu_pair(pre_buf[j % 2])
            h_buf[slot, :, cols] = value.astype(BF16)
            d_pre = (dh_buf[j % 2] * slope).astype(BF16)
            p_buf[slot, :, cols] = d_pre
            part = dot_nt(d_pre, up_ref[:, cols])
            if j == 0:
                acc_ref[...] = g_buf[rows, :].astype(F32) + part
            elif j < n_tiles - 1:
                acc_ref[...] += part
            else:
                dx_buf[rows, :] = (acc_ref[...] + part).astype(BF16)

        products(0)
        for j in range(n_tiles):
            if j + 1 < n_tiles:
                products(j + 1)
            rest(j)
        for copy in out_copies(c, slot):
            copy.start()

        @pl.when(stage > 0)
        def _():
            send_of(c).start()

        return carry

    lax.fori_loop(0, n_chunks, chunk, 0)

    for c in (n_chunks - 2, n_chunks - 1):
        for copy in out_copies(c, c % 2):
            copy.wait()

    def finish(c, carry):
        gown_copy(c).wait()

        @pl.when(stage > 0)
        def _():
            send_of(c).wait_send()

        return carry

    lax.fori_loop(0, n_chunks, finish, 0)


def backward(n_stages, acts, loss_grad, up32, down32):
    _, rows, width = acts.shape
    hidden = up32.shape[2]
    n_chunks = rows // BACK_ROWS
    u_rows, v_rows = width // 12, hidden // 12
    wide = jax.ShapeDtypeStruct((rows, hidden), BF16)
    return pl.pallas_call(
        functools.partial(back_kernel, n_stages),
        name="backward",
        out_shape=(wide, wide, jax.ShapeDtypeStruct((rows, width), BF16)),
        in_specs=[pl.BlockSpec(memory_space=pltpu.VMEM), ANY, ANY, ANY],
        out_specs=(ANY, ANY, ANY),
        scratch_shapes=[
            pltpu.VMEM((width, hidden), BF16),
            pltpu.VMEM((hidden, width), BF16),
            pltpu.VMEM((rows, width), BF16),
            pltpu.VMEM((2, BACK_ROWS, hidden), BF16),
            pltpu.VMEM((2, BACK_ROWS, hidden), BF16),
            pltpu.VMEM((rows, width), BF16),
            pltpu.VMEM((BACK_ROWS, width), F32),
            pltpu.VMEM((2, BACK_ROWS, BACK_TILE), F32),
            pltpu.VMEM((2, BACK_ROWS, BACK_TILE), F32),
            pltpu.VMEM((STAGING, u_rows, hidden), F32),
            pltpu.VMEM((STAGING, v_rows, width), F32),
            pltpu.SemaphoreType.DMA((STAGING,)),
            pltpu.SemaphoreType.DMA((STAGING,)),
            pltpu.SemaphoreType.DMA((n_chunks,)),
            pltpu.SemaphoreType.DMA((n_chunks,)),
            pltpu.SemaphoreType.DMA((n_chunks,)),
            pltpu.SemaphoreType.DMA((2,)),
            pltpu.SemaphoreType.DMA((2,)),
        ],
        compiler_params=pltpu.CompilerParams(collective_id=0, has_side_effects=True, vmem_limit_bytes=VMEM_LIMIT),
        cost_estimate=pl.CostEstimate(flops=6 * rows * width * hidden, bytes_accessed=6 * rows * hidden, transcendentals=rows * hidden),
    )(acts, loss_grad, up32, down32)


def wgrad_kernel(owner_ref, left_ref, right_ref, grad_ref, sum_ref):
    lead = (0,) * (len(left_ref.shape) - 2)
    sum_ref[...] = grad_ref[0, 0]

    def step(k, carry):
        part = span(k, WGRAD_STEP)
        sum_ref[...] += dot_tn(left_ref[lead + (part, slice(None))], right_ref[part, :])
        return carry

    lax.fori_loop(0, right_ref.shape[0] // WGRAD_STEP, step, 0)


def wgrad_call(owner, operands, in_specs, out_spec, shape, steps):
    rows = operands[1].shape[0]
    return pl.pallas_call(
        wgrad_kernel,
        out_shape=jax.ShapeDtypeStruct(shape, F32),
        grid_spec=pltpu.PrefetchScalarGridSpec(num_scalar_prefetch=1, grid=(steps,), in_specs=in_specs, out_specs=out_spec),
        compiler_params=pltpu.CompilerParams(vmem_limit_bytes=VMEM_LIMIT),
        cost_estimate=pl.CostEstimate(flops=2 * rows * shape[0] * shape[1], bytes_accessed=15 * 1024 * 1024, transcendentals=0),
    )(owner, *operands)


def wgrad_up(k, owner, acts, d_pre, grad_up):
    _, rows, width = acts.shape
    half, piece = width // 2, d_pre.shape[1] // PIECES
    steps = WGRAD_GRID
    un = piece // steps
    in_specs = [
        pl.BlockSpec((1, rows, half), lambda i, own: (0, 0, own[0])),
        pl.BlockSpec((rows, un), lambda i, own: (0, k * steps + i)),
        pl.BlockSpec((1, 1, half, un), lambda i, own: (0, 0, own[0], k * steps + i)),
    ]
    return wgrad_call(owner, (acts, d_pre, grad_up), in_specs, pl.BlockSpec((half, un), lambda i, own: (0, i)), (half, piece), steps)


def wgrad_down(k, owner, hid, g_own, grad_down):
    rows, width = g_own.shape
    piece = hid.shape[1] // 2 // PIECES
    steps = WGRAD_GRID
    vm = piece // steps
    in_specs = [
        pl.BlockSpec((rows, vm), lambda i, own: (0, (own[0] * PIECES + k) * steps + i)),
        pl.BlockSpec((rows, width), lambda i, own: (0, 0)),
        pl.BlockSpec((1, 1, vm, width), lambda i, own: (0, 0, (own[0] * PIECES + k) * steps + i, 0)),
    ]
    return wgrad_call(owner, (hid, g_own, grad_down), in_specs, pl.BlockSpec((vm, width), lambda i, own: (i, 0)), (piece, width), steps)


def update_kernel(n_pieces, n_alias, owner_ref, lr_ref, clip_ref, w_ref, m_ref, v_ref, *rest):
    g_refs = rest[:n_pieces]
    w_out, m_out, v_out = rest[n_pieces + n_alias:n_pieces + n_alias + 3]
    b_outs = rest[n_pieces + n_alias + 3:]
    clip, lr = clip_ref[0:1, 0:1], lr_ref[0]

    def run(g_ref, b_out):
        w = w_ref[0]
        q = clip * g_ref[...]
        m_new = BETA1 * m_ref[0] + (1.0 - BETA1) * q
        v_new = BETA2 * v_ref[0] + (1.0 - BETA2) * q * q
        m_hat = m_new * (1.0 / (1.0 - BETA1 ** ADAM_STEP))
        v_hat = v_new * (1.0 / (1.0 - BETA2 ** ADAM_STEP))
        w_new = w - lr * (m_hat / (jnp.sqrt(v_hat) + ADAM_EPS) + WEIGHT_DECAY * w)
        w_out[0], m_out[0], v_out[0] = w_new, m_new, v_new
        if b_out is not None:
            b_out[...] = w_new.astype(BF16)

    if n_pieces == 1:
        run(g_refs[0], b_outs[0] if b_outs else None)
    else:
        for p in range(n_pieces):
            pl.when(pl.program_id(0) == p)(functools.partial(run, g_refs[p], None))


def update_units(kind, first, owner, knobs, state, grads, chain, want_bf16):
    rows, cols = grads[0].shape
    n = len(grads)
    steps = UPDATE_GRID
    block = rows // steps
    if kind == 0:
        spec = pl.BlockSpec((1, block, cols), lambda p, i, own: (0, own[0] * steps + i, first + p))
    else:
        spec = pl.BlockSpec((1, block, cols), lambda p, i, own: (0, (own[0] * PIECES + first + p) * steps + i, 0))

    def piece_spec(q):
        return pl.BlockSpec((block, cols), lambda p, i, own: (jnp.clip((p - q) * steps + i, 0, steps - 1), 0))

    full = jax.ShapeDtypeStruct(state[0].shape, F32)
    out_shape, out_specs = (full,) * 3, (spec,) * 3
    if want_bf16:
        out_shape += (jax.ShapeDtypeStruct((rows, cols), BF16),)
        out_specs += (piece_spec(0),)
    size = n * rows * cols
    return pl.pallas_call(
        functools.partial(update_kernel, n, len(chain)),
        out_shape=out_shape,
        grid_spec=pltpu.PrefetchScalarGridSpec(
            num_scalar_prefetch=1,
            grid=(n, steps),
            in_specs=[pl.BlockSpec(memory_space=pltpu.SMEM), pl.BlockSpec(memory_space=pltpu.VMEM)] + [spec] * 3 + [piece_spec(q) for q in range(n)] + [ANY] * len(chain),
            out_specs=out_specs,
        ),
        input_output_aliases={6 + n + i: i for i in range(len(chain))},
        compiler_params=pltpu.CompilerParams(vmem_limit_bytes=UPDATE_VMEM),
        cost_estimate=pl.CostEstimate(flops=30 * size, bytes_accessed=28 * size, transcendentals=size),
    )(owner, *knobs, *state, *grads, *chain)


def norm_kernel(n_stages, n_rep, n_parts, *refs):
    parts, (max_ref, clip_ref, mine, slots, send_sem, recv_sem) = refs[:n_parts], refs[n_parts:]
    n_dev = n_stages * n_rep
    me = lax.axis_index("data") * n_stages + lax.axis_index("stage")
    total = parts[0][0]
    for part in parts[1:]:
        total = total + part[0]
    mine[...] = jnp.full(mine.shape, total, F32)
    slots[me] = jnp.full(mine.shape, total, F32)

    def place(d):
        q = lax.rem(me + d, n_dev)
        return {"data": q // n_stages, "stage": lax.rem(q, n_stages)}

    barrier = pltpu.get_barrier_semaphore()
    for d in range(1, n_dev):
        pl.semaphore_signal(barrier, inc=1, device_id=place(d), device_id_type=MESH_ID)
    pl.semaphore_wait(barrier, n_dev - 1)
    copies = []
    for d in range(1, n_dev):
        copies.append(pltpu.make_async_remote_copy(
            src_ref=mine, dst_ref=slots.at[me], send_sem=send_sem.at[d - 1], recv_sem=recv_sem.at[d - 1],
            device_id=place(d), device_id_type=MESH_ID))
        copies[-1].start()
    for copy in copies:
        copy.wait()
    square = slots[0]
    for q in range(1, n_dev):
        square = square + slots[q]
    clip_ref[...] = jnp.minimum(1.0, max_ref[0] / (jnp.sqrt(square) + NORM_EPS))


def clip_factor(n_stages, n_rep, parts, max_norm):
    n_dev = n_stages * n_rep
    return pl.pallas_call(
        functools.partial(norm_kernel, n_stages, n_rep, len(parts)),
        name="clip_factor",
        out_shape=jax.ShapeDtypeStruct((8, 128), F32),
        in_specs=[pl.BlockSpec(memory_space=pltpu.SMEM)] * (len(parts) + 1),
        out_specs=pl.BlockSpec(memory_space=pltpu.VMEM),
        scratch_shapes=[
            pltpu.VMEM((8, 128), F32),
            pltpu.VMEM((n_dev, 8, 128), F32),
            pltpu.SemaphoreType.DMA((n_dev - 1,)),
            pltpu.SemaphoreType.DMA((n_dev - 1,)),
        ],
        compiler_params=pltpu.CompilerParams(collective_id=2, has_side_effects=True),
        cost_estimate=pl.CostEstimate(flops=40000000, bytes_accessed=4096, transcendentals=0),
    )(*parts, max_norm)


def fwd_kernel(n_stages, n_rep, batch_ref, *refs):
    n_w = 2 * PIECES * n_rep
    w_refs = refs[:n_w]
    out_ref, up_ref, down_ref, x_buf, acc_ref, pre_buf, w_sem, recv_sem, send_sem = refs[n_w:]
    stage = lax.axis_index("stage")
    me = lax.axis_index("data")
    last = n_stages - 1
    n_chunks = x_buf.shape[0]
    hidden = up_ref.shape[1]
    n_tiles = hidden // FWD_TILE
    chunks_per_micro = n_chunks // batch_ref.shape[0]

    def batch_chunk(ref, c, lead):
        return ref.at[lead + (c // chunks_per_micro, span(lax.rem(c, chunks_per_micro), FWD_ROWS), slice(None))]

    copies = []
    for side in range(n_rep):
        owner = me if side == 0 else 1 - me
        for k in range(PIECES):
            u_src = w_refs[(2 * side) * PIECES + k]
            v_src = w_refs[(2 * side + 1) * PIECES + k]
            half_w, piece_n = u_src.shape
            piece_m = v_src.shape[0]
            u_dst = up_ref.at[span(owner, half_w), pl.ds(k * piece_n, piece_n)]
            v_dst = down_ref.at[span(owner * PIECES + k, piece_m), :]
            copies.append(pltpu.make_async_copy(u_src, u_dst, w_sem.at[len(copies)]))
            copies.append(pltpu.make_async_copy(v_src, v_dst, w_sem.at[len(copies)]))
    for copy in copies:
        copy.start()

    @pl.when(stage == 0)
    def _():
        def load(c, carry):
            pltpu.make_async_copy(batch_chunk(batch_ref, c, ()), x_buf.at[c], recv_sem.at[c]).start()
            return carry

        lax.fori_loop(0, n_chunks, load, 0)

    meet_neighbours(stage, n_stages)
    for copy in copies:
        copy.wait()

    def send_of(c):
        return pltpu.make_async_remote_copy(
            src_ref=batch_chunk(out_ref, c, (0,)), dst_ref=x_buf.at[c],
            send_sem=send_sem.at[c], recv_sem=recv_sem.at[c],
            device_id={"stage": stage + 1}, device_id_type=MESH_ID)

    def chunk(c, carry):
        pltpu.make_async_copy(batch_chunk(batch_ref, c, ()), x_buf.at[c], recv_sem.at[c]).wait()

        def products(j):
            pre_buf[j % 2] = dot_nn(x_buf[c], up_ref[:, pl.ds(j * FWD_TILE, FWD_TILE)])

        def rest(j):
            hid = gelu_value(pre_buf[j % 2]).astype(BF16)
            part = dot_nn(hid, down_ref[pl.ds(j * FWD_TILE, FWD_TILE), :])
            if j == 0:
                acc_ref[...] = x_buf[c].astype(F32) + part
            elif j < n_tiles - 1:
                acc_ref[...] += part
            else:
                out_ref[0, c // chunks_per_micro, span(lax.rem(c, chunks_per_micro), FWD_ROWS), :] = (acc_ref[...] + part).astype(BF16)

        products(0)
        for j in range(n_tiles):
            if j + 1 < n_tiles:
                products(j + 1)
            rest(j)

        @pl.when(stage < last)
        def _():
            send_of(c).start()

        return carry

    lax.fori_loop(0, n_chunks, chunk, 0)

    @pl.when(stage < last)
    def _():
        def finish(c, carry):
            send_of(c).wait_send()
            return carry

        lax.fori_loop(0, n_chunks, finish, 0)


def forward(n_stages, n_rep, next_batch, weights):
    n_micro, rows, width = next_batch.shape
    hidden = PIECES * weights[0].shape[1]
    n_chunks = n_micro * rows // FWD_ROWS
    return pl.pallas_call(
        functools.partial(fwd_kernel, n_stages, n_rep),
        name="forward",
        out_shape=pltpu.VMEM((1, n_micro, rows, width), BF16),
        in_specs=[ANY] * (1 + len(weights)),
        out_specs=pl.BlockSpec(memory_space=pltpu.VMEM),
        scratch_shapes=[
            pltpu.VMEM((width, hidden), BF16),
            pltpu.VMEM((hidden, width), BF16),
            pltpu.VMEM((n_chunks, FWD_ROWS, width), BF16),
            pltpu.VMEM((FWD_ROWS, width), F32),
            pltpu.VMEM((2, FWD_ROWS, FWD_TILE), F32),
            pltpu.SemaphoreType.DMA((len(weights),)),
            pltpu.SemaphoreType.DMA((n_chunks,)),
            pltpu.SemaphoreType.DMA((n_chunks,)),
        ],
        compiler_params=pltpu.CompilerParams(collective_id=1, has_side_effects=True, vmem_limit_bytes=FWD_VMEM),
        cost_estimate=pl.CostEstimate(flops=4 * n_micro * rows * width * hidden, bytes_accessed=6 * rows * hidden, transcendentals=n_micro * rows * hidden),
    )(next_batch, *weights)


def store_kernel(y_ref, out_ref, sem):
    copies = []
    for i in range(y_ref.shape[1]):
        copies.append(pltpu.make_async_copy(y_ref.at[0, i], out_ref.at[0, i], sem.at[i]))
        copies[-1].start()
    for copy in copies:
        copy.wait()


def store(y):
    return pl.pallas_call(
        store_kernel,
        name="store",
        out_shape=jax.ShapeDtypeStruct(y.shape, y.dtype),
        in_specs=[pl.BlockSpec(memory_space=pltpu.VMEM)],
        out_specs=ANY,
        scratch_shapes=[pltpu.SemaphoreType.DMA((y.shape[1],))],
        compiler_params=pltpu.CompilerParams(vmem_limit_bytes=STORE_VMEM),
        cost_estimate=pl.CostEstimate(flops=4000000, bytes_accessed=2 * y.size, transcendentals=0),
    )(y)


def solution(mesh):
    n_stages = mesh.shape["stage"]
    n_rep = mesh.shape["data"]
    swap = [(i, n_rep - 1 - i) for i in range(n_rep)]

    def exchange(x):
        return lax.ppermute(x, "data", swap)

    def local_step(master_up, master_down, mom1_up, mom1_down, mom2_up, mom2_down, grad_up, grad_down, stage_acts, loss_grad, next_batch, learn_rate, max_norm):
        me = lax.axis_index("data")
        mine = jnp.reshape(me, (1,)).astype(jnp.int32)
        other = 1 - mine
        hid, d_pre, g_own = backward(n_stages, stage_acts, loss_grad, master_up, master_down)

        units = [(kind, k) for k in range(PIECES) for kind in (0, 1)]

        def wgrad(unit, owner):
            if unit[0] == 0:
                return wgrad_up(unit[1], owner, stage_acts, d_pre, grad_up)
            return wgrad_down(unit[1], owner, hid, g_own, grad_down)

        arrived, whose = {}, other
        for unit in units:
            part = wgrad(unit, whose)
            arrived[unit] = exchange(part)
            whose = lax.optimization_barrier((other, part))[0]
        gbar, squares = {}, []
        for unit in units:
            gbar[unit] = (wgrad(unit, mine) + arrived[unit]) * (1.0 / n_rep)
            squares.append(jnp.reshape(jnp.sum(gbar[unit] * gbar[unit]), (1,)))
        clip = clip_factor(n_stages, n_rep, squares, jnp.reshape(max_norm, (1,)))
        knobs = (jnp.reshape(learn_rate, (1,)), clip)
        gbar_other = {}
        for unit in F32_FIRST:
            gbar_other[unit] = exchange(lax.optimization_barrier((gbar[unit], clip))[0])
        state = ((master_up, mom1_up, mom2_up), (master_down, mom1_down, mom2_down))
        chain = [(), ()]

        def update(unit, owner, grad):
            res = update_units(unit[0], unit[1], owner, knobs, state[unit[0]], [grad], chain[unit[0]], True)
            chain[unit[0]] = res[:3]
            return res[3]

        def update_group(kind, first, stop):
            grads = [gbar_other[kind, k] for k in range(first, stop)]
            chain[kind] = update_units(kind, first, other, knobs, state[kind], grads, chain[kind], False)

        late = [unit for unit in units if unit not in F32_FIRST]
        own_w, other_w = {}, {}
        for unit in late + list(F32_FIRST):
            own_w[unit] = update(unit, mine, gbar[unit])
            if unit in late:
                other_w[unit] = exchange(own_w[unit])
        for unit in late:
            ready = lax.optimization_barrier((gbar[unit], own_w[late[-1]]))[0]
            gbar_other[unit] = exchange(ready)
        for unit in F32_FIRST:
            other_w[unit] = update(unit, other, gbar_other[unit])
        weights = []
        for side in (own_w, other_w):
            for kind in (0, 1):
                weights += [side[kind, k] for k in range(PIECES)]
        stage_outs = store(forward(n_stages, n_rep, next_batch, weights))
        for kind, first, stop in TAIL:
            update_group(kind, first, stop)
        (new_up, new_m1_up, new_m2_up), (new_down, new_m1_down, new_m2_down) = chain
        return (new_up, new_down, new_m1_up, new_m1_down, new_m2_up, new_m2_down, stage_outs)

    w_spec = P("stage", None, None)
    g_spec = P("data", "stage", None, None)
    in_specs = (w_spec,) * 6 + (g_spec, g_spec, P("stage", "data", None), P("data", None), P(None, "data", None), P(), P())
    out_specs = (w_spec,) * 6 + (P("stage", None, "data", None),)
    return jax.shard_map(local_step, mesh=mesh, in_specs=in_specs, out_specs=out_specs, check_vma=False)
```

```python
import functools

import jax
import jax.numpy as jnp
from jax import lax
from jax.experimental import pallas as pl
from jax.experimental.pallas import tpu as pltpu
from jax.sharding import PartitionSpec as P


BETA1 = 0.9
BETA2 = 0.95
ADAM_EPS = 1e-8
WEIGHT_DECAY = 0.1
NORM_EPS = 1e-6
ADAM_STEP = 8
SQRT_TWO_PI = 0.7978845608028654
GELU_CUBIC = 0.044715

BACK_ROWS = 256
FWD_ROWS = 256
BACK_TILE = 512
FWD_TILE = 512
PIECES = 6
F32_FIRST = ((0, 0),)
GROUPS = ((0, 0, 1), (1, 0, 2), (0, 1, 2), (1, 2, 2), (0, 3, 2), (1, 4, 2), (0, 5, 1))
TAIL = ((1, 0, 4), (0, 1, 5), (1, 4, 6), (0, 5, 6))
STAGING = 3
WGRAD_STEP = 4096
SLAB = 32

BF16 = jnp.bfloat16
F32 = jnp.float32
MESH_ID = pl.DeviceIdType.MESH
ANY = pl.BlockSpec(memory_space=pl.ANY)
VMEM_LIMIT = 60 * 1024 * 1024
FWD_VMEM = 54000000
STORE_VMEM = 4 * 1024 * 1024
UPDATE_VMEM = 60 * 1024 * 1024


def dot_nn(left, right):
    return lax.dot_general(left, right, (((1,), (0,)), ((), ())), preferred_element_type=F32)


def dot_nt(left, right):
    return lax.dot_general(left, right, (((1,), (1,)), ((), ())), preferred_element_type=F32)


def dot_tn(left, right):
    return lax.dot_general(left, right, (((0,), (0,)), ((), ())), preferred_element_type=F32)


def span(index, size):
    return pl.ds(pl.multiple_of(index * size, size), size)


def tanh_part(x, sq):
    return jnp.tanh(x * (SQRT_TWO_PI + (SQRT_TWO_PI * GELU_CUBIC) * sq))


def gelu_value(x):
    return x * (0.5 + 0.5 * tanh_part(x, x * x))


def gelu_pair(x):
    sq = x * x
    th = tanh_part(x, sq)
    half = 0.5 + 0.5 * th
    value = x * half
    slope = half + value * (1.0 - th) * (SQRT_TWO_PI + (3.0 * SQRT_TWO_PI * GELU_CUBIC) * sq)
    return value, slope


def meet_neighbours(stage, n_stages):
    barrier = pltpu.get_barrier_semaphore()

    @pl.when(stage > 0)
    def _():
        pl.semaphore_signal(barrier, inc=1, device_id={"stage": stage - 1}, device_id_type=MESH_ID)

    @pl.when(stage < n_stages - 1)
    def _():
        pl.semaphore_signal(barrier, inc=1, device_id={"stage": stage + 1}, device_id_type=MESH_ID)

    pl.semaphore_wait(barrier, jnp.minimum(stage, 1) + jnp.minimum(n_stages - 1 - stage, 1))


def back_kernel(n_stages, acts_ref, dy_ref, up32_ref, down32_ref, hid_ref, dpre_ref, gown_ref,
                up_ref, down_ref, a_buf, g_buf, h_buf, p_buf, dx_buf, acc_ref, pre_buf, dh_buf, stage_u, stage_v,
                u_sem, v_sem, a_sem, recv_sem, send_sem, gown_sem, h_sem, p_sem):
    stage = lax.axis_index("stage")
    last = n_stages - 1
    rows_all = g_buf.shape[0]
    hidden = up_ref.shape[1]
    n_chunks = rows_all // BACK_ROWS
    n_tiles = hidden // BACK_TILE

    def tile_copies(j):
        slot, cols = j % STAGING, pl.ds(j * BACK_TILE, BACK_TILE)
        return (pltpu.make_async_copy(up32_ref.at[0, :, cols], stage_u.at[slot], u_sem.at[slot]),
                pltpu.make_async_copy(down32_ref.at[0, cols, :], stage_v.at[slot], v_sem.at[slot]))

    def rows_of(c):
        return pl.ds(c * BACK_ROWS, BACK_ROWS) if isinstance(c, int) else span(c, BACK_ROWS)

    def a_copy(c):
        return pltpu.make_async_copy(acts_ref.at[0, rows_of(c), :], a_buf.at[rows_of(c), :], a_sem.at[c])

    def dy_copy(c):
        return pltpu.make_async_copy(dy_ref.at[rows_of(c), :], g_buf.at[rows_of(c), :], recv_sem.at[c])

    a_copy(0).start()

    @pl.when(stage == last)
    def _():
        dy_copy(0).start()

    for j in range(STAGING):
        for copy in tile_copies(j):
            copy.start()

    def load_rest(c, carry):
        a_copy(c).start()

        @pl.when(stage == last)
        def _():
            dy_copy(c).start()

        return carry

    def cast_tile(j):
        cols = pl.ds(j * BACK_TILE, BACK_TILE)
        for copy in tile_copies(j):
            copy.wait()
        up_ref[:, cols] = stage_u[j % STAGING].astype(BF16)
        down_ref[cols, :] = stage_v[j % STAGING].astype(BF16)
        if j + STAGING < n_tiles:
            for copy in tile_copies(j + STAGING):
                copy.start()
        if j == n_tiles - STAGING:
            lax.fori_loop(1, n_chunks, load_rest, 0)

    meet_neighbours(stage, n_stages)

    def send_of(c):
        return pltpu.make_async_remote_copy(
            src_ref=dx_buf.at[rows_of(c), :], dst_ref=g_buf.at[rows_of(c), :],
            send_sem=send_sem.at[c], recv_sem=recv_sem.at[c],
            device_id={"stage": stage - 1}, device_id_type=MESH_ID)

    def out_copies(c, slot):
        return (pltpu.make_async_copy(h_buf.at[slot], hid_ref.at[rows_of(c), :], h_sem.at[slot]),
                pltpu.make_async_copy(p_buf.at[slot], dpre_ref.at[rows_of(c), :], p_sem.at[slot]))

    def gown_copy(c):
        return pltpu.make_async_copy(g_buf.at[rows_of(c), :], gown_ref.at[rows_of(c), :], gown_sem.at[c])

    def chunk(c, carry, casting=False):
        slot = c % 2 if casting else lax.rem(c, 2)
        rows = rows_of(c)
        if not casting:
            @pl.when(c >= 2)
            def _():
                for copy in out_copies(c - 2, slot):
                    copy.wait()

        a_copy(c).wait()
        dy_copy(c).wait()
        gown_copy(c).start()

        def products(j):
            if casting:
                cast_tile(j)
            cols = pl.ds(j * BACK_TILE, BACK_TILE)
            pre_buf[j % 2] = dot_nn(a_buf[rows, :], up_ref[:, cols])
            dh_buf[j % 2] = dot_nt(g_buf[rows, :], down_ref[cols, :])

        def rest(j):
            cols = pl.ds(j * BACK_TILE, BACK_TILE)
            value, slope = gelu_pair(pre_buf[j % 2])
            h_buf[slot, :, cols] = value.astype(BF16)
            d_pre = (dh_buf[j % 2] * slope).astype(BF16)
            p_buf[slot, :, cols] = d_pre
            part = dot_nt(d_pre, up_ref[:, cols])
            if j == 0:
                acc_ref[...] = g_buf[rows, :].astype(F32) + part
            elif j < n_tiles - 1:
                acc_ref[...] += part
            else:
                dx_buf[rows, :] = (acc_ref[...] + part).astype(BF16)

        products(0)
        for j in range(n_tiles):
            if j + 1 < n_tiles:
                products(j + 1)
            rest(j)
        for copy in out_copies(c, slot):
            copy.start()

        @pl.when(stage > 0)
        def _():
            send_of(c).start()

        return carry

    @pl.when(stage == last)
    def _():
        chunk(0, 0, casting=True)

    @pl.when(stage < last)
    def _():
        for j in range(n_tiles):
            cast_tile(j)

    lax.fori_loop(stage // last, n_chunks, chunk, 0)

    for c in (n_chunks - 2, n_chunks - 1):
        for copy in out_copies(c, c % 2):
            copy.wait()

    def finish(c, carry):
        gown_copy(c).wait()

        @pl.when(stage > 0)
        def _():
            send_of(c).wait_send()

        return carry

    lax.fori_loop(0, n_chunks, finish, 0)


def backward(n_stages, acts, loss_grad, up32, down32):
    _, rows, width = acts.shape
    hidden = up32.shape[2]
    n_chunks = rows // BACK_ROWS
    wide = jax.ShapeDtypeStruct((rows, hidden), BF16)
    return pl.pallas_call(
        functools.partial(back_kernel, n_stages),
        name="backward",
        out_shape=(wide, wide, jax.ShapeDtypeStruct((rows, width), BF16)),
        in_specs=[ANY] * 4,
        out_specs=(ANY, ANY, ANY),
        scratch_shapes=[
            pltpu.VMEM((width, hidden), BF16),
            pltpu.VMEM((hidden, width), BF16),
            pltpu.VMEM((rows, width), BF16),
            pltpu.VMEM((rows, width), BF16),
            pltpu.VMEM((2, BACK_ROWS, hidden), BF16),
            pltpu.VMEM((2, BACK_ROWS, hidden), BF16),
            pltpu.VMEM((rows, width), BF16),
            pltpu.VMEM((BACK_ROWS, width), F32),
            pltpu.VMEM((2, BACK_ROWS, BACK_TILE), F32),
            pltpu.VMEM((2, BACK_ROWS, BACK_TILE), F32),
            pltpu.VMEM((STAGING, width, BACK_TILE), F32),
            pltpu.VMEM((STAGING, BACK_TILE, width), F32),
            pltpu.SemaphoreType.DMA((STAGING,)),
            pltpu.SemaphoreType.DMA((STAGING,)),
            pltpu.SemaphoreType.DMA((n_chunks,)),
            pltpu.SemaphoreType.DMA((n_chunks,)),
            pltpu.SemaphoreType.DMA((n_chunks,)),
            pltpu.SemaphoreType.DMA((n_chunks,)),
            pltpu.SemaphoreType.DMA((2,)),
            pltpu.SemaphoreType.DMA((2,)),
        ],
        compiler_params=pltpu.CompilerParams(collective_id=0, has_side_effects=True, vmem_limit_bytes=VMEM_LIMIT),
        cost_estimate=pl.CostEstimate(flops=6 * rows * width * hidden, bytes_accessed=6 * rows * hidden, transcendentals=rows * hidden),
    )(acts, loss_grad, up32, down32)


def wgrad_kernel(owner_ref, left_ref, right_ref, grad_ref, *refs):
    sum_refs, acc_ref = refs[:-1], refs[-1]
    lead = (0,) * (len(left_ref.shape) - 2)
    acc_ref[...] = grad_ref[0, 0]

    def step(k, carry):
        part = span(k, WGRAD_STEP)
        acc_ref[...] += dot_tn(left_ref[lead + (part, slice(None))], right_ref[part, :])
        return carry

    lax.fori_loop(0, right_ref.shape[0] // WGRAD_STEP, step, 0)
    for p, sum_ref in enumerate(sum_refs):
        def put(ref=sum_ref):
            ref[...] = acc_ref[...]

        if len(sum_refs) == 1:
            put()
        else:
            pl.when(pl.program_id(0) == p)(put)


def wgrad_units(kind, first, count, owner, left, right, grad):
    rows = right.shape[0]
    if kind == 0:
        half, piece = left.shape[2] // 2, right.shape[1] // PIECES
        shape = (half, piece)
        in_specs = [
            pl.BlockSpec((1, rows, half), lambda i, own: (0, 0, own[0])),
            pl.BlockSpec((rows, piece), lambda i, own: (0, first + i)),
            pl.BlockSpec((1, 1, half, piece), lambda i, own: (0, 0, own[0], first + i)),
        ]
    else:
        width, piece = right.shape[1], left.shape[1] // 2 // PIECES
        shape = (piece, width)
        in_specs = [
            pl.BlockSpec((rows, piece), lambda i, own: (0, own[0] * PIECES + first + i)),
            pl.BlockSpec((rows, width), lambda i, own: (0, 0)),
            pl.BlockSpec((1, 1, piece, width), lambda i, own: (0, 0, own[0] * PIECES + first + i, 0)),
        ]
    return pl.pallas_call(
        wgrad_kernel,
        out_shape=(jax.ShapeDtypeStruct(shape, F32),) * count,
        grid_spec=pltpu.PrefetchScalarGridSpec(
            num_scalar_prefetch=1,
            grid=(count,),
            in_specs=in_specs,
            out_specs=(pl.BlockSpec(shape, lambda i, own: (0, 0)),) * count,
            scratch_shapes=[pltpu.VMEM(shape, F32)],
        ),
        compiler_params=pltpu.CompilerParams(vmem_limit_bytes=VMEM_LIMIT),
        cost_estimate=pl.CostEstimate(flops=2 * rows * shape[0] * shape[1] * count, bytes_accessed=15 * 1024 * 1024, transcendentals=0),
    )(owner, left, right, grad)


def combine_kernel(scale, mine_ref, theirs_ref, sq_ref, gbar_ref, sq_out):
    n_rows, cols = mine_ref.shape

    def slab(i, fold):
        rows = span(i, SLAB)
        mean = (mine_ref[rows, :] + theirs_ref[rows, :]) * scale
        gbar_ref[rows, :] = mean
        part = jnp.sum((mean * mean).reshape(SLAB // 8, 8, cols), axis=0)
        for j in range(cols // 128):
            fold = fold + part[:, j * 128:(j + 1) * 128]
        return fold

    fold = lax.fori_loop(0, n_rows // SLAB, slab, jnp.zeros((8, 128), F32))
    first = pl.program_id(0) == 0

    @pl.when(first)
    def _():
        sq_out[...] = sq_ref[...] + fold

    @pl.when(jnp.logical_not(first))
    def _():
        sq_out[...] += fold


def combine(scale, mine, theirs, squares):
    rows, cols = mine.shape
    steps = 2
    spec = pl.BlockSpec((rows // steps, cols), lambda i: (i, 0))
    small = pl.BlockSpec((8, 128), lambda i: (0, 0))
    return pl.pallas_call(
        functools.partial(combine_kernel, scale),
        name="combine",
        out_shape=(jax.ShapeDtypeStruct((rows, cols), F32), jax.ShapeDtypeStruct((8, 128), F32)),
        grid=(steps,),
        in_specs=[spec, spec, small],
        out_specs=(spec, small),
        compiler_params=pltpu.CompilerParams(vmem_limit_bytes=VMEM_LIMIT),
        cost_estimate=pl.CostEstimate(flops=4 * rows * cols, bytes_accessed=12 * rows * cols, transcendentals=0),
    )(mine, theirs, squares)


def update_kernel(n_pieces, n_alias, owner_ref, lr_ref, clip_ref, w_ref, m_ref, v_ref, *rest):
    g_refs = rest[:n_pieces]
    w_out, m_out, v_out = rest[n_pieces + n_alias:n_pieces + n_alias + 3]
    b_outs = rest[n_pieces + n_alias + 3:]
    clip, lr = clip_ref[0:1, 0:1], lr_ref[0]

    def run(g_ref, b_out):
        def slab(i, carry):
            rows = span(i, SLAB)
            w = w_ref[0, rows, :]
            q = clip * g_ref[rows, :]
            m_new = BETA1 * m_ref[0, rows, :] + (1.0 - BETA1) * q
            v_new = BETA2 * v_ref[0, rows, :] + (1.0 - BETA2) * q * q
            m_hat = m_new * (1.0 / (1.0 - BETA1 ** ADAM_STEP))
            v_hat = v_new * (1.0 / (1.0 - BETA2 ** ADAM_STEP))
            w_new = w - lr * (m_hat / (jnp.sqrt(v_hat) + ADAM_EPS) + WEIGHT_DECAY * w)
            w_out[0, rows, :], m_out[0, rows, :], v_out[0, rows, :] = w_new, m_new, v_new
            if b_out is not None:
                b_out[rows, :] = w_new.astype(BF16)
            return carry

        lax.fori_loop(0, g_ref.shape[0] // SLAB, slab, 0)

    if n_pieces == 1:
        run(g_refs[0], b_outs[0] if b_outs else None)
    else:
        for p in range(n_pieces):
            pl.when(pl.program_id(0) == p)(functools.partial(run, g_refs[p], None))


def update_units(kind, first, owner, knobs, state, grads, chain, want_bf16):
    rows, cols = grads[0].shape
    n = len(grads)
    steps = 2 if n == 1 else 1
    block = rows // steps
    if kind == 0:
        spec = pl.BlockSpec((1, block, cols), lambda p, i, own: (0, own[0] * steps + i, first + p))
    else:
        spec = pl.BlockSpec((1, block, cols), lambda p, i, own: (0, (own[0] * PIECES + first + p) * steps + i, 0))

    def piece_spec(q):
        return pl.BlockSpec((block, cols), lambda p, i, own: (jnp.clip((p - q) * steps + i, 0, steps - 1), 0))

    full = jax.ShapeDtypeStruct(state[0].shape, F32)
    out_shape, out_specs = (full,) * 3, (spec,) * 3
    if want_bf16:
        out_shape += (jax.ShapeDtypeStruct((rows, cols), BF16),)
        out_specs += (piece_spec(0),)
    size = n * rows * cols
    return pl.pallas_call(
        functools.partial(update_kernel, n, len(chain)),
        out_shape=out_shape,
        grid_spec=pltpu.PrefetchScalarGridSpec(
            num_scalar_prefetch=1,
            grid=(n, steps),
            in_specs=[pl.BlockSpec(memory_space=pltpu.SMEM), pl.BlockSpec(memory_space=pltpu.VMEM)] + [spec] * 3 + [piece_spec(q) for q in range(n)] + [ANY] * len(chain),
            out_specs=out_specs,
        ),
        input_output_aliases={6 + n + i: i for i in range(len(chain))},
        compiler_params=pltpu.CompilerParams(vmem_limit_bytes=UPDATE_VMEM),
        cost_estimate=pl.CostEstimate(flops=30 * size, bytes_accessed=28 * size, transcendentals=size),
    )(owner, *knobs, *state, *grads, *chain)


def norm_kernel(n_stages, n_rep, sq_ref, max_ref, clip_ref, slots, send_sem, recv_sem):
    n_dev = n_stages * n_rep
    me = lax.axis_index("data") * n_stages + lax.axis_index("stage")
    slots[me] = sq_ref[...]

    def place(d):
        q = lax.rem(me + d, n_dev)
        return {"data": q // n_stages, "stage": lax.rem(q, n_stages)}

    barrier = pltpu.get_barrier_semaphore()
    for d in range(1, n_dev):
        pl.semaphore_signal(barrier, inc=1, device_id=place(d), device_id_type=MESH_ID)
    pl.semaphore_wait(barrier, n_dev - 1)
    copies = []
    for d in range(1, n_dev):
        copies.append(pltpu.make_async_remote_copy(
            src_ref=sq_ref, dst_ref=slots.at[me], send_sem=send_sem.at[d - 1], recv_sem=recv_sem.at[d - 1],
            device_id=place(d), device_id_type=MESH_ID))
        copies[-1].start()
    for copy in copies:
        copy.wait()
    square = slots[0]
    for q in range(1, n_dev):
        square = square + slots[q]
    total = jnp.full(clip_ref.shape, jnp.sum(square), F32)
    clip_ref[...] = jnp.minimum(1.0, max_ref[0] / (jnp.sqrt(total) + NORM_EPS))


def clip_factor(n_stages, n_rep, squares, max_norm):
    n_dev = n_stages * n_rep
    return pl.pallas_call(
        functools.partial(norm_kernel, n_stages, n_rep),
        name="clip_factor",
        out_shape=jax.ShapeDtypeStruct((8, 128), F32),
        in_specs=[pl.BlockSpec(memory_space=pltpu.VMEM), pl.BlockSpec(memory_space=pltpu.SMEM)],
        out_specs=pl.BlockSpec(memory_space=pltpu.VMEM),
        scratch_shapes=[
            pltpu.VMEM((n_dev, 8, 128), F32),
            pltpu.SemaphoreType.DMA((n_dev - 1,)),
            pltpu.SemaphoreType.DMA((n_dev - 1,)),
        ],
        compiler_params=pltpu.CompilerParams(collective_id=2, has_side_effects=True),
        cost_estimate=pl.CostEstimate(flops=40000000, bytes_accessed=4096, transcendentals=0),
    )(squares, max_norm)


def fwd_kernel(n_stages, n_rep, batch_ref, *refs):
    n_w = 2 * PIECES * n_rep
    w_refs = refs[:n_w]
    out_ref, up_ref, down_ref, x_buf, acc_ref, pre_buf, w_sem, recv_sem, send_sem = refs[n_w:]
    stage = lax.axis_index("stage")
    me = lax.axis_index("data")
    last = n_stages - 1
    n_chunks = x_buf.shape[0]
    hidden = up_ref.shape[1]
    n_tiles = hidden // FWD_TILE
    chunks_per_micro = n_chunks // batch_ref.shape[0]

    def batch_chunk(ref, c, lead):
        return ref.at[lead + (c // chunks_per_micro, span(lax.rem(c, chunks_per_micro), FWD_ROWS), slice(None))]

    copies = []
    for side in range(n_rep):
        owner = me if side == 0 else 1 - me
        for k in range(PIECES):
            u_src = w_refs[(2 * side) * PIECES + k]
            v_src = w_refs[(2 * side + 1) * PIECES + k]
            half_w, piece_n = u_src.shape
            piece_m = v_src.shape[0]
            u_dst = up_ref.at[span(owner, half_w), pl.ds(k * piece_n, piece_n)]
            v_dst = down_ref.at[span(owner * PIECES + k, piece_m), :]
            copies.append(pltpu.make_async_copy(u_src, u_dst, w_sem.at[len(copies)]))
            copies.append(pltpu.make_async_copy(v_src, v_dst, w_sem.at[len(copies)]))
    for copy in copies:
        copy.start()

    @pl.when(stage == 0)
    def _():
        def load(c, carry):
            pltpu.make_async_copy(batch_chunk(batch_ref, c, ()), x_buf.at[c], recv_sem.at[c]).start()
            return carry

        lax.fori_loop(0, n_chunks, load, 0)

    meet_neighbours(stage, n_stages)
    for copy in copies:
        copy.wait()

    def send_of(c):
        return pltpu.make_async_remote_copy(
            src_ref=batch_chunk(out_ref, c, (0,)), dst_ref=x_buf.at[c],
            send_sem=send_sem.at[c], recv_sem=recv_sem.at[c],
            device_id={"stage": stage + 1}, device_id_type=MESH_ID)

    def chunk(c, carry):
        pltpu.make_async_copy(batch_chunk(batch_ref, c, ()), x_buf.at[c], recv_sem.at[c]).wait()

        def products(j):
            pre_buf[j % 2] = dot_nn(x_buf[c], up_ref[:, pl.ds(j * FWD_TILE, FWD_TILE)])

        def rest(j):
            hid = gelu_value(pre_buf[j % 2]).astype(BF16)
            part = dot_nn(hid, down_ref[pl.ds(j * FWD_TILE, FWD_TILE), :])
            if j == 0:
                acc_ref[...] = x_buf[c].astype(F32) + part
            elif j < n_tiles - 1:
                acc_ref[...] += part
            else:
                out_ref[0, c // chunks_per_micro, span(lax.rem(c, chunks_per_micro), FWD_ROWS), :] = (acc_ref[...] + part).astype(BF16)

        products(0)
        for j in range(n_tiles):
            if j + 1 < n_tiles:
                products(j + 1)
            rest(j)

        @pl.when(stage < last)
        def _():
            send_of(c).start()

        return carry

    lax.fori_loop(0, n_chunks, chunk, 0)

    @pl.when(stage < last)
    def _():
        def finish(c, carry):
            send_of(c).wait_send()
            return carry

        lax.fori_loop(0, n_chunks, finish, 0)


def forward(n_stages, n_rep, next_batch, weights):
    n_micro, rows, width = next_batch.shape
    hidden = PIECES * weights[0].shape[1]
    n_chunks = n_micro * rows // FWD_ROWS
    return pl.pallas_call(
        functools.partial(fwd_kernel, n_stages, n_rep),
        name="forward",
        out_shape=pltpu.VMEM((1, n_micro, rows, width), BF16),
        in_specs=[ANY] * (1 + len(weights)),
        out_specs=pl.BlockSpec(memory_space=pltpu.VMEM),
        scratch_shapes=[
            pltpu.VMEM((width, hidden), BF16),
            pltpu.VMEM((hidden, width), BF16),
            pltpu.VMEM((n_chunks, FWD_ROWS, width), BF16),
            pltpu.VMEM((FWD_ROWS, width), F32),
            pltpu.VMEM((2, FWD_ROWS, FWD_TILE), F32),
            pltpu.SemaphoreType.DMA((len(weights),)),
            pltpu.SemaphoreType.DMA((n_chunks,)),
            pltpu.SemaphoreType.DMA((n_chunks,)),
        ],
        compiler_params=pltpu.CompilerParams(collective_id=1, has_side_effects=True, vmem_limit_bytes=FWD_VMEM),
        cost_estimate=pl.CostEstimate(flops=4 * n_micro * rows * width * hidden, bytes_accessed=6 * rows * hidden, transcendentals=n_micro * rows * hidden),
    )(next_batch, *weights)


def store_kernel(y_ref, out_ref, sem):
    copies = []
    for i in range(y_ref.shape[1]):
        copies.append(pltpu.make_async_copy(y_ref.at[0, i], out_ref.at[0, i], sem.at[i]))
        copies[-1].start()
    for copy in copies:
        copy.wait()


def store(y):
    return pl.pallas_call(
        store_kernel,
        name="store",
        out_shape=jax.ShapeDtypeStruct(y.shape, y.dtype),
        in_specs=[pl.BlockSpec(memory_space=pltpu.VMEM)],
        out_specs=ANY,
        scratch_shapes=[pltpu.SemaphoreType.DMA((y.shape[1],))],
        compiler_params=pltpu.CompilerParams(vmem_limit_bytes=STORE_VMEM),
        cost_estimate=pl.CostEstimate(flops=4000000, bytes_accessed=2 * y.size, transcendentals=0),
    )(y)


def part_of(parts):
    return next(iter(parts.values()))


def solution(mesh):
    n_stages = mesh.shape["stage"]
    n_rep = mesh.shape["data"]
    swap = [(i, n_rep - 1 - i) for i in range(n_rep)]

    def exchange(x):
        return lax.ppermute(x, "data", swap)

    def local_step(master_up, master_down, mom1_up, mom1_down, mom2_up, mom2_down, grad_up, grad_down, stage_acts, loss_grad, next_batch, learn_rate, max_norm):
        me = lax.axis_index("data")
        mine = jnp.reshape(me, (1,)).astype(jnp.int32)
        other = 1 - mine
        hid, d_pre, g_own = backward(n_stages, stage_acts, loss_grad, master_up, master_down)

        units = [(kind, first + i) for kind, first, count in GROUPS for i in range(count)]

        def wgrad(group, owner):
            kind, first, count = group
            operands = (stage_acts, d_pre, grad_up) if kind == 0 else (hid, g_own, grad_down)
            parts = wgrad_units(kind, first, count, owner, *operands)
            return {(kind, first + i): parts[i] for i in range(count)}

        arrived, whose = {}, other
        for group in GROUPS:
            parts = wgrad(group, whose)
            for unit, part in parts.items():
                arrived[unit] = exchange(part)
            whose = lax.optimization_barrier((other, part_of(parts)))[0]
        gbar, squares = {}, jnp.zeros((8, 128), F32)
        own_part = {}
        for kind in (0, 1):
            own_part.update(wgrad((kind, 0, PIECES), mine))
        for unit in units:
            gbar[unit], squares = combine(1.0 / n_rep, own_part[unit], arrived[unit], squares)
        clip = clip_factor(n_stages, n_rep, squares, jnp.reshape(max_norm, (1,)))
        knobs = (jnp.reshape(learn_rate, (1,)), clip)
        gbar_other = {}
        for unit in F32_FIRST:
            gbar_other[unit] = exchange(lax.optimization_barrier((gbar[unit], clip))[0])
        state = ((master_up, mom1_up, mom2_up), (master_down, mom1_down, mom2_down))
        chain = [(), ()]

        def update(unit, owner, grad):
            res = update_units(unit[0], unit[1], owner, knobs, state[unit[0]], [grad], chain[unit[0]], True)
            chain[unit[0]] = res[:3]
            return res[3]

        def update_group(kind, first, stop):
            grads = [gbar_other[kind, k] for k in range(first, stop)]
            chain[kind] = update_units(kind, first, other, knobs, state[kind], grads, chain[kind], False)

        late = [unit for unit in units if unit not in F32_FIRST]
        own_w, other_w = {}, {}
        for unit in late + list(F32_FIRST):
            own_w[unit] = update(unit, mine, gbar[unit])
            if unit in late:
                other_w[unit] = exchange(own_w[unit])
        for unit in late:
            ready = lax.optimization_barrier((gbar[unit], own_w[late[-1]]))[0]
            gbar_other[unit] = exchange(ready)
        for unit in F32_FIRST:
            other_w[unit] = update(unit, other, gbar_other[unit])
        weights = []
        for side in (own_w, other_w):
            for kind in (0, 1):
                weights += [side[kind, k] for k in range(PIECES)]
        stage_outs = store(forward(n_stages, n_rep, next_batch, weights))
        for kind, first, stop in TAIL:
            update_group(kind, first, stop)
        (new_up, new_m1_up, new_m2_up), (new_down, new_m1_down, new_m2_down) = chain
        return (new_up, new_down, new_m1_up, new_m1_down, new_m2_up, new_m2_down, stage_outs)

    w_spec = P("stage", None, None)
    g_spec = P("data", "stage", None, None)
    in_specs = (w_spec,) * 6 + (g_spec, g_spec, P("stage", "data", None), P("data", None), P(None, "data", None), P(), P())
    out_specs = (w_spec,) * 6 + (P("stage", None, "data", None),)
    return jax.shard_map(local_step, mesh=mesh, in_specs=in_specs, out_specs=out_specs, check_vma=False)
```

```python
import functools

import jax
import jax.numpy as jnp
from jax import lax
from jax.experimental import pallas as pl
from jax.experimental.pallas import tpu as pltpu
from jax.sharding import PartitionSpec as P


BETA1 = 0.9
BETA2 = 0.95
ADAM_EPS = 1e-8
WEIGHT_DECAY = 0.1
NORM_EPS = 1e-6
ADAM_STEP = 8
SQRT_TWO_PI = 0.7978845608028654
GELU_CUBIC = 0.044715

BACK_ROWS = 256
FWD_ROWS = 256
HEAD = 128
BACK_TILE = 512
FWD_TILE = 512
PIECES = 6
F32_FIRST = ((0, 0),)
GROUPS = ((0, 0, 1), (1, 0, 2), (0, 1, 2), (1, 2, 2), (0, 3, 2), (1, 4, 2), (0, 5, 1))
TAIL = ((1, 0, 4), (0, 1, 5), (1, 4, 6), (0, 5, 6))
STAGING = 3
WGRAD_STEP = 2048
SLAB = 16

BF16 = jnp.bfloat16
F32 = jnp.float32
MESH_ID = pl.DeviceIdType.MESH
ANY = pl.BlockSpec(memory_space=pl.ANY)
VMEM_LIMIT = 60 * 1024 * 1024
FWD_VMEM = 54000000
STORE_VMEM = 4 * 1024 * 1024
UPDATE_VMEM = 60 * 1024 * 1024


def dot_nn(left, right):
    return lax.dot_general(left, right, (((1,), (0,)), ((), ())), preferred_element_type=F32)


def dot_nt(left, right):
    return lax.dot_general(left, right, (((1,), (1,)), ((), ())), preferred_element_type=F32)


def dot_tn(left, right):
    return lax.dot_general(left, right, (((0,), (0,)), ((), ())), preferred_element_type=F32)


def span(index, size):
    if isinstance(index, int):
        return pl.ds(index * size, size)
    return pl.ds(pl.multiple_of(index * size, size), size)


def chunk_rows(c, total, size):
    if isinstance(c, int):
        return pl.ds(0 if c == 0 else total - HEAD, HEAD)
    return pl.ds(pl.multiple_of(HEAD + (c - 1) * size, HEAD), size)


def tanh_part(x, sq):
    return jnp.tanh(x * (SQRT_TWO_PI + (SQRT_TWO_PI * GELU_CUBIC) * sq))


def gelu_value(x):
    return x * (0.5 + 0.5 * tanh_part(x, x * x))


def gelu_pair(x):
    sq = x * x
    th = tanh_part(x, sq)
    half = 0.5 + 0.5 * th
    value = x * half
    slope = half + value * (1.0 - th) * (SQRT_TWO_PI + (3.0 * SQRT_TWO_PI * GELU_CUBIC) * sq)
    return value, slope


def meet_neighbours(stage, n_stages):
    barrier = pltpu.get_barrier_semaphore()

    @pl.when(stage > 0)
    def _():
        pl.semaphore_signal(barrier, inc=1, device_id={"stage": stage - 1}, device_id_type=MESH_ID)

    @pl.when(stage < n_stages - 1)
    def _():
        pl.semaphore_signal(barrier, inc=1, device_id={"stage": stage + 1}, device_id_type=MESH_ID)

    pl.semaphore_wait(barrier, jnp.minimum(stage, 1) + jnp.minimum(n_stages - 1 - stage, 1))


def back_kernel(n_stages, acts_ref, dy_ref, up32_ref, down32_ref, hid_ref, dpre_ref, gown_ref,
                up_ref, down_ref, a_buf, g_buf, h_buf, p_buf, dx_buf, acc_ref, pre_buf, dh_buf, stage_u, stage_v,
                u_sem, v_sem, a_sem, recv_sem, send_sem, gown_sem, h_sem, p_sem):
    stage = lax.axis_index("stage")
    last = n_stages - 1
    rows_all = g_buf.shape[0]
    hidden = up_ref.shape[1]
    n_chunks = (rows_all - 2 * HEAD) // BACK_ROWS + 2
    final = n_chunks - 1
    n_tiles = hidden // BACK_TILE

    def tile_copies(j):
        slot, cols = j % STAGING, pl.ds(j * BACK_TILE, BACK_TILE)
        return (pltpu.make_async_copy(up32_ref.at[0, :, cols], stage_u.at[slot], u_sem.at[slot]),
                pltpu.make_async_copy(down32_ref.at[0, cols, :], stage_v.at[slot], v_sem.at[slot]))

    def rows_of(c):
        return chunk_rows(c, rows_all, BACK_ROWS)

    def a_copy(c):
        return pltpu.make_async_copy(acts_ref.at[0, rows_of(c), :], a_buf.at[rows_of(c), :], a_sem.at[c])

    def dy_copy(c):
        return pltpu.make_async_copy(dy_ref.at[rows_of(c), :], g_buf.at[rows_of(c), :], recv_sem.at[c])

    def load(c):
        a_copy(c).start()

        @pl.when(stage == last)
        def _():
            dy_copy(c).start()

    load(0)
    for j in range(STAGING):
        for copy in tile_copies(j):
            copy.start()

    def load_rest(c, carry):
        load(c)
        return carry

    def cast_tile(j):
        cols = pl.ds(j * BACK_TILE, BACK_TILE)
        for copy in tile_copies(j):
            copy.wait()
        up_ref[:, cols] = stage_u[j % STAGING].astype(BF16)
        down_ref[cols, :] = stage_v[j % STAGING].astype(BF16)
        if j + STAGING < n_tiles:
            for copy in tile_copies(j + STAGING):
                copy.start()
        if j == n_tiles - STAGING:
            lax.fori_loop(1, final, load_rest, 0)
            load(final)

    meet_neighbours(stage, n_stages)

    def send_of(c):
        return pltpu.make_async_remote_copy(
            src_ref=dx_buf.at[rows_of(c), :], dst_ref=g_buf.at[rows_of(c), :],
            send_sem=send_sem.at[c], recv_sem=recv_sem.at[c],
            device_id={"stage": stage - 1}, device_id_type=MESH_ID)

    def slot_of(c):
        return 2 if isinstance(c, int) else lax.rem(c, 2)

    def out_copies(c):
        slot, size = slot_of(c), pl.ds(0, HEAD if isinstance(c, int) else BACK_ROWS)
        return (pltpu.make_async_copy(h_buf.at[slot, size, :], hid_ref.at[rows_of(c), :], h_sem.at[slot]),
                pltpu.make_async_copy(p_buf.at[slot, size, :], dpre_ref.at[rows_of(c), :], p_sem.at[slot]))

    def gown_copy(c):
        return pltpu.make_async_copy(g_buf.at[rows_of(c), :], gown_ref.at[rows_of(c), :], gown_sem.at[c])

    def chunk(c, carry, casting=False):
        slot, rows = slot_of(c), rows_of(c)
        size = pl.ds(0, HEAD if isinstance(c, int) else BACK_ROWS)
        if not isinstance(c, int):
            @pl.when(c >= 3)
            def _():
                for copy in out_copies(c - 2):
                    copy.wait()
        elif c == final:
            for copy in out_copies(0):
                copy.wait()

        a_copy(c).wait()
        dy_copy(c).wait()
        gown_copy(c).start()

        def products(j):
            if casting:
                cast_tile(j)
            cols = pl.ds(j * BACK_TILE, BACK_TILE)
            pre_buf[j % 2, size, :] = dot_nn(a_buf[rows, :], up_ref[:, cols])
            dh_buf[j % 2, size, :] = dot_nt(g_buf[rows, :], down_ref[cols, :])

        def rest(j):
            cols = pl.ds(j * BACK_TILE, BACK_TILE)
            value, slope = gelu_pair(pre_buf[j % 2, size, :])
            h_buf[slot, size, cols] = value.astype(BF16)
            d_pre = (dh_buf[j % 2, size, :] * slope).astype(BF16)
            p_buf[slot, size, cols] = d_pre
            part = dot_nt(d_pre, up_ref[:, cols])
            if j == 0:
                acc_ref[size, :] = g_buf[rows, :].astype(F32) + part
            elif j < n_tiles - 1:
                acc_ref[size, :] += part
            else:
                dx_buf[rows, :] = (acc_ref[size, :] + part).astype(BF16)

        products(0)
        for j in range(n_tiles):
            if j + 1 < n_tiles:
                products(j + 1)
            rest(j)
        for copy in out_copies(c):
            copy.start()

        @pl.when(stage > 0)
        def _():
            send_of(c).start()

        return carry

    @pl.when(stage == last)
    def _():
        chunk(0, 0, casting=True)

    @pl.when(stage < last)
    def _():
        for j in range(n_tiles):
            cast_tile(j)
        chunk(0, 0)

    lax.fori_loop(1, final, chunk, 0)
    chunk(final, 0)

    def finish(c, carry):
        gown_copy(c).wait()

        @pl.when(stage > 0)
        def _():
            send_of(c).wait_send()

        return carry

    for c in (final - 2, final - 1):
        for copy in out_copies(jnp.int32(c)):
            copy.wait()
    for copy in out_copies(final):
        copy.wait()
    finish(0, 0)
    lax.fori_loop(1, final, finish, 0)
    finish(final, 0)


def backward(n_stages, acts, loss_grad, up32, down32):
    _, rows, width = acts.shape
    hidden = up32.shape[2]
    n_chunks = (rows - 2 * HEAD) // BACK_ROWS + 2
    wide = jax.ShapeDtypeStruct((rows, hidden), BF16)
    return pl.pallas_call(
        functools.partial(back_kernel, n_stages),
        name="backward",
        out_shape=(wide, wide, jax.ShapeDtypeStruct((rows, width), BF16)),
        in_specs=[ANY] * 4,
        out_specs=(ANY, ANY, ANY),
        scratch_shapes=[
            pltpu.VMEM((width, hidden), BF16),
            pltpu.VMEM((hidden, width), BF16),
            pltpu.VMEM((rows, width), BF16),
            pltpu.VMEM((rows, width), BF16),
            pltpu.VMEM((3, BACK_ROWS, hidden), BF16),
            pltpu.VMEM((3, BACK_ROWS, hidden), BF16),
            pltpu.VMEM((rows, width), BF16),
            pltpu.VMEM((BACK_ROWS, width), F32),
            pltpu.VMEM((2, BACK_ROWS, BACK_TILE), F32),
            pltpu.VMEM((2, BACK_ROWS, BACK_TILE), F32),
            pltpu.VMEM((STAGING, width, BACK_TILE), F32),
            pltpu.VMEM((STAGING, BACK_TILE, width), F32),
            pltpu.SemaphoreType.DMA((STAGING,)),
            pltpu.SemaphoreType.DMA((STAGING,)),
            pltpu.SemaphoreType.DMA((n_chunks,)),
            pltpu.SemaphoreType.DMA((n_chunks,)),
            pltpu.SemaphoreType.DMA((n_chunks,)),
            pltpu.SemaphoreType.DMA((n_chunks,)),
            pltpu.SemaphoreType.DMA((3,)),
            pltpu.SemaphoreType.DMA((3,)),
        ],
        compiler_params=pltpu.CompilerParams(collective_id=0, has_side_effects=True, vmem_limit_bytes=VMEM_LIMIT),
        cost_estimate=pl.CostEstimate(flops=6 * rows * width * hidden, bytes_accessed=6 * rows * hidden, transcendentals=rows * hidden),
    )(acts, loss_grad, up32, down32)


def wgrad_kernel(owner_ref, left_ref, right_ref, grad_ref, *refs):
    sum_refs, acc_ref = refs[:-1], refs[-1]
    lead = (0,) * (len(left_ref.shape) - 2)
    acc_ref[...] = grad_ref[0, 0]

    def step(k, carry):
        part = span(k, WGRAD_STEP)
        acc_ref[...] += dot_tn(left_ref[lead + (part, slice(None))], right_ref[part, :])
        return carry

    lax.fori_loop(0, right_ref.shape[0] // WGRAD_STEP, step, 0)
    for p, sum_ref in enumerate(sum_refs):
        def put(ref=sum_ref):
            ref[...] = acc_ref[...]

        if len(sum_refs) == 1:
            put()
        else:
            pl.when(pl.program_id(0) == p)(put)


def wgrad_units(kind, first, count, owner, left, right, grad):
    rows = right.shape[0]
    if kind == 0:
        half, piece = left.shape[2] // 2, right.shape[1] // PIECES
        shape = (half, piece)
        in_specs = [
            pl.BlockSpec((1, rows, half), lambda i, own: (0, 0, own[0])),
            pl.BlockSpec((rows, piece), lambda i, own: (0, first + i)),
            pl.BlockSpec((1, 1, half, piece), lambda i, own: (0, 0, own[0], first + i)),
        ]
    else:
        width, piece = right.shape[1], left.shape[1] // 2 // PIECES
        shape = (piece, width)
        in_specs = [
            pl.BlockSpec((rows, piece), lambda i, own: (0, own[0] * PIECES + first + i)),
            pl.BlockSpec((rows, width), lambda i, own: (0, 0)),
            pl.BlockSpec((1, 1, piece, width), lambda i, own: (0, 0, own[0] * PIECES + first + i, 0)),
        ]
    return pl.pallas_call(
        wgrad_kernel,
        out_shape=(jax.ShapeDtypeStruct(shape, F32),) * count,
        grid_spec=pltpu.PrefetchScalarGridSpec(
            num_scalar_prefetch=1,
            grid=(count,),
            in_specs=in_specs,
            out_specs=(pl.BlockSpec(shape, lambda i, own: (0, 0)),) * count,
            scratch_shapes=[pltpu.VMEM(shape, F32)],
        ),
        compiler_params=pltpu.CompilerParams(vmem_limit_bytes=VMEM_LIMIT),
        cost_estimate=pl.CostEstimate(flops=2 * rows * shape[0] * shape[1] * count, bytes_accessed=15 * 1024 * 1024, transcendentals=0),
    )(owner, left, right, grad)


def combine_kernel(scale, mine_ref, theirs_ref, sq_ref, gbar_ref, sq_out):
    n_rows, cols = mine_ref.shape

    def slab(i, fold):
        rows = span(i, SLAB)
        mean = (mine_ref[rows, :] + theirs_ref[rows, :]) * scale
        gbar_ref[rows, :] = mean
        part = jnp.sum((mean * mean).reshape(SLAB // 8, 8, cols), axis=0)
        for j in range(cols // 128):
            fold = fold + part[:, j * 128:(j + 1) * 128]
        return fold

    fold = lax.fori_loop(0, n_rows // SLAB, slab, jnp.zeros((8, 128), F32))
    first = pl.program_id(0) == 0

    @pl.when(first)
    def _():
        sq_out[...] = sq_ref[...] + fold

    @pl.when(jnp.logical_not(first))
    def _():
        sq_out[...] += fold


def combine(scale, mine, theirs, squares):
    rows, cols = mine.shape
    steps = 2
    spec = pl.BlockSpec((rows // steps, cols), lambda i: (i, 0))
    small = pl.BlockSpec((8, 128), lambda i: (0, 0))
    return pl.pallas_call(
        functools.partial(combine_kernel, scale),
        name="combine",
        out_shape=(jax.ShapeDtypeStruct((rows, cols), F32), jax.ShapeDtypeStruct((8, 128), F32)),
        grid=(steps,),
        in_specs=[spec, spec, small],
        out_specs=(spec, small),
        compiler_params=pltpu.CompilerParams(vmem_limit_bytes=VMEM_LIMIT),
        cost_estimate=pl.CostEstimate(flops=4 * rows * cols, bytes_accessed=12 * rows * cols, transcendentals=0),
    )(mine, theirs, squares)


def update_kernel(n_pieces, n_alias, want_bf16, owner_ref, lr_ref, clip_ref, w_ref, m_ref, v_ref, *rest):
    g_refs = rest[:n_pieces]
    w_out, m_out, v_out, last_out = rest[n_pieces + n_alias:]
    clip, lr = clip_ref[0:1, 0:1], lr_ref[0]

    def run(g_ref, b_out):
        def slab(i, carry):
            rows = span(i, SLAB)
            w = w_ref[0, rows, :]
            q = clip * g_ref[rows, :]
            m_new = BETA1 * m_ref[0, rows, :] + (1.0 - BETA1) * q
            v_new = BETA2 * v_ref[0, rows, :] + (1.0 - BETA2) * q * q
            m_hat = m_new * (1.0 / (1.0 - BETA1 ** ADAM_STEP))
            v_hat = v_new * (1.0 / (1.0 - BETA2 ** ADAM_STEP))
            w_new = w - lr * (m_hat / (jnp.sqrt(v_hat) + ADAM_EPS) + WEIGHT_DECAY * w)
            w_out[0, rows, :], m_out[0, rows, :], v_out[0, rows, :] = w_new, m_new, v_new
            if b_out is not None:
                b_out[rows, :] = w_new.astype(BF16)
            return carry

        lax.fori_loop(0, g_ref.shape[0] // SLAB, slab, 0)

    if n_pieces == 1:
        run(g_refs[0], last_out if want_bf16 else None)
    else:
        for p in range(n_pieces):
            pl.when(pl.program_id(0) == p)(functools.partial(run, g_refs[p], None))
    if not want_bf16:
        last_out[...] = clip_ref[...]


def update_units(kind, first, owner, knobs, state, grads, chain, want_bf16):
    rows, cols = grads[0].shape
    n = len(grads)
    steps = 2 if n == 1 else 1
    block = rows // steps
    if kind == 0:
        spec = pl.BlockSpec((1, block, cols), lambda p, i, own: (0, own[0] * steps + i, first + p))
    else:
        spec = pl.BlockSpec((1, block, cols), lambda p, i, own: (0, (own[0] * PIECES + first + p) * steps + i, 0))

    def piece_spec(q):
        return pl.BlockSpec((block, cols), lambda p, i, own: (jnp.clip((p - q) * steps + i, 0, steps - 1), 0))

    full = jax.ShapeDtypeStruct(state[0].shape, F32)
    out_shape, out_specs = (full,) * 3, (spec,) * 3
    if want_bf16:
        out_shape += (jax.ShapeDtypeStruct((rows, cols), BF16),)
        out_specs += (piece_spec(0),)
    else:
        out_shape += (jax.ShapeDtypeStruct((8, 128), F32),)
        out_specs += (pl.BlockSpec((8, 128), lambda p, i, own: (0, 0)),)
    size = n * rows * cols
    return pl.pallas_call(
        functools.partial(update_kernel, n, len(chain), want_bf16),
        out_shape=out_shape,
        grid_spec=pltpu.PrefetchScalarGridSpec(
            num_scalar_prefetch=1,
            grid=(n, steps),
            in_specs=[pl.BlockSpec(memory_space=pltpu.SMEM), pl.BlockSpec(memory_space=pltpu.VMEM)] + [spec] * 3 + [piece_spec(q) for q in range(n)] + [ANY] * len(chain),
            out_specs=out_specs,
        ),
        input_output_aliases={6 + n + i: i for i in range(len(chain))},
        compiler_params=pltpu.CompilerParams(vmem_limit_bytes=UPDATE_VMEM),
        cost_estimate=pl.CostEstimate(flops=30 * size, bytes_accessed=28 * size, transcendentals=size),
    )(owner, *knobs, *state, *grads, *chain)


def norm_kernel(n_stages, n_rep, sq_ref, max_ref, clip_ref, slots, send_sem, recv_sem):
    n_dev = n_stages * n_rep
    me = lax.axis_index("data") * n_stages + lax.axis_index("stage")
    slots[me] = sq_ref[...]

    def place(d):
        q = lax.rem(me + d, n_dev)
        return {"data": q // n_stages, "stage": lax.rem(q, n_stages)}

    barrier = pltpu.get_barrier_semaphore()
    for d in range(1, n_dev):
        pl.semaphore_signal(barrier, inc=1, device_id=place(d), device_id_type=MESH_ID)
    pl.semaphore_wait(barrier, n_dev - 1)
    copies = []
    for d in range(1, n_dev):
        copies.append(pltpu.make_async_remote_copy(
            src_ref=sq_ref, dst_ref=slots.at[me], send_sem=send_sem.at[d - 1], recv_sem=recv_sem.at[d - 1],
            device_id=place(d), device_id_type=MESH_ID))
        copies[-1].start()
    for copy in copies:
        copy.wait()
    square = slots[0]
    for q in range(1, n_dev):
        square = square + slots[q]
    total = jnp.full(clip_ref.shape, jnp.sum(square), F32)
    clip_ref[...] = jnp.minimum(1.0, max_ref[0] / (jnp.sqrt(total) + NORM_EPS))


def clip_factor(n_stages, n_rep, squares, max_norm):
    n_dev = n_stages * n_rep
    return pl.pallas_call(
        functools.partial(norm_kernel, n_stages, n_rep),
        name="clip_factor",
        out_shape=jax.ShapeDtypeStruct((8, 128), F32),
        in_specs=[pl.BlockSpec(memory_space=pltpu.VMEM), pl.BlockSpec(memory_space=pltpu.SMEM)],
        out_specs=pl.BlockSpec(memory_space=pltpu.VMEM),
        scratch_shapes=[
            pltpu.VMEM((n_dev, 8, 128), F32),
            pltpu.SemaphoreType.DMA((n_dev - 1,)),
            pltpu.SemaphoreType.DMA((n_dev - 1,)),
        ],
        compiler_params=pltpu.CompilerParams(collective_id=2, has_side_effects=True),
        cost_estimate=pl.CostEstimate(flops=40000000, bytes_accessed=4096, transcendentals=0),
    )(squares, max_norm)


def fwd_kernel(n_stages, n_rep, batch_ref, *refs):
    n_w = 2 * PIECES * n_rep
    w_refs = refs[:n_w]
    out_ref, up_ref, down_ref, x_buf, acc_ref, pre_buf, w_sem, recv_sem, send_sem = refs[n_w:]
    stage = lax.axis_index("stage")
    me = lax.axis_index("data")
    last = n_stages - 1
    total = x_buf.shape[0]
    hidden = up_ref.shape[1]
    n_tiles = hidden // FWD_TILE
    n_chunks = (total - 2 * HEAD) // FWD_ROWS + 2
    final = n_chunks - 1

    def rows_of(c):
        return chunk_rows(c, total, FWD_ROWS)

    def batch_copy(c):
        return pltpu.make_async_copy(batch_ref.at[rows_of(c), :], x_buf.at[rows_of(c), :], recv_sem.at[c])

    copies = []
    for side in range(n_rep):
        owner = me if side == 0 else 1 - me
        for k in range(PIECES):
            u_src = w_refs[(2 * side) * PIECES + k]
            v_src = w_refs[(2 * side + 1) * PIECES + k]
            half_w, piece_n = u_src.shape
            piece_m = v_src.shape[0]
            u_dst = up_ref.at[span(owner, half_w), pl.ds(k * piece_n, piece_n)]
            v_dst = down_ref.at[span(owner * PIECES + k, piece_m), :]
            copies.append(pltpu.make_async_copy(u_src, u_dst, w_sem.at[len(copies)]))
            copies.append(pltpu.make_async_copy(v_src, v_dst, w_sem.at[len(copies)]))
    for copy in copies:
        copy.start()

    @pl.when(stage == 0)
    def _():
        def load(c, carry):
            batch_copy(c).start()
            return carry

        load(0, 0)
        lax.fori_loop(1, final, load, 0)
        load(final, 0)

    meet_neighbours(stage, n_stages)
    for copy in copies:
        copy.wait()

    def send_of(c):
        return pltpu.make_async_remote_copy(
            src_ref=out_ref.at[rows_of(c), :], dst_ref=x_buf.at[rows_of(c), :],
            send_sem=send_sem.at[c], recv_sem=recv_sem.at[c],
            device_id={"stage": stage + 1}, device_id_type=MESH_ID)

    def chunk(c, carry):
        rows = rows_of(c)
        size = pl.ds(0, HEAD if isinstance(c, int) else FWD_ROWS)
        batch_copy(c).wait()

        def products(j):
            pre_buf[j % 2, size, :] = dot_nn(x_buf[rows, :], up_ref[:, pl.ds(j * FWD_TILE, FWD_TILE)])

        def rest(j):
            hid = gelu_value(pre_buf[j % 2, size, :]).astype(BF16)
            part = dot_nn(hid, down_ref[pl.ds(j * FWD_TILE, FWD_TILE), :])
            if j == 0:
                acc_ref[size, :] = x_buf[rows, :].astype(F32) + part
            elif j < n_tiles - 1:
                acc_ref[size, :] += part
            else:
                out_ref[rows, :] = (acc_ref[size, :] + part).astype(BF16)

        products(0)
        for j in range(n_tiles):
            if j + 1 < n_tiles:
                products(j + 1)
            rest(j)

        @pl.when(stage < last)
        def _():
            send_of(c).start()

        return carry

    chunk(0, 0)
    lax.fori_loop(1, final, chunk, 0)
    chunk(final, 0)

    @pl.when(stage < last)
    def _():
        def finish(c, carry):
            send_of(c).wait_send()
            return carry

        finish(0, 0)
        lax.fori_loop(1, final, finish, 0)
        finish(final, 0)


def forward(n_stages, n_rep, next_batch, weights):
    n_micro, rows, width = next_batch.shape
    total = n_micro * rows
    hidden = PIECES * weights[0].shape[1]
    n_chunks = (total - 2 * HEAD) // FWD_ROWS + 2
    return pl.pallas_call(
        functools.partial(fwd_kernel, n_stages, n_rep),
        name="forward",
        out_shape=pltpu.VMEM((total, width), BF16),
        in_specs=[ANY] * (1 + len(weights)),
        out_specs=pl.BlockSpec(memory_space=pltpu.VMEM),
        scratch_shapes=[
            pltpu.VMEM((width, hidden), BF16),
            pltpu.VMEM((hidden, width), BF16),
            pltpu.VMEM((total, width), BF16),
            pltpu.VMEM((FWD_ROWS, width), F32),
            pltpu.VMEM((2, FWD_ROWS, FWD_TILE), F32),
            pltpu.SemaphoreType.DMA((len(weights),)),
            pltpu.SemaphoreType.DMA((n_chunks,)),
            pltpu.SemaphoreType.DMA((n_chunks,)),
        ],
        compiler_params=pltpu.CompilerParams(collective_id=1, has_side_effects=True, vmem_limit_bytes=FWD_VMEM),
        cost_estimate=pl.CostEstimate(flops=4 * n_micro * rows * width * hidden, bytes_accessed=6 * rows * hidden, transcendentals=n_micro * rows * hidden),
    )(next_batch.reshape(total, width), *weights)


def store_kernel(y_ref, out_ref, sem):
    half = y_ref.shape[0] // 2
    copies = [pltpu.make_async_copy(y_ref.at[span(i, half), :], out_ref.at[span(i, half), :], sem.at[i]) for i in range(2)]
    for copy in copies:
        copy.start()
    for copy in copies:
        copy.wait()


def store(y):
    return pl.pallas_call(
        store_kernel,
        name="store",
        out_shape=jax.ShapeDtypeStruct(y.shape, y.dtype),
        in_specs=[pl.BlockSpec(memory_space=pltpu.VMEM)],
        out_specs=ANY,
        scratch_shapes=[pltpu.SemaphoreType.DMA((2,))],
        compiler_params=pltpu.CompilerParams(vmem_limit_bytes=STORE_VMEM),
        cost_estimate=pl.CostEstimate(flops=4000000, bytes_accessed=2 * y.size, transcendentals=0),
    )(y)


def part_of(parts):
    return next(iter(parts.values()))


def solution(mesh):
    n_stages = mesh.shape["stage"]
    n_rep = mesh.shape["data"]
    swap = [(i, n_rep - 1 - i) for i in range(n_rep)]

    def exchange(x):
        return lax.ppermute(x, "data", swap)

    def local_step(master_up, master_down, mom1_up, mom1_down, mom2_up, mom2_down, grad_up, grad_down, stage_acts, loss_grad, next_batch, learn_rate, max_norm):
        me = lax.axis_index("data")
        mine = jnp.reshape(me, (1,)).astype(jnp.int32)
        other = 1 - mine
        hid, d_pre, g_own = backward(n_stages, stage_acts, loss_grad, master_up, master_down)

        units = [(kind, first + i) for kind, first, count in GROUPS for i in range(count)]

        def wgrad(group, owner):
            kind, first, count = group
            operands = (stage_acts, d_pre, grad_up) if kind == 0 else (hid, g_own, grad_down)
            parts = wgrad_units(kind, first, count, owner, *operands)
            return {(kind, first + i): parts[i] for i in range(count)}

        arrived, whose = {}, other
        for group in GROUPS:
            parts = wgrad(group, whose)
            for unit, part in parts.items():
                arrived[unit] = exchange(part)
            whose = lax.optimization_barrier((other, part_of(parts)))[0]
        gbar, squares = {}, jnp.zeros((8, 128), F32)
        own_part = {}
        for kind in (0, 1):
            own_part.update(wgrad((kind, 0, PIECES), mine))
        for unit in units:
            gbar[unit], squares = combine(1.0 / n_rep, own_part[unit], arrived[unit], squares)
        clip = clip_factor(n_stages, n_rep, squares, jnp.reshape(max_norm, (1,)))
        knobs = (jnp.reshape(learn_rate, (1,)), clip)
        gbar_other = {}
        for unit in F32_FIRST:
            gbar_other[unit] = exchange(lax.optimization_barrier((gbar[unit], clip))[0])
        state = ((master_up, mom1_up, mom2_up), (master_down, mom1_down, mom2_down))
        chain = [(), ()]

        def update(unit, owner, grad):
            res = update_units(unit[0], unit[1], owner, knobs, state[unit[0]], [grad], chain[unit[0]], True)
            chain[unit[0]] = res[:3]
            return res[3]

        def update_group(kind, first, stop, clip):
            grads = [gbar_other[kind, k] for k in range(first, stop)]
            res = update_units(kind, first, other, (knobs[0], clip), state[kind], grads, chain[kind], False)
            chain[kind] = res[:3]
            return res[3]

        late = [unit for unit in units if unit not in F32_FIRST]
        own_w, other_w = {}, {}
        for unit in late + list(F32_FIRST):
            own_w[unit] = update(unit, mine, gbar[unit])
            if unit in late:
                other_w[unit] = exchange(own_w[unit])
        for unit in late:
            ready = lax.optimization_barrier((gbar[unit], own_w[late[-1]]))[0]
            gbar_other[unit] = exchange(ready)
        for unit in F32_FIRST:
            other_w[unit] = update(unit, other, gbar_other[unit])
        weights = []
        for side in (own_w, other_w):
            for kind in (0, 1):
                weights += [side[kind, k] for k in range(PIECES)]
        stage_outs = store(forward(n_stages, n_rep, next_batch, weights)).reshape((1,) + next_batch.shape)
        for kind, first, stop in TAIL:
            clip = update_group(kind, first, stop, clip)
        (new_up, new_m1_up, new_m2_up), (new_down, new_m1_down, new_m2_down) = chain
        return (new_up, new_down, new_m1_up, new_m1_down, new_m2_up, new_m2_down, stage_outs)

    w_spec = P("stage", None, None)
    g_spec = P("data", "stage", None, None)
    in_specs = (w_spec,) * 6 + (g_spec, g_spec, P("stage", "data", None), P("data", None), P(None, "data", None), P(), P())
    out_specs = (w_spec,) * 6 + (P("stage", None, "data", None),)
    return jax.shard_map(local_step, mesh=mesh, in_specs=in_specs, out_specs=out_specs, check_vma=False)
```

```python
import functools

import jax
import jax.numpy as jnp
from jax import lax
from jax.experimental import pallas as pl
from jax.experimental.pallas import tpu as pltpu
from jax.sharding import PartitionSpec as P


BETA1 = 0.9
BETA2 = 0.95
ADAM_EPS = 1e-8
WEIGHT_DECAY = 0.1
NORM_EPS = 1e-6
ADAM_STEP = 8
SQRT_TWO_PI = 0.7978845608028654
GELU_CUBIC = 0.044715

BACK_ROWS = 256
FWD_ROWS = 256
HEAD = 128
BACK_TILE = 512
FWD_TILE = 512
PIECES = 6
F32_FIRST = ((0, 0),)
GROUPS = ((0, 0, 1), (1, 0, 2), (0, 1, 2), (1, 2, 2), (0, 3, 2), (1, 4, 2), (0, 5, 1))
TAIL = ((0, 1, 5), (1, 0, 6), (0, 5, 6))
STAGING = 3
WGRAD_STEP = 1024
SLAB = 16

BF16 = jnp.bfloat16
F32 = jnp.float32
MESH_ID = pl.DeviceIdType.MESH
ANY = pl.BlockSpec(memory_space=pl.ANY)
VMEM_LIMIT = 60 * 1024 * 1024
FWD_VMEM = 54000000
STORE_VMEM = 4 * 1024 * 1024
UPDATE_VMEM = 60 * 1024 * 1024


def dot_nn(left, right):
    return lax.dot_general(left, right, (((1,), (0,)), ((), ())), preferred_element_type=F32)


def dot_nt(left, right):
    return lax.dot_general(left, right, (((1,), (1,)), ((), ())), preferred_element_type=F32)


def dot_tn(left, right):
    return lax.dot_general(left, right, (((0,), (0,)), ((), ())), preferred_element_type=F32)


def span(index, size):
    if isinstance(index, int):
        return pl.ds(index * size, size)
    return pl.ds(pl.multiple_of(index * size, size), size)


def chunk_rows(c, total, size):
    if isinstance(c, int):
        return pl.ds(0 if c == 0 else total - HEAD, HEAD)
    return pl.ds(pl.multiple_of(HEAD + (c - 1) * size, HEAD), size)


def tanh_part(x, sq):
    return jnp.tanh(x * (SQRT_TWO_PI + (SQRT_TWO_PI * GELU_CUBIC) * sq))


def gelu_value(x):
    return x * (0.5 + 0.5 * tanh_part(x, x * x))


def gelu_pair(x):
    sq = x * x
    th = tanh_part(x, sq)
    half = 0.5 + 0.5 * th
    value = x * half
    slope = half + value * (1.0 - th) * (SQRT_TWO_PI + (3.0 * SQRT_TWO_PI * GELU_CUBIC) * sq)
    return value, slope


def meet_neighbours(stage, n_stages):
    barrier = pltpu.get_barrier_semaphore()

    @pl.when(stage > 0)
    def _():
        pl.semaphore_signal(barrier, inc=1, device_id={"stage": stage - 1}, device_id_type=MESH_ID)

    @pl.when(stage < n_stages - 1)
    def _():
        pl.semaphore_signal(barrier, inc=1, device_id={"stage": stage + 1}, device_id_type=MESH_ID)

    pl.semaphore_wait(barrier, jnp.minimum(stage, 1) + jnp.minimum(n_stages - 1 - stage, 1))


def back_kernel(n_stages, acts_ref, dy_ref, up32_ref, down32_ref, hid_ref, dpre_ref, gown_ref,
                up_ref, down_ref, a_buf, g_buf, h_buf, p_buf, dx_buf, acc_ref, pre_buf, dh_buf, stage_u, stage_v,
                u_sem, v_sem, a_sem, recv_sem, send_sem, gown_sem, h_sem, p_sem):
    stage = lax.axis_index("stage")
    last = n_stages - 1
    rows_all = g_buf.shape[0]
    hidden = up_ref.shape[1]
    n_chunks = rows_all // BACK_ROWS
    n_tiles = hidden // BACK_TILE

    def tile_copies(j):
        slot, cols = j % STAGING, pl.ds(j * BACK_TILE, BACK_TILE)
        return (pltpu.make_async_copy(up32_ref.at[0, :, cols], stage_u.at[slot], u_sem.at[slot]),
                pltpu.make_async_copy(down32_ref.at[0, cols, :], stage_v.at[slot], v_sem.at[slot]))

    def rows_of(c):
        return pl.ds(c * BACK_ROWS, BACK_ROWS) if isinstance(c, int) else span(c, BACK_ROWS)

    def a_copy(c):
        return pltpu.make_async_copy(acts_ref.at[0, rows_of(c), :], a_buf.at[rows_of(c), :], a_sem.at[c])

    def dy_copy(c):
        return pltpu.make_async_copy(dy_ref.at[rows_of(c), :], g_buf.at[rows_of(c), :], recv_sem.at[c])

    a_copy(0).start()

    @pl.when(stage == last)
    def _():
        dy_copy(0).start()

    for j in range(STAGING):
        for copy in tile_copies(j):
            copy.start()

    def load_rest(c, carry):
        a_copy(c).start()

        @pl.when(stage == last)
        def _():
            dy_copy(c).start()

        return carry

    def cast_tile(j):
        cols = pl.ds(j * BACK_TILE, BACK_TILE)
        for copy in tile_copies(j):
            copy.wait()
        up_ref[:, cols] = stage_u[j % STAGING].astype(BF16)
        down_ref[cols, :] = stage_v[j % STAGING].astype(BF16)
        if j + STAGING < n_tiles:
            for copy in tile_copies(j + STAGING):
                copy.start()
        if j == n_tiles - STAGING:
            lax.fori_loop(1, n_chunks, load_rest, 0)

    meet_neighbours(stage, n_stages)

    def send_of(c):
        return pltpu.make_async_remote_copy(
            src_ref=dx_buf.at[rows_of(c), :], dst_ref=g_buf.at[rows_of(c), :],
            send_sem=send_sem.at[c], recv_sem=recv_sem.at[c],
            device_id={"stage": stage - 1}, device_id_type=MESH_ID)

    def out_copies(c, slot):
        return (pltpu.make_async_copy(h_buf.at[slot], hid_ref.at[rows_of(c), :], h_sem.at[slot]),
                pltpu.make_async_copy(p_buf.at[slot], dpre_ref.at[rows_of(c), :], p_sem.at[slot]))

    def gown_copy(c):
        return pltpu.make_async_copy(g_buf.at[rows_of(c), :], gown_ref.at[rows_of(c), :], gown_sem.at[c])

    def chunk(c, carry, casting=False):
        slot = c % 2 if casting else lax.rem(c, 2)
        rows = rows_of(c)
        if not casting:
            @pl.when(c >= 2)
            def _():
                for copy in out_copies(c - 2, slot):
                    copy.wait()

        a_copy(c).wait()
        dy_copy(c).wait()
        gown_copy(c).start()

        def products(j):
            if casting:
                cast_tile(j)
            cols = pl.ds(j * BACK_TILE, BACK_TILE)
            pre_buf[j % 2] = dot_nn(a_buf[rows, :], up_ref[:, cols])
            dh_buf[j % 2] = dot_nt(g_buf[rows, :], down_ref[cols, :])

        def rest(j):
            cols = pl.ds(j * BACK_TILE, BACK_TILE)
            value, slope = gelu_pair(pre_buf[j % 2])
            h_buf[slot, :, cols] = value.astype(BF16)
            d_pre = (dh_buf[j % 2] * slope).astype(BF16)
            p_buf[slot, :, cols] = d_pre
            part = dot_nt(d_pre, up_ref[:, cols])
            if j == 0:
                acc_ref[...] = g_buf[rows, :].astype(F32) + part
            elif j < n_tiles - 1:
                acc_ref[...] += part
            else:
                dx_buf[rows, :] = (acc_ref[...] + part).astype(BF16)

        products(0)
        for j in range(n_tiles):
            if j + 1 < n_tiles:
                products(j + 1)
            rest(j)
        for copy in out_copies(c, slot):
            copy.start()

        @pl.when(stage > 0)
        def _():
            send_of(c).start()

        return carry

    @pl.when(stage == last)
    def _():
        chunk(0, 0, casting=True)

    @pl.when(stage < last)
    def _():
        for j in range(n_tiles):
            cast_tile(j)

    lax.fori_loop(stage // last, n_chunks, chunk, 0)

    for c in (n_chunks - 2, n_chunks - 1):
        for copy in out_copies(c, c % 2):
            copy.wait()

    def finish(c, carry):
        gown_copy(c).wait()

        @pl.when(stage > 0)
        def _():
            send_of(c).wait_send()

        return carry

    lax.fori_loop(0, n_chunks, finish, 0)


def backward(n_stages, acts, loss_grad, up32, down32):
    _, rows, width = acts.shape
    hidden = up32.shape[2]
    n_chunks = rows // BACK_ROWS
    wide = jax.ShapeDtypeStruct((rows, hidden), BF16)
    return pl.pallas_call(
        functools.partial(back_kernel, n_stages),
        name="backward",
        out_shape=(wide, wide, jax.ShapeDtypeStruct((rows, width), BF16)),
        in_specs=[ANY] * 4,
        out_specs=(ANY, ANY, ANY),
        scratch_shapes=[
            pltpu.VMEM((width, hidden), BF16),
            pltpu.VMEM((hidden, width), BF16),
            pltpu.VMEM((rows, width), BF16),
            pltpu.VMEM((rows, width), BF16),
            pltpu.VMEM((2, BACK_ROWS, hidden), BF16),
            pltpu.VMEM((2, BACK_ROWS, hidden), BF16),
            pltpu.VMEM((rows, width), BF16),
            pltpu.VMEM((BACK_ROWS, width), F32),
            pltpu.VMEM((2, BACK_ROWS, BACK_TILE), F32),
            pltpu.VMEM((2, BACK_ROWS, BACK_TILE), F32),
            pltpu.VMEM((STAGING, width, BACK_TILE), F32),
            pltpu.VMEM((STAGING, BACK_TILE, width), F32),
            pltpu.SemaphoreType.DMA((STAGING,)),
            pltpu.SemaphoreType.DMA((STAGING,)),
            pltpu.SemaphoreType.DMA((n_chunks,)),
            pltpu.SemaphoreType.DMA((n_chunks,)),
            pltpu.SemaphoreType.DMA((n_chunks,)),
            pltpu.SemaphoreType.DMA((n_chunks,)),
            pltpu.SemaphoreType.DMA((2,)),
            pltpu.SemaphoreType.DMA((2,)),
        ],
        compiler_params=pltpu.CompilerParams(collective_id=0, has_side_effects=True, vmem_limit_bytes=VMEM_LIMIT),
        cost_estimate=pl.CostEstimate(flops=6 * rows * width * hidden, bytes_accessed=6 * rows * hidden, transcendentals=rows * hidden),
    )(acts, loss_grad, up32, down32)


def wgrad_kernel(owner_ref, left_ref, right_ref, grad_ref, *refs):
    sum_refs, acc_ref = refs[:-1], refs[-1]
    lead = (0,) * (len(left_ref.shape) - 2)
    k = pl.program_id(1)
    part = dot_tn(left_ref[lead + (slice(None), slice(None))], right_ref[...])
    acc_ref[...] = jnp.where(k == 0, grad_ref[0, 0], acc_ref[...]) + part
    for p, sum_ref in enumerate(sum_refs):
        @pl.when((pl.program_id(0) == p) & (k == pl.num_programs(1) - 1))
        def _(ref=sum_ref):
            ref[...] = acc_ref[...]


def wgrad_units(kind, first, count, owner, left, right, grad):
    rows = right.shape[0]
    if kind == 0:
        half, piece = left.shape[2] // 2, right.shape[1] // PIECES
        shape = (half, piece)
        in_specs = [
            pl.BlockSpec((1, WGRAD_STEP, half), lambda i, k, own: (0, k, own[0])),
            pl.BlockSpec((WGRAD_STEP, piece), lambda i, k, own: (k, first + i)),
            pl.BlockSpec((1, 1, half, piece), lambda i, k, own: (0, 0, own[0], first + i)),
        ]
    else:
        width, piece = right.shape[1], left.shape[1] // 2 // PIECES
        shape = (piece, width)
        in_specs = [
            pl.BlockSpec((WGRAD_STEP, piece), lambda i, k, own: (k, own[0] * PIECES + first + i)),
            pl.BlockSpec((WGRAD_STEP, width), lambda i, k, own: (k, 0)),
            pl.BlockSpec((1, 1, piece, width), lambda i, k, own: (0, 0, own[0] * PIECES + first + i, 0)),
        ]
    return pl.pallas_call(
        wgrad_kernel,
        out_shape=(jax.ShapeDtypeStruct(shape, F32),) * count,
        grid_spec=pltpu.PrefetchScalarGridSpec(
            num_scalar_prefetch=1,
            grid=(count, rows // WGRAD_STEP),
            in_specs=in_specs,
            out_specs=(pl.BlockSpec(shape, lambda i, k, own: (0, 0)),) * count,
            scratch_shapes=[pltpu.VMEM(shape, F32)],
        ),
        compiler_params=pltpu.CompilerParams(vmem_limit_bytes=VMEM_LIMIT),
        cost_estimate=pl.CostEstimate(flops=2 * rows * shape[0] * shape[1] * count, bytes_accessed=15 * 1024 * 1024, transcendentals=0),
    )(owner, left, right, grad)


def combine_kernel(scale, mine_ref, theirs_ref, sq_ref, gbar_ref, sq_out):
    n_rows, cols = mine_ref.shape

    def slab(i, fold):
        rows = span(i, SLAB)
        mean = (mine_ref[rows, :] + theirs_ref[rows, :]) * scale
        gbar_ref[rows, :] = mean
        part = jnp.sum((mean * mean).reshape(SLAB // 8, 8, cols), axis=0)
        for j in range(cols // 128):
            fold = fold + part[:, j * 128:(j + 1) * 128]
        return fold

    fold = lax.fori_loop(0, n_rows // SLAB, slab, jnp.zeros((8, 128), F32))
    first = pl.program_id(0) == 0

    @pl.when(first)
    def _():
        sq_out[...] = sq_ref[...] + fold

    @pl.when(jnp.logical_not(first))
    def _():
        sq_out[...] += fold


def combine(scale, mine, theirs, squares):
    rows, cols = mine.shape
    steps = 2
    spec = pl.BlockSpec((rows // steps, cols), lambda i: (i, 0))
    small = pl.BlockSpec((8, 128), lambda i: (0, 0))
    return pl.pallas_call(
        functools.partial(combine_kernel, scale),
        name="combine",
        out_shape=(jax.ShapeDtypeStruct((rows, cols), F32), jax.ShapeDtypeStruct((8, 128), F32)),
        grid=(steps,),
        in_specs=[spec, spec, small],
        out_specs=(spec, small),
        compiler_params=pltpu.CompilerParams(vmem_limit_bytes=VMEM_LIMIT),
        cost_estimate=pl.CostEstimate(flops=4 * rows * cols, bytes_accessed=12 * rows * cols, transcendentals=0),
    )(mine, theirs, squares)


def update_kernel(n_pieces, n_alias, want_bf16, owner_ref, lr_ref, clip_ref, w_ref, m_ref, v_ref, *rest):
    g_refs = rest[:n_pieces]
    w_out, m_out, v_out, last_out = rest[n_pieces + n_alias:]
    clip, lr = clip_ref[0:1, 0:1], lr_ref[0]

    def run(g_ref, b_out):
        def slab(i, carry):
            rows = span(i, SLAB)
            w = w_ref[0, rows, :]
            q = clip * g_ref[rows, :]
            m_new = BETA1 * m_ref[0, rows, :] + (1.0 - BETA1) * q
            v_new = BETA2 * v_ref[0, rows, :] + (1.0 - BETA2) * q * q
            m_hat = m_new * (1.0 / (1.0 - BETA1 ** ADAM_STEP))
            v_hat = v_new * (1.0 / (1.0 - BETA2 ** ADAM_STEP))
            w_new = w - lr * (m_hat / (jnp.sqrt(v_hat) + ADAM_EPS) + WEIGHT_DECAY * w)
            w_out[0, rows, :], m_out[0, rows, :], v_out[0, rows, :] = w_new, m_new, v_new
            if b_out is not None:
                b_out[rows, :] = w_new.astype(BF16)
            return carry

        lax.fori_loop(0, g_ref.shape[0] // SLAB, slab, 0)

    if n_pieces == 1:
        run(g_refs[0], last_out if want_bf16 else None)
    else:
        for p in range(n_pieces):
            pl.when(pl.program_id(0) == p)(functools.partial(run, g_refs[p], None))
    if not want_bf16:
        last_out[...] = clip_ref[...]


def update_units(kind, first, owner, knobs, state, grads, chain, want_bf16):
    rows, cols = grads[0].shape
    n = len(grads)
    steps = 2 if n == 1 else 1
    block = rows // steps
    if kind == 0:
        spec = pl.BlockSpec((1, block, cols), lambda p, i, own: (0, own[0] * steps + i, first + p))
    else:
        spec = pl.BlockSpec((1, block, cols), lambda p, i, own: (0, (own[0] * PIECES + first + p) * steps + i, 0))

    def piece_spec(q):
        return pl.BlockSpec((block, cols), lambda p, i, own: (jnp.clip((p - q) * steps + i, 0, steps - 1), 0))

    full = jax.ShapeDtypeStruct(state[0].shape, F32)
    out_shape, out_specs = (full,) * 3, (spec,) * 3
    if want_bf16:
        out_shape += (jax.ShapeDtypeStruct((rows, cols), BF16),)
        out_specs += (piece_spec(0),)
    else:
        out_shape += (jax.ShapeDtypeStruct((8, 128), F32),)
        out_specs += (pl.BlockSpec((8, 128), lambda p, i, own: (0, 0)),)
    size = n * rows * cols
    return pl.pallas_call(
        functools.partial(update_kernel, n, len(chain), want_bf16),
        out_shape=out_shape,
        grid_spec=pltpu.PrefetchScalarGridSpec(
            num_scalar_prefetch=1,
            grid=(n, steps),
            in_specs=[pl.BlockSpec(memory_space=pltpu.SMEM), pl.BlockSpec(memory_space=pltpu.VMEM)] + [spec] * 3 + [piece_spec(q) for q in range(n)] + [ANY] * len(chain),
            out_specs=out_specs,
        ),
        input_output_aliases={6 + n + i: i for i in range(len(chain))},
        compiler_params=pltpu.CompilerParams(vmem_limit_bytes=UPDATE_VMEM),
        cost_estimate=pl.CostEstimate(flops=30 * size, bytes_accessed=28 * size, transcendentals=size),
    )(owner, *knobs, *state, *grads, *chain)


def norm_kernel(n_stages, n_rep, sq_ref, max_ref, clip_ref, slots, send_sem, recv_sem):
    n_dev = n_stages * n_rep
    me = lax.axis_index("data") * n_stages + lax.axis_index("stage")
    slots[me] = sq_ref[...]

    def place(d):
        q = lax.rem(me + d, n_dev)
        return {"data": q // n_stages, "stage": lax.rem(q, n_stages)}

    barrier = pltpu.get_barrier_semaphore()
    for d in range(1, n_dev):
        pl.semaphore_signal(barrier, inc=1, device_id=place(d), device_id_type=MESH_ID)
    pl.semaphore_wait(barrier, n_dev - 1)
    copies = []
    for d in range(1, n_dev):
        copies.append(pltpu.make_async_remote_copy(
            src_ref=sq_ref, dst_ref=slots.at[me], send_sem=send_sem.at[d - 1], recv_sem=recv_sem.at[d - 1],
            device_id=place(d), device_id_type=MESH_ID))
        copies[-1].start()
    for copy in copies:
        copy.wait()
    square = slots[0]
    for q in range(1, n_dev):
        square = square + slots[q]
    total = jnp.full(clip_ref.shape, jnp.sum(square), F32)
    clip_ref[...] = jnp.minimum(1.0, max_ref[0] / (jnp.sqrt(total) + NORM_EPS))


def clip_factor(n_stages, n_rep, squares, max_norm):
    n_dev = n_stages * n_rep
    return pl.pallas_call(
        functools.partial(norm_kernel, n_stages, n_rep),
        name="clip_factor",
        out_shape=jax.ShapeDtypeStruct((8, 128), F32),
        in_specs=[pl.BlockSpec(memory_space=pltpu.VMEM), pl.BlockSpec(memory_space=pltpu.SMEM)],
        out_specs=pl.BlockSpec(memory_space=pltpu.VMEM),
        scratch_shapes=[
            pltpu.VMEM((n_dev, 8, 128), F32),
            pltpu.SemaphoreType.DMA((n_dev - 1,)),
            pltpu.SemaphoreType.DMA((n_dev - 1,)),
        ],
        compiler_params=pltpu.CompilerParams(collective_id=2, has_side_effects=True),
        cost_estimate=pl.CostEstimate(flops=40000000, bytes_accessed=4096, transcendentals=0),
    )(squares, max_norm)


def fwd_kernel(n_stages, n_rep, batch_ref, *refs):
    n_w = 2 * PIECES * n_rep
    w_refs = refs[:n_w]
    out_ref, up_ref, down_ref, x_buf, acc_ref, pre_buf, up_sem, down_sem, recv_sem, send_sem = refs[n_w:]
    stage = lax.axis_index("stage")
    me = lax.axis_index("data")
    last = n_stages - 1
    total = x_buf.shape[0]
    hidden = up_ref.shape[1]
    n_tiles = hidden // FWD_TILE
    n_chunks = (total - 2 * HEAD) // FWD_ROWS + 2
    final = n_chunks - 1

    def rows_of(c):
        return chunk_rows(c, total, FWD_ROWS)

    def batch_copy(c):
        return pltpu.make_async_copy(batch_ref.at[rows_of(c), :], x_buf.at[rows_of(c), :], recv_sem.at[c])

    half_w, piece_n = w_refs[0].shape
    piece_m = w_refs[PIECES].shape[0]
    per_tile = FWD_TILE // piece_m

    def up_copy(side, k):
        owner = me if side == 0 else 1 - me
        dst = up_ref.at[span(owner, half_w), pl.ds(k * piece_n, piece_n)]
        return pltpu.make_async_copy(w_refs[2 * side * PIECES + k], dst, up_sem.at[side * PIECES + k])

    def down_copy(side, g):
        src = w_refs[(2 * side + 1) * PIECES + g % PIECES]
        return pltpu.make_async_copy(src, down_ref.at[pl.ds(g * piece_m, piece_m), :], down_sem.at[g])

    @pl.when(stage == 0)
    def _():
        batch_copy(0).start()

    for j in range(n_tiles):
        for side in range(n_rep):
            up_copy(side, j).start()
        for g in range(j * per_tile, (j + 1) * per_tile):
            @pl.when(me == g // PIECES)
            def _(g=g):
                down_copy(0, g).start()

            @pl.when(me != g // PIECES)
            def _(g=g):
                down_copy(1, g).start()

    meet_neighbours(stage, n_stages)

    def send_of(c):
        return pltpu.make_async_remote_copy(
            src_ref=out_ref.at[rows_of(c), :], dst_ref=x_buf.at[rows_of(c), :],
            send_sem=send_sem.at[c], recv_sem=recv_sem.at[c],
            device_id={"stage": stage + 1}, device_id_type=MESH_ID)

    def chunk(c, carry, first=False):
        rows = rows_of(c)
        size = pl.ds(0, HEAD if isinstance(c, int) else FWD_ROWS)
        batch_copy(c).wait()

        def products(j):
            if first:
                for side in range(n_rep):
                    up_copy(side, j).wait()
            pre_buf[j % 2, size, :] = dot_nn(x_buf[rows, :], up_ref[:, pl.ds(j * FWD_TILE, FWD_TILE)])

        def rest(j):
            if first:
                for g in range(j * per_tile, (j + 1) * per_tile):
                    down_copy(0, g).wait()
            hid = gelu_value(pre_buf[j % 2, size, :]).astype(BF16)
            part = dot_nn(hid, down_ref[pl.ds(j * FWD_TILE, FWD_TILE), :])
            if j == 0:
                acc_ref[size, :] = x_buf[rows, :].astype(F32) + part
            elif j < n_tiles - 1:
                acc_ref[size, :] += part
            else:
                out_ref[rows, :] = (acc_ref[size, :] + part).astype(BF16)

        products(0)
        for j in range(n_tiles):
            if j + 1 < n_tiles:
                products(j + 1)
            rest(j)

        @pl.when(stage < last)
        def _():
            send_of(c).start()

        return carry

    chunk(0, 0, first=True)

    @pl.when(stage == 0)
    def _():
        def load(c, carry):
            batch_copy(c).start()
            return carry

        lax.fori_loop(1, final, load, 0)
        load(final, 0)

    lax.fori_loop(1, final, chunk, 0)
    chunk(final, 0)

    @pl.when(stage < last)
    def _():
        def finish(c, carry):
            send_of(c).wait_send()
            return carry

        finish(0, 0)
        lax.fori_loop(1, final, finish, 0)
        finish(final, 0)


def forward(n_stages, n_rep, next_batch, weights):
    n_micro, rows, width = next_batch.shape
    total = n_micro * rows
    hidden = PIECES * weights[0].shape[1]
    n_chunks = (total - 2 * HEAD) // FWD_ROWS + 2
    return pl.pallas_call(
        functools.partial(fwd_kernel, n_stages, n_rep),
        name="forward",
        out_shape=pltpu.VMEM((total, width), BF16),
        in_specs=[ANY] * (1 + len(weights)),
        out_specs=pl.BlockSpec(memory_space=pltpu.VMEM),
        scratch_shapes=[
            pltpu.VMEM((width, hidden), BF16),
            pltpu.VMEM((hidden, width), BF16),
            pltpu.VMEM((total, width), BF16),
            pltpu.VMEM((FWD_ROWS, width), F32),
            pltpu.VMEM((2, FWD_ROWS, FWD_TILE), F32),
            pltpu.SemaphoreType.DMA((n_rep * PIECES,)),
            pltpu.SemaphoreType.DMA((n_rep * PIECES,)),
            pltpu.SemaphoreType.DMA((n_chunks,)),
            pltpu.SemaphoreType.DMA((n_chunks,)),
        ],
        compiler_params=pltpu.CompilerParams(collective_id=1, has_side_effects=True, vmem_limit_bytes=FWD_VMEM),
        cost_estimate=pl.CostEstimate(flops=4 * n_micro * rows * width * hidden, bytes_accessed=6 * rows * hidden, transcendentals=n_micro * rows * hidden),
    )(next_batch.reshape(total, width), *weights)


def store_kernel(y_ref, out_ref, sem):
    half = y_ref.shape[0] // 2
    copies = [pltpu.make_async_copy(y_ref.at[span(i, half), :], out_ref.at[span(i, half), :], sem.at[i]) for i in range(2)]
    for copy in copies:
        copy.start()
    for copy in copies:
        copy.wait()


def store(y):
    return pl.pallas_call(
        store_kernel,
        name="store",
        out_shape=jax.ShapeDtypeStruct(y.shape, y.dtype),
        in_specs=[pl.BlockSpec(memory_space=pltpu.VMEM)],
        out_specs=ANY,
        scratch_shapes=[pltpu.SemaphoreType.DMA((2,))],
        compiler_params=pltpu.CompilerParams(vmem_limit_bytes=STORE_VMEM),
        cost_estimate=pl.CostEstimate(flops=4000000, bytes_accessed=2 * y.size, transcendentals=0),
    )(y)


def part_of(parts):
    return next(iter(parts.values()))


def solution(mesh):
    n_stages = mesh.shape["stage"]
    n_rep = mesh.shape["data"]
    swap = [(i, n_rep - 1 - i) for i in range(n_rep)]

    def exchange(x):
        return lax.ppermute(x, "data", swap)

    def local_step(master_up, master_down, mom1_up, mom1_down, mom2_up, mom2_down, grad_up, grad_down, stage_acts, loss_grad, next_batch, learn_rate, max_norm):
        me = lax.axis_index("data")
        mine = jnp.reshape(me, (1,)).astype(jnp.int32)
        other = 1 - mine
        hid, d_pre, g_own = backward(n_stages, stage_acts, loss_grad, master_up, master_down)

        units = [(kind, first + i) for kind, first, count in GROUPS for i in range(count)]

        def wgrad(group, owner):
            kind, first, count = group
            operands = (stage_acts, d_pre, grad_up) if kind == 0 else (hid, g_own, grad_down)
            parts = wgrad_units(kind, first, count, owner, *operands)
            return {(kind, first + i): parts[i] for i in range(count)}

        arrived, whose = {}, other
        for group in GROUPS:
            parts = wgrad(group, whose)
            for unit, part in parts.items():
                arrived[unit] = exchange(part)
            whose = lax.optimization_barrier((other, part_of(parts)))[0]
        gbar, squares = {}, jnp.zeros((8, 128), F32)
        own_part = {}
        for kind in (0, 1):
            own_part.update(wgrad((kind, 0, PIECES), mine))
        for unit in units:
            gbar[unit], squares = combine(1.0 / n_rep, own_part[unit], arrived[unit], squares)
        clip = clip_factor(n_stages, n_rep, squares, jnp.reshape(max_norm, (1,)))
        knobs = (jnp.reshape(learn_rate, (1,)), clip)
        gbar_other = {}
        for unit in F32_FIRST:
            half = gbar[unit].shape[0] // 2
            top = exchange(gbar[unit][:half])
            low = exchange(lax.optimization_barrier((gbar[unit][half:], clip))[0])
            gbar_other[unit] = jnp.concatenate([top, low], axis=0)
        state = ((master_up, mom1_up, mom2_up), (master_down, mom1_down, mom2_down))
        chain = [(), ()]

        def update(unit, owner, grad):
            res = update_units(unit[0], unit[1], owner, knobs, state[unit[0]], [grad], chain[unit[0]], True)
            chain[unit[0]] = res[:3]
            return res[3]

        def update_group(kind, first, stop, clip):
            grads = [gbar_other[kind, k] for k in range(first, stop)]
            res = update_units(kind, first, other, (knobs[0], clip), state[kind], grads, chain[kind], False)
            chain[kind] = res[:3]
            return res[3]

        late = [unit for unit in units if unit not in F32_FIRST]
        own_w, other_w = {}, {}
        for unit in late + list(F32_FIRST):
            own_w[unit] = update(unit, mine, gbar[unit])
            if unit in late:
                other_w[unit] = exchange(own_w[unit])
        for unit in late:
            ready = lax.optimization_barrier((gbar[unit], own_w[late[-1]]))[0]
            gbar_other[unit] = exchange(ready)
        for unit in F32_FIRST:
            other_w[unit] = update(unit, other, gbar_other[unit])
        weights = []
        for side in (own_w, other_w):
            for kind in (0, 1):
                weights += [side[kind, k] for k in range(PIECES)]
        stage_outs = store(forward(n_stages, n_rep, next_batch, weights)).reshape((1,) + next_batch.shape)
        for kind, first, stop in TAIL:
            clip = update_group(kind, first, stop, clip)
        (new_up, new_m1_up, new_m2_up), (new_down, new_m1_down, new_m2_down) = chain
        return (new_up, new_down, new_m1_up, new_m1_down, new_m2_up, new_m2_down, stage_outs)

    w_spec = P("stage", None, None)
    g_spec = P("data", "stage", None, None)
    in_specs = (w_spec,) * 6 + (g_spec, g_spec, P("stage", "data", None), P("data", None), P(None, "data", None), P(), P())
    out_specs = (w_spec,) * 6 + (P("stage", None, "data", None),)
    return jax.shard_map(local_step, mesh=mesh, in_specs=in_specs, out_specs=out_specs, check_vma=False)
```

```python
import functools

import jax
import jax.numpy as jnp
from jax import lax
from jax.experimental import pallas as pl
from jax.experimental.pallas import tpu as pltpu
from jax.sharding import PartitionSpec as P


BETA1 = 0.9
BETA2 = 0.95
ADAM_EPS = 1e-8
WEIGHT_DECAY = 0.1
NORM_EPS = 1e-6
ADAM_STEP = 8
SQRT_TWO_PI = 0.7978845608028654
GELU_CUBIC = 0.044715

BACK_ROWS = 256
FWD_ROWS = 256
HEAD = 128
BACK_TILE = 512
FWD_TILE = 512
PIECES = 6
F32_FIRST = ((0, 0),)
GROUPS = ((0, 0, 1), (1, 0, 2), (0, 1, 2), (1, 2, 2), (0, 3, 2), (1, 4, 2), (0, 5, 1))
TAIL = ((0, 1, 5), (1, 0, 6), (0, 5, 6))
STAGING = 3
WGRAD_STEP = 4096
SLAB = 16

BF16 = jnp.bfloat16
F32 = jnp.float32
MESH_ID = pl.DeviceIdType.MESH
ANY = pl.BlockSpec(memory_space=pl.ANY)
VMEM_LIMIT = 60 * 1024 * 1024
FWD_VMEM = 54000000
STORE_VMEM = 4 * 1024 * 1024
UPDATE_VMEM = 60 * 1024 * 1024


def dot_nn(left, right):
    return lax.dot_general(left, right, (((1,), (0,)), ((), ())), preferred_element_type=F32)


def dot_nt(left, right):
    return lax.dot_general(left, right, (((1,), (1,)), ((), ())), preferred_element_type=F32)


def dot_tn(left, right):
    return lax.dot_general(left, right, (((0,), (0,)), ((), ())), preferred_element_type=F32)


def span(index, size):
    if isinstance(index, int):
        return pl.ds(index * size, size)
    return pl.ds(pl.multiple_of(index * size, size), size)


def chunk_rows(c, total, size):
    if isinstance(c, int):
        return pl.ds(0 if c == 0 else total - HEAD, HEAD)
    return pl.ds(pl.multiple_of(HEAD + (c - 1) * size, HEAD), size)


def tanh_part(x, sq):
    return jnp.tanh(x * (SQRT_TWO_PI + (SQRT_TWO_PI * GELU_CUBIC) * sq))


def gelu_value(x):
    return x * (0.5 + 0.5 * tanh_part(x, x * x))


def gelu_pair(x):
    sq = x * x
    th = tanh_part(x, sq)
    half = 0.5 + 0.5 * th
    value = x * half
    slope = half + value * (1.0 - th) * (SQRT_TWO_PI + (3.0 * SQRT_TWO_PI * GELU_CUBIC) * sq)
    return value, slope


def meet_neighbours(stage, n_stages):
    barrier = pltpu.get_barrier_semaphore()

    @pl.when(stage > 0)
    def _():
        pl.semaphore_signal(barrier, inc=1, device_id={"stage": stage - 1}, device_id_type=MESH_ID)

    @pl.when(stage < n_stages - 1)
    def _():
        pl.semaphore_signal(barrier, inc=1, device_id={"stage": stage + 1}, device_id_type=MESH_ID)

    pl.semaphore_wait(barrier, jnp.minimum(stage, 1) + jnp.minimum(n_stages - 1 - stage, 1))


def back_kernel(n_stages, acts_ref, dy_ref, up32_ref, down32_ref, hid_ref, dpre_ref, gown_ref,
                up_ref, down_ref, a_buf, g_buf, h_buf, p_buf, dx_buf, acc_ref, pre_buf, dh_buf, stage_u, stage_v,
                u_sem, v_sem, a_sem, recv_sem, send_sem, gown_sem, h_sem, p_sem):
    stage = lax.axis_index("stage")
    last = n_stages - 1
    rows_all = g_buf.shape[0]
    hidden = up_ref.shape[1]
    n_chunks = rows_all // BACK_ROWS
    n_tiles = hidden // BACK_TILE

    def tile_copies(j):
        slot, cols = j % STAGING, pl.ds(j * BACK_TILE, BACK_TILE)
        return (pltpu.make_async_copy(up32_ref.at[0, :, cols], stage_u.at[slot], u_sem.at[slot]),
                pltpu.make_async_copy(down32_ref.at[0, cols, :], stage_v.at[slot], v_sem.at[slot]))

    def rows_of(c):
        return pl.ds(c * BACK_ROWS, BACK_ROWS) if isinstance(c, int) else span(c, BACK_ROWS)

    def a_copy(c):
        return pltpu.make_async_copy(acts_ref.at[0, rows_of(c), :], a_buf.at[rows_of(c), :], a_sem.at[c])

    def dy_copy(c):
        return pltpu.make_async_copy(dy_ref.at[rows_of(c), :], g_buf.at[rows_of(c), :], recv_sem.at[c])

    a_copy(0).start()

    @pl.when(stage == last)
    def _():
        dy_copy(0).start()

    for j in range(STAGING):
        for copy in tile_copies(j):
            copy.start()

    def load_rest(c, carry):
        a_copy(c).start()

        @pl.when(stage == last)
        def _():
            dy_copy(c).start()

        return carry

    def cast_tile(j):
        cols = pl.ds(j * BACK_TILE, BACK_TILE)
        for copy in tile_copies(j):
            copy.wait()
        up_ref[:, cols] = stage_u[j % STAGING].astype(BF16)
        down_ref[cols, :] = stage_v[j % STAGING].astype(BF16)
        if j + STAGING < n_tiles:
            for copy in tile_copies(j + STAGING):
                copy.start()
        if j == n_tiles - STAGING:
            lax.fori_loop(1, n_chunks, load_rest, 0)

    meet_neighbours(stage, n_stages)

    def send_of(c):
        return pltpu.make_async_remote_copy(
            src_ref=dx_buf.at[rows_of(c), :], dst_ref=g_buf.at[rows_of(c), :],
            send_sem=send_sem.at[c], recv_sem=recv_sem.at[c],
            device_id={"stage": stage - 1}, device_id_type=MESH_ID)

    def out_copies(c, slot):
        return (pltpu.make_async_copy(h_buf.at[slot], hid_ref.at[rows_of(c), :], h_sem.at[slot]),
                pltpu.make_async_copy(p_buf.at[slot], dpre_ref.at[rows_of(c), :], p_sem.at[slot]))

    def gown_copy(c):
        return pltpu.make_async_copy(g_buf.at[rows_of(c), :], gown_ref.at[rows_of(c), :], gown_sem.at[c])

    def chunk(c, carry, casting=False):
        slot = c % 2 if casting else lax.rem(c, 2)
        rows = rows_of(c)
        if not casting:
            @pl.when(c >= 2)
            def _():
                for copy in out_copies(c - 2, slot):
                    copy.wait()

        a_copy(c).wait()
        dy_copy(c).wait()
        gown_copy(c).start()

        def products(j):
            if casting:
                cast_tile(j)
            cols = pl.ds(j * BACK_TILE, BACK_TILE)
            pre_buf[j % 2] = dot_nn(a_buf[rows, :], up_ref[:, cols])
            dh_buf[j % 2] = dot_nt(g_buf[rows, :], down_ref[cols, :])

        def rest(j):
            cols = pl.ds(j * BACK_TILE, BACK_TILE)
            value, slope = gelu_pair(pre_buf[j % 2])
            h_buf[slot, :, cols] = value.astype(BF16)
            d_pre = (dh_buf[j % 2] * slope).astype(BF16)
            p_buf[slot, :, cols] = d_pre
            part = dot_nt(d_pre, up_ref[:, cols])
            if j == 0:
                acc_ref[...] = g_buf[rows, :].astype(F32) + part
            elif j < n_tiles - 1:
                acc_ref[...] += part
            else:
                dx_buf[rows, :] = (acc_ref[...] + part).astype(BF16)

        products(0)
        for j in range(n_tiles):
            if j + 1 < n_tiles:
                products(j + 1)
            rest(j)
        for copy in out_copies(c, slot):
            copy.start()

        @pl.when(stage > 0)
        def _():
            send_of(c).start()

        return carry

    @pl.when(stage == last)
    def _():
        chunk(0, 0, casting=True)

    @pl.when(stage < last)
    def _():
        for j in range(n_tiles):
            cast_tile(j)

    lax.fori_loop(stage // last, n_chunks, chunk, 0)

    for c in (n_chunks - 2, n_chunks - 1):
        for copy in out_copies(c, c % 2):
            copy.wait()

    def finish(c, carry):
        gown_copy(c).wait()

        @pl.when(stage > 0)
        def _():
            send_of(c).wait_send()

        return carry

    lax.fori_loop(0, n_chunks, finish, 0)


def backward(n_stages, acts, loss_grad, up32, down32):
    _, rows, width = acts.shape
    hidden = up32.shape[2]
    n_chunks = rows // BACK_ROWS
    wide = jax.ShapeDtypeStruct((rows, hidden), BF16)
    return pl.pallas_call(
        functools.partial(back_kernel, n_stages),
        name="backward",
        out_shape=(wide, wide, jax.ShapeDtypeStruct((rows, width), BF16)),
        in_specs=[ANY] * 4,
        out_specs=(ANY, ANY, ANY),
        scratch_shapes=[
            pltpu.VMEM((width, hidden), BF16),
            pltpu.VMEM((hidden, width), BF16),
            pltpu.VMEM((rows, width), BF16),
            pltpu.VMEM((rows, width), BF16),
            pltpu.VMEM((2, BACK_ROWS, hidden), BF16),
            pltpu.VMEM((2, BACK_ROWS, hidden), BF16),
            pltpu.VMEM((rows, width), BF16),
            pltpu.VMEM((BACK_ROWS, width), F32),
            pltpu.VMEM((2, BACK_ROWS, BACK_TILE), F32),
            pltpu.VMEM((2, BACK_ROWS, BACK_TILE), F32),
            pltpu.VMEM((STAGING, width, BACK_TILE), F32),
            pltpu.VMEM((STAGING, BACK_TILE, width), F32),
            pltpu.SemaphoreType.DMA((STAGING,)),
            pltpu.SemaphoreType.DMA((STAGING,)),
            pltpu.SemaphoreType.DMA((n_chunks,)),
            pltpu.SemaphoreType.DMA((n_chunks,)),
            pltpu.SemaphoreType.DMA((n_chunks,)),
            pltpu.SemaphoreType.DMA((n_chunks,)),
            pltpu.SemaphoreType.DMA((2,)),
            pltpu.SemaphoreType.DMA((2,)),
        ],
        compiler_params=pltpu.CompilerParams(collective_id=0, has_side_effects=True, vmem_limit_bytes=VMEM_LIMIT),
        cost_estimate=pl.CostEstimate(flops=6 * rows * width * hidden, bytes_accessed=6 * rows * hidden, transcendentals=rows * hidden),
    )(acts, loss_grad, up32, down32)


def wgrad_kernel(owner_ref, left_ref, right_ref, grad_ref, *refs):
    sum_refs, acc_ref = refs[:-1], refs[-1]
    lead = (0,) * (len(left_ref.shape) - 2)
    acc_ref[...] = grad_ref[0, 0]

    def step(k, carry):
        part = span(k, WGRAD_STEP)
        acc_ref[...] += dot_tn(left_ref[lead + (part, slice(None))], right_ref[part, :])
        return carry

    lax.fori_loop(0, right_ref.shape[0] // WGRAD_STEP, step, 0)
    for p, sum_ref in enumerate(sum_refs):
        def put(ref=sum_ref):
            ref[...] = acc_ref[...]

        if len(sum_refs) == 1:
            put()
        else:
            pl.when(pl.program_id(0) == p)(put)


def wgrad_units(kind, first, count, owner, left, right, grad):
    rows = right.shape[0]
    if kind == 0:
        half, piece = left.shape[2] // 2, right.shape[1] // PIECES
        shape = (half, piece)
        in_specs = [
            pl.BlockSpec((1, rows, half), lambda i, own: (0, 0, own[0])),
            pl.BlockSpec((rows, piece), lambda i, own: (0, first + i)),
            pl.BlockSpec((1, 1, half, piece), lambda i, own: (0, 0, own[0], first + i)),
        ]
    else:
        width, piece = right.shape[1], left.shape[1] // 2 // PIECES
        shape = (piece, width)
        in_specs = [
            pl.BlockSpec((rows, piece), lambda i, own: (0, own[0] * PIECES + first + i)),
            pl.BlockSpec((rows, width), lambda i, own: (0, 0)),
            pl.BlockSpec((1, 1, piece, width), lambda i, own: (0, 0, own[0] * PIECES + first + i, 0)),
        ]
    return pl.pallas_call(
        wgrad_kernel,
        out_shape=(jax.ShapeDtypeStruct(shape, F32),) * count,
        grid_spec=pltpu.PrefetchScalarGridSpec(
            num_scalar_prefetch=1,
            grid=(count,),
            in_specs=in_specs,
            out_specs=(pl.BlockSpec(shape, lambda i, own: (0, 0)),) * count,
            scratch_shapes=[pltpu.VMEM(shape, F32)],
        ),
        compiler_params=pltpu.CompilerParams(vmem_limit_bytes=VMEM_LIMIT),
        cost_estimate=pl.CostEstimate(flops=2 * rows * shape[0] * shape[1] * count, bytes_accessed=15 * 1024 * 1024, transcendentals=0),
    )(owner, left, right, grad)


def combine_kernel(scale, mine_ref, theirs_ref, sq_ref, gbar_ref, sq_out):
    n_rows, cols = mine_ref.shape

    def slab(i, fold):
        rows = span(i, SLAB)
        mean = (mine_ref[rows, :] + theirs_ref[rows, :]) * scale
        gbar_ref[rows, :] = mean
        part = jnp.sum((mean * mean).reshape(SLAB // 8, 8, cols), axis=0)
        for j in range(cols // 128):
            fold = fold + part[:, j * 128:(j + 1) * 128]
        return fold

    fold = lax.fori_loop(0, n_rows // SLAB, slab, jnp.zeros((8, 128), F32))
    first = pl.program_id(0) == 0

    @pl.when(first)
    def _():
        sq_out[...] = sq_ref[...] + fold

    @pl.when(jnp.logical_not(first))
    def _():
        sq_out[...] += fold


def combine(scale, mine, theirs, squares):
    rows, cols = mine.shape
    steps = 2
    spec = pl.BlockSpec((rows // steps, cols), lambda i: (i, 0))
    small = pl.BlockSpec((8, 128), lambda i: (0, 0))
    return pl.pallas_call(
        functools.partial(combine_kernel, scale),
        name="combine",
        out_shape=(jax.ShapeDtypeStruct((rows, cols), F32), jax.ShapeDtypeStruct((8, 128), F32)),
        grid=(steps,),
        in_specs=[spec, spec, small],
        out_specs=(spec, small),
        compiler_params=pltpu.CompilerParams(vmem_limit_bytes=VMEM_LIMIT),
        cost_estimate=pl.CostEstimate(flops=4 * rows * cols, bytes_accessed=12 * rows * cols, transcendentals=0),
    )(mine, theirs, squares)


def update_kernel(n_pieces, n_alias, want_bf16, owner_ref, lr_ref, clip_ref, w_ref, m_ref, v_ref, *rest):
    g_refs = rest[:n_pieces]
    w_out, m_out, v_out, last_out = rest[n_pieces + n_alias:]
    clip, lr = clip_ref[0:1, 0:1], lr_ref[0]

    def run(g_ref, b_out):
        def slab(i, carry):
            rows = span(i, SLAB)
            w = w_ref[0, rows, :]
            q = clip * g_ref[rows, :]
            m_new = BETA1 * m_ref[0, rows, :] + (1.0 - BETA1) * q
            v_new = BETA2 * v_ref[0, rows, :] + (1.0 - BETA2) * q * q
            m_hat = m_new * (1.0 / (1.0 - BETA1 ** ADAM_STEP))
            v_hat = v_new * (1.0 / (1.0 - BETA2 ** ADAM_STEP))
            w_new = w - lr * (m_hat / (jnp.sqrt(v_hat) + ADAM_EPS) + WEIGHT_DECAY * w)
            w_out[0, rows, :], m_out[0, rows, :], v_out[0, rows, :] = w_new, m_new, v_new
            if b_out is not None:
                b_out[rows, :] = w_new.astype(BF16)
            return carry

        lax.fori_loop(0, g_ref.shape[0] // SLAB, slab, 0)

    if n_pieces == 1:
        run(g_refs[0], last_out if want_bf16 else None)
    else:
        for p in range(n_pieces):
            pl.when(pl.program_id(0) == p)(functools.partial(run, g_refs[p], None))
    if not want_bf16:
        last_out[...] = clip_ref[...]


def update_units(kind, first, owner, knobs, state, grads, chain, want_bf16):
    rows, cols = grads[0].shape
    n = len(grads)
    steps = 2 if n == 1 else 1
    block = rows // steps
    if kind == 0:
        spec = pl.BlockSpec((1, block, cols), lambda p, i, own: (0, own[0] * steps + i, first + p))
    else:
        spec = pl.BlockSpec((1, block, cols), lambda p, i, own: (0, (own[0] * PIECES + first + p) * steps + i, 0))

    def piece_spec(q):
        return pl.BlockSpec((block, cols), lambda p, i, own: (jnp.clip((p - q) * steps + i, 0, steps - 1), 0))

    full = jax.ShapeDtypeStruct(state[0].shape, F32)
    out_shape, out_specs = (full,) * 3, (spec,) * 3
    if want_bf16:
        out_shape += (jax.ShapeDtypeStruct((rows, cols), BF16),)
        out_specs += (piece_spec(0),)
    else:
        out_shape += (jax.ShapeDtypeStruct((8, 128), F32),)
        out_specs += (pl.BlockSpec((8, 128), lambda p, i, own: (0, 0)),)
    size = n * rows * cols
    return pl.pallas_call(
        functools.partial(update_kernel, n, len(chain), want_bf16),
        out_shape=out_shape,
        grid_spec=pltpu.PrefetchScalarGridSpec(
            num_scalar_prefetch=1,
            grid=(n, steps),
            in_specs=[pl.BlockSpec(memory_space=pltpu.SMEM), pl.BlockSpec(memory_space=pltpu.VMEM)] + [spec] * 3 + [piece_spec(q) for q in range(n)] + [ANY] * len(chain),
            out_specs=out_specs,
        ),
        input_output_aliases={6 + n + i: i for i in range(len(chain))},
        compiler_params=pltpu.CompilerParams(vmem_limit_bytes=UPDATE_VMEM),
        cost_estimate=pl.CostEstimate(flops=30 * size, bytes_accessed=28 * size, transcendentals=size),
    )(owner, *knobs, *state, *grads, *chain)


def norm_kernel(n_stages, n_rep, sq_ref, max_ref, clip_ref, slots, send_sem, recv_sem):
    n_dev = n_stages * n_rep
    me = lax.axis_index("data") * n_stages + lax.axis_index("stage")
    slots[me] = sq_ref[...]

    def place(d):
        q = lax.rem(me + d, n_dev)
        return {"data": q // n_stages, "stage": lax.rem(q, n_stages)}

    barrier = pltpu.get_barrier_semaphore()
    for d in range(1, n_dev):
        pl.semaphore_signal(barrier, inc=1, device_id=place(d), device_id_type=MESH_ID)
    pl.semaphore_wait(barrier, n_dev - 1)
    copies = []
    for d in range(1, n_dev):
        copies.append(pltpu.make_async_remote_copy(
            src_ref=sq_ref, dst_ref=slots.at[me], send_sem=send_sem.at[d - 1], recv_sem=recv_sem.at[d - 1],
            device_id=place(d), device_id_type=MESH_ID))
        copies[-1].start()
    for copy in copies:
        copy.wait()
    square = slots[0]
    for q in range(1, n_dev):
        square = square + slots[q]
    total = jnp.full(clip_ref.shape, jnp.sum(square), F32)
    clip_ref[...] = jnp.minimum(1.0, max_ref[0] / (jnp.sqrt(total) + NORM_EPS))


def clip_factor(n_stages, n_rep, squares, max_norm):
    n_dev = n_stages * n_rep
    return pl.pallas_call(
        functools.partial(norm_kernel, n_stages, n_rep),
        name="clip_factor",
        out_shape=jax.ShapeDtypeStruct((8, 128), F32),
        in_specs=[pl.BlockSpec(memory_space=pltpu.VMEM), pl.BlockSpec(memory_space=pltpu.SMEM)],
        out_specs=pl.BlockSpec(memory_space=pltpu.VMEM),
        scratch_shapes=[
            pltpu.VMEM((n_dev, 8, 128), F32),
            pltpu.SemaphoreType.DMA((n_dev - 1,)),
            pltpu.SemaphoreType.DMA((n_dev - 1,)),
        ],
        compiler_params=pltpu.CompilerParams(collective_id=2, has_side_effects=True),
        cost_estimate=pl.CostEstimate(flops=40000000, bytes_accessed=4096, transcendentals=0),
    )(squares, max_norm)


def fwd_kernel(n_stages, n_rep, batch_ref, *refs):
    n_w = 2 * PIECES * n_rep
    w_refs = refs[:n_w]
    out_ref, up_ref, down_ref, x_buf, acc_ref, pre_buf, w_sem, recv_sem, send_sem = refs[n_w:]
    stage = lax.axis_index("stage")
    me = lax.axis_index("data")
    last = n_stages - 1
    total = x_buf.shape[0]
    hidden = up_ref.shape[1]
    n_tiles = hidden // FWD_TILE
    n_chunks = (total - 2 * HEAD) // FWD_ROWS + 2
    final = n_chunks - 1

    def rows_of(c):
        return chunk_rows(c, total, FWD_ROWS)

    def batch_copy(c):
        return pltpu.make_async_copy(batch_ref.at[rows_of(c), :], x_buf.at[rows_of(c), :], recv_sem.at[c])

    @pl.when(stage == 0)
    def _():
        batch_copy(0).start()

    copies = []
    for side in range(n_rep):
        owner = me if side == 0 else 1 - me
        for k in range(PIECES):
            u_src = w_refs[(2 * side) * PIECES + k]
            v_src = w_refs[(2 * side + 1) * PIECES + k]
            half_w, piece_n = u_src.shape
            piece_m = v_src.shape[0]
            u_dst = up_ref.at[span(owner, half_w), pl.ds(k * piece_n, piece_n)]
            v_dst = down_ref.at[span(owner * PIECES + k, piece_m), :]
            copies.append(pltpu.make_async_copy(u_src, u_dst, w_sem.at[len(copies)]))
            copies.append(pltpu.make_async_copy(v_src, v_dst, w_sem.at[len(copies)]))
    for copy in copies:
        copy.start()

    meet_neighbours(stage, n_stages)
    for copy in copies:
        copy.wait()

    @pl.when(stage == 0)
    def _():
        def load(c, carry):
            batch_copy(c).start()
            return carry

        lax.fori_loop(1, final, load, 0)
        load(final, 0)

    def send_of(c):
        return pltpu.make_async_remote_copy(
            src_ref=out_ref.at[rows_of(c), :], dst_ref=x_buf.at[rows_of(c), :],
            send_sem=send_sem.at[c], recv_sem=recv_sem.at[c],
            device_id={"stage": stage + 1}, device_id_type=MESH_ID)

    def chunk(c, carry):
        rows = rows_of(c)
        size = pl.ds(0, HEAD if isinstance(c, int) else FWD_ROWS)
        batch_copy(c).wait()

        def products(j):
            pre_buf[j % 2, size, :] = dot_nn(x_buf[rows, :], up_ref[:, pl.ds(j * FWD_TILE, FWD_TILE)])

        def rest(j):
            hid = gelu_value(pre_buf[j % 2, size, :]).astype(BF16)
            part = dot_nn(hid, down_ref[pl.ds(j * FWD_TILE, FWD_TILE), :])
            if j == 0:
                acc_ref[size, :] = x_buf[rows, :].astype(F32) + part
            elif j < n_tiles - 1:
                acc_ref[size, :] += part
            else:
                out_ref[rows, :] = (acc_ref[size, :] + part).astype(BF16)

        products(0)
        for j in range(n_tiles):
            if j + 1 < n_tiles:
                products(j + 1)
            rest(j)

        @pl.when(stage < last)
        def _():
            send_of(c).start()

        return carry

    chunk(0, 0)
    lax.fori_loop(1, final, chunk, 0)
    chunk(final, 0)

    @pl.when(stage < last)
    def _():
        def finish(c, carry):
            send_of(c).wait_send()
            return carry

        finish(0, 0)
        lax.fori_loop(1, final, finish, 0)
        finish(final, 0)


def forward(n_stages, n_rep, next_batch, weights):
    n_micro, rows, width = next_batch.shape
    total = n_micro * rows
    hidden = PIECES * weights[0].shape[1]
    n_chunks = (total - 2 * HEAD) // FWD_ROWS + 2
    return pl.pallas_call(
        functools.partial(fwd_kernel, n_stages, n_rep),
        name="forward",
        out_shape=pltpu.VMEM((total, width), BF16),
        in_specs=[ANY] * (1 + len(weights)),
        out_specs=pl.BlockSpec(memory_space=pltpu.VMEM),
        scratch_shapes=[
            pltpu.VMEM((width, hidden), BF16),
            pltpu.VMEM((hidden, width), BF16),
            pltpu.VMEM((total, width), BF16),
            pltpu.VMEM((FWD_ROWS, width), F32),
            pltpu.VMEM((2, FWD_ROWS, FWD_TILE), F32),
            pltpu.SemaphoreType.DMA((len(weights),)),
            pltpu.SemaphoreType.DMA((n_chunks,)),
            pltpu.SemaphoreType.DMA((n_chunks,)),
        ],
        compiler_params=pltpu.CompilerParams(collective_id=1, has_side_effects=True, vmem_limit_bytes=FWD_VMEM),
        cost_estimate=pl.CostEstimate(flops=4 * n_micro * rows * width * hidden, bytes_accessed=6 * rows * hidden, transcendentals=n_micro * rows * hidden),
    )(next_batch.reshape(total, width), *weights)


def store_kernel(y_ref, out_ref, sem):
    half = y_ref.shape[0] // 2
    copies = [pltpu.make_async_copy(y_ref.at[span(i, half), :], out_ref.at[span(i, half), :], sem.at[i]) for i in range(2)]
    for copy in copies:
        copy.start()
    for copy in copies:
        copy.wait()


def store(y):
    return pl.pallas_call(
        store_kernel,
        name="store",
        out_shape=jax.ShapeDtypeStruct(y.shape, y.dtype),
        in_specs=[pl.BlockSpec(memory_space=pltpu.VMEM)],
        out_specs=ANY,
        scratch_shapes=[pltpu.SemaphoreType.DMA((2,))],
        compiler_params=pltpu.CompilerParams(vmem_limit_bytes=STORE_VMEM),
        cost_estimate=pl.CostEstimate(flops=4000000, bytes_accessed=2 * y.size, transcendentals=0),
    )(y)


def part_of(parts):
    return next(iter(parts.values()))


def solution(mesh):
    n_stages = mesh.shape["stage"]
    n_rep = mesh.shape["data"]
    swap = [(i, n_rep - 1 - i) for i in range(n_rep)]

    def exchange(x):
        return lax.ppermute(x, "data", swap)

    def local_step(master_up, master_down, mom1_up, mom1_down, mom2_up, mom2_down, grad_up, grad_down, stage_acts, loss_grad, next_batch, learn_rate, max_norm):
        me = lax.axis_index("data")
        mine = jnp.reshape(me, (1,)).astype(jnp.int32)
        other = 1 - mine
        hid, d_pre, g_own = backward(n_stages, stage_acts, loss_grad, master_up, master_down)

        units = [(kind, first + i) for kind, first, count in GROUPS for i in range(count)]

        def wgrad(group, owner):
            kind, first, count = group
            operands = (stage_acts, d_pre, grad_up) if kind == 0 else (hid, g_own, grad_down)
            parts = wgrad_units(kind, first, count, owner, *operands)
            return {(kind, first + i): parts[i] for i in range(count)}

        arrived, whose = {}, other
        for group in GROUPS:
            parts = wgrad(group, whose)
            for unit, part in parts.items():
                arrived[unit] = exchange(part)
            whose = lax.optimization_barrier((other, part_of(parts)))[0]
        gbar, squares = {}, jnp.zeros((8, 128), F32)
        own_part = {}
        for kind in (0, 1):
            own_part.update(wgrad((kind, 0, PIECES), mine))
        for unit in units:
            gbar[unit], squares = combine(1.0 / n_rep, own_part[unit], arrived[unit], squares)
        clip = clip_factor(n_stages, n_rep, squares, jnp.reshape(max_norm, (1,)))
        knobs = (jnp.reshape(learn_rate, (1,)), clip)
        gbar_other = {}
        for unit in F32_FIRST:
            half = gbar[unit].shape[0] // 2
            top = exchange(gbar[unit][:half])
            low = exchange(lax.optimization_barrier((gbar[unit][half:], clip))[0])
            gbar_other[unit] = jnp.concatenate([top, low], axis=0)
        state = ((master_up, mom1_up, mom2_up), (master_down, mom1_down, mom2_down))
        chain = [(), ()]

        def update(unit, owner, grad):
            res = update_units(unit[0], unit[1], owner, knobs, state[unit[0]], [grad], chain[unit[0]], True)
            chain[unit[0]] = res[:3]
            return res[3]

        def update_group(kind, first, stop, clip):
            grads = [gbar_other[kind, k] for k in range(first, stop)]
            res = update_units(kind, first, other, (knobs[0], clip), state[kind], grads, chain[kind], False)
            chain[kind] = res[:3]
            return res[3]

        late = [unit for unit in units if unit not in F32_FIRST]
        own_w, other_w = {}, {}
        for unit in late + list(F32_FIRST):
            own_w[unit] = update(unit, mine, gbar[unit])
            if unit in late:
                other_w[unit] = exchange(own_w[unit])
        for unit in late:
            ready = lax.optimization_barrier((gbar[unit], own_w[late[-1]]))[0]
            gbar_other[unit] = exchange(ready)
        for unit in F32_FIRST:
            other_w[unit] = update(unit, other, gbar_other[unit])
        weights = []
        for side in (own_w, other_w):
            for kind in (0, 1):
                weights += [side[kind, k] for k in range(PIECES)]
        stage_outs = store(forward(n_stages, n_rep, next_batch, weights)).reshape((1,) + next_batch.shape)
        for kind, first, stop in TAIL:
            clip = update_group(kind, first, stop, clip)
        (new_up, new_m1_up, new_m2_up), (new_down, new_m1_down, new_m2_down) = chain
        return (new_up, new_down, new_m1_up, new_m1_down, new_m2_up, new_m2_down, stage_outs)

    w_spec = P("stage", None, None)
    g_spec = P("data", "stage", None, None)
    in_specs = (w_spec,) * 6 + (g_spec, g_spec, P("stage", "data", None), P("data", None), P(None, "data", None), P(), P())
    out_specs = (w_spec,) * 6 + (P("stage", None, "data", None),)
    return jax.shard_map(local_step, mesh=mesh, in_specs=in_specs, out_specs=out_specs, check_vma=False)
```

```python
import functools

import jax
import jax.numpy as jnp
from jax import lax
from jax.experimental import pallas as pl
from jax.experimental.pallas import tpu as pltpu
from jax.sharding import PartitionSpec as P


BETA1 = 0.9
BETA2 = 0.95
ADAM_EPS = 1e-8
WEIGHT_DECAY = 0.1
NORM_EPS = 1e-6
ADAM_STEP = 8
SQRT_TWO_PI = 0.7978845608028654
GELU_CUBIC = 0.044715

BACK_ROWS = 256
FWD_ROWS = 256
HEAD = 128
BACK_TILE = 512
FWD_TILE = 512
PIECES = 6
F32_FIRST = ((0, 0),)
GROUPS = ((0, 0, 1), (1, 0, 2), (0, 1, 2), (1, 2, 2), (0, 3, 2), (1, 4, 2), (0, 5, 1))
TAIL = ((0, 1, 5), (1, 0, 6), (0, 5, 6))
STAGING = 3
WGRAD_STEP = 2048
SLAB = 32

BF16 = jnp.bfloat16
F32 = jnp.float32
MESH_ID = pl.DeviceIdType.MESH
ANY = pl.BlockSpec(memory_space=pl.ANY)
VMEM_LIMIT = 60 * 1024 * 1024
FWD_VMEM = 54000000
STORE_VMEM = 4 * 1024 * 1024
UPDATE_VMEM = 60 * 1024 * 1024


def dot_nn(left, right):
    return lax.dot_general(left, right, (((1,), (0,)), ((), ())), preferred_element_type=F32)


def dot_nt(left, right):
    return lax.dot_general(left, right, (((1,), (1,)), ((), ())), preferred_element_type=F32)


def dot_tn(left, right):
    return lax.dot_general(left, right, (((0,), (0,)), ((), ())), preferred_element_type=F32)


def span(index, size):
    if isinstance(index, int):
        return pl.ds(index * size, size)
    return pl.ds(pl.multiple_of(index * size, size), size)


def chunk_rows(c, total, size):
    if isinstance(c, int):
        return pl.ds(0 if c == 0 else total - HEAD, HEAD)
    return pl.ds(pl.multiple_of(HEAD + (c - 1) * size, HEAD), size)


def tanh_part(x, sq):
    return jnp.tanh(x * (SQRT_TWO_PI + (SQRT_TWO_PI * GELU_CUBIC) * sq))


def gelu_value(x):
    return x * (0.5 + 0.5 * tanh_part(x, x * x))


def gelu_pair(x):
    sq = x * x
    th = tanh_part(x, sq)
    half = 0.5 + 0.5 * th
    value = x * half
    slope = half + value * (1.0 - th) * (SQRT_TWO_PI + (3.0 * SQRT_TWO_PI * GELU_CUBIC) * sq)
    return value, slope


def meet_neighbours(stage, n_stages):
    barrier = pltpu.get_barrier_semaphore()

    @pl.when(stage > 0)
    def _():
        pl.semaphore_signal(barrier, inc=1, device_id={"stage": stage - 1}, device_id_type=MESH_ID)

    @pl.when(stage < n_stages - 1)
    def _():
        pl.semaphore_signal(barrier, inc=1, device_id={"stage": stage + 1}, device_id_type=MESH_ID)

    pl.semaphore_wait(barrier, jnp.minimum(stage, 1) + jnp.minimum(n_stages - 1 - stage, 1))


def back_kernel(n_stages, acts_ref, dy_ref, up32_ref, down32_ref, hid_ref, dpre_ref, gown_ref,
                up_ref, down_ref, a_buf, g_buf, h_buf, p_buf, dx_buf, acc_ref, pre_buf, dh_buf, stage_u, stage_v,
                u_sem, v_sem, a_sem, recv_sem, send_sem, gown_sem, h_sem, p_sem):
    stage = lax.axis_index("stage")
    last = n_stages - 1
    rows_all = g_buf.shape[0]
    hidden = up_ref.shape[1]
    n_chunks = rows_all // BACK_ROWS
    n_tiles = hidden // BACK_TILE

    def tile_copies(j):
        slot, cols = j % STAGING, pl.ds(j * BACK_TILE, BACK_TILE)
        return (pltpu.make_async_copy(up32_ref.at[0, :, cols], stage_u.at[slot], u_sem.at[slot]),
                pltpu.make_async_copy(down32_ref.at[0, cols, :], stage_v.at[slot], v_sem.at[slot]))

    def rows_of(c):
        return pl.ds(c * BACK_ROWS, BACK_ROWS) if isinstance(c, int) else span(c, BACK_ROWS)

    def a_copy(c):
        return pltpu.make_async_copy(acts_ref.at[0, rows_of(c), :], a_buf.at[rows_of(c), :], a_sem.at[c])

    def dy_copy(c):
        return pltpu.make_async_copy(dy_ref.at[rows_of(c), :], g_buf.at[rows_of(c), :], recv_sem.at[c])

    a_copy(0).start()

    @pl.when(stage == last)
    def _():
        dy_copy(0).start()

    for j in range(STAGING):
        for copy in tile_copies(j):
            copy.start()

    def load_rest(c, carry):
        a_copy(c).start()

        @pl.when(stage == last)
        def _():
            dy_copy(c).start()

        return carry

    def cast_tile(j):
        cols = pl.ds(j * BACK_TILE, BACK_TILE)
        for copy in tile_copies(j):
            copy.wait()
        up_ref[:, cols] = stage_u[j % STAGING].astype(BF16)
        down_ref[cols, :] = stage_v[j % STAGING].astype(BF16)
        if j + STAGING < n_tiles:
            for copy in tile_copies(j + STAGING):
                copy.start()
        if j == n_tiles - STAGING:
            lax.fori_loop(1, n_chunks, load_rest, 0)

    meet_neighbours(stage, n_stages)

    def send_of(c):
        return pltpu.make_async_remote_copy(
            src_ref=dx_buf.at[rows_of(c), :], dst_ref=g_buf.at[rows_of(c), :],
            send_sem=send_sem.at[c], recv_sem=recv_sem.at[c],
            device_id={"stage": stage - 1}, device_id_type=MESH_ID)

    def out_copies(c, slot):
        return (pltpu.make_async_copy(h_buf.at[slot], hid_ref.at[rows_of(c), :], h_sem.at[slot]),
                pltpu.make_async_copy(p_buf.at[slot], dpre_ref.at[rows_of(c), :], p_sem.at[slot]))

    def gown_copy(c):
        return pltpu.make_async_copy(g_buf.at[rows_of(c), :], gown_ref.at[rows_of(c), :], gown_sem.at[c])

    def chunk(c, carry, casting=False):
        slot = c % 2 if casting else lax.rem(c, 2)
        rows = rows_of(c)
        if not casting:
            @pl.when(c >= 2)
            def _():
                for copy in out_copies(c - 2, slot):
                    copy.wait()

        a_copy(c).wait()
        dy_copy(c).wait()
        gown_copy(c).start()

        def products(j):
            if casting:
                cast_tile(j)
            cols = pl.ds(j * BACK_TILE, BACK_TILE)
            pre_buf[j % 2] = dot_nn(a_buf[rows, :], up_ref[:, cols])
            dh_buf[j % 2] = dot_nt(g_buf[rows, :], down_ref[cols, :])

        def rest(j):
            cols = pl.ds(j * BACK_TILE, BACK_TILE)
            value, slope = gelu_pair(pre_buf[j % 2])
            h_buf[slot, :, cols] = value.astype(BF16)
            d_pre = (dh_buf[j % 2] * slope).astype(BF16)
            p_buf[slot, :, cols] = d_pre
            part = dot_nt(d_pre, up_ref[:, cols])
            if j == 0:
                acc_ref[...] = g_buf[rows, :].astype(F32) + part
            elif j < n_tiles - 1:
                acc_ref[...] += part
            else:
                dx_buf[rows, :] = (acc_ref[...] + part).astype(BF16)

        products(0)
        for j in range(n_tiles):
            if j + 1 < n_tiles:
                products(j + 1)
            rest(j)
        for copy in out_copies(c, slot):
            copy.start()

        @pl.when(stage > 0)
        def _():
            send_of(c).start()

        return carry

    @pl.when(stage == last)
    def _():
        chunk(0, 0, casting=True)

    @pl.when(stage < last)
    def _():
        for j in range(n_tiles):
            cast_tile(j)

    lax.fori_loop(stage // last, n_chunks, chunk, 0)

    for c in (n_chunks - 2, n_chunks - 1):
        for copy in out_copies(c, c % 2):
            copy.wait()

    def finish(c, carry):
        gown_copy(c).wait()

        @pl.when(stage > 0)
        def _():
            send_of(c).wait_send()

        return carry

    lax.fori_loop(0, n_chunks, finish, 0)


def backward(n_stages, acts, loss_grad, up32, down32):
    _, rows, width = acts.shape
    hidden = up32.shape[2]
    n_chunks = rows // BACK_ROWS
    wide = jax.ShapeDtypeStruct((rows, hidden), BF16)
    return pl.pallas_call(
        functools.partial(back_kernel, n_stages),
        name="backward",
        out_shape=(wide, wide, jax.ShapeDtypeStruct((rows, width), BF16)),
        in_specs=[ANY] * 4,
        out_specs=(ANY, ANY, ANY),
        scratch_shapes=[
            pltpu.VMEM((width, hidden), BF16),
            pltpu.VMEM((hidden, width), BF16),
            pltpu.VMEM((rows, width), BF16),
            pltpu.VMEM((rows, width), BF16),
            pltpu.VMEM((2, BACK_ROWS, hidden), BF16),
            pltpu.VMEM((2, BACK_ROWS, hidden), BF16),
            pltpu.VMEM((rows, width), BF16),
            pltpu.VMEM((BACK_ROWS, width), F32),
            pltpu.VMEM((2, BACK_ROWS, BACK_TILE), F32),
            pltpu.VMEM((2, BACK_ROWS, BACK_TILE), F32),
            pltpu.VMEM((STAGING, width, BACK_TILE), F32),
            pltpu.VMEM((STAGING, BACK_TILE, width), F32),
            pltpu.SemaphoreType.DMA((STAGING,)),
            pltpu.SemaphoreType.DMA((STAGING,)),
            pltpu.SemaphoreType.DMA((n_chunks,)),
            pltpu.SemaphoreType.DMA((n_chunks,)),
            pltpu.SemaphoreType.DMA((n_chunks,)),
            pltpu.SemaphoreType.DMA((n_chunks,)),
            pltpu.SemaphoreType.DMA((2,)),
            pltpu.SemaphoreType.DMA((2,)),
        ],
        compiler_params=pltpu.CompilerParams(collective_id=0, has_side_effects=True, vmem_limit_bytes=VMEM_LIMIT),
        cost_estimate=pl.CostEstimate(flops=6 * rows * width * hidden, bytes_accessed=6 * rows * hidden, transcendentals=rows * hidden),
    )(acts, loss_grad, up32, down32)


def wgrad_kernel(owner_ref, left_ref, right_ref, grad_ref, *refs):
    sum_refs, acc_ref = refs[:-1], refs[-1]
    lead = (0,) * (len(left_ref.shape) - 2)
    acc_ref[...] = grad_ref[0, 0]

    def step(k, carry):
        part = span(k, WGRAD_STEP)
        acc_ref[...] += dot_tn(left_ref[lead + (part, slice(None))], right_ref[part, :])
        return carry

    lax.fori_loop(0, right_ref.shape[0] // WGRAD_STEP, step, 0)
    for p, sum_ref in enumerate(sum_refs):
        def put(ref=sum_ref):
            ref[...] = acc_ref[...]

        if len(sum_refs) == 1:
            put()
        else:
            pl.when(pl.program_id(0) == p)(put)


def wgrad_units(kind, first, count, owner, left, right, grad):
    rows = right.shape[0]
    if kind == 0:
        half, piece = left.shape[2] // 2, right.shape[1] // PIECES
        shape = (half, piece)
        in_specs = [
            pl.BlockSpec((1, rows, half), lambda i, own: (0, 0, own[0])),
            pl.BlockSpec((rows, piece), lambda i, own: (0, first + i)),
            pl.BlockSpec((1, 1, half, piece), lambda i, own: (0, 0, own[0], first + i)),
        ]
    else:
        width, piece = right.shape[1], left.shape[1] // 2 // PIECES
        shape = (piece, width)
        in_specs = [
            pl.BlockSpec((rows, piece), lambda i, own: (0, own[0] * PIECES + first + i)),
            pl.BlockSpec((rows, width), lambda i, own: (0, 0)),
            pl.BlockSpec((1, 1, piece, width), lambda i, own: (0, 0, own[0] * PIECES + first + i, 0)),
        ]
    return pl.pallas_call(
        wgrad_kernel,
        out_shape=(jax.ShapeDtypeStruct(shape, F32),) * count,
        grid_spec=pltpu.PrefetchScalarGridSpec(
            num_scalar_prefetch=1,
            grid=(count,),
            in_specs=in_specs,
            out_specs=(pl.BlockSpec(shape, lambda i, own: (0, 0)),) * count,
            scratch_shapes=[pltpu.VMEM(shape, F32)],
        ),
        compiler_params=pltpu.CompilerParams(vmem_limit_bytes=VMEM_LIMIT),
        cost_estimate=pl.CostEstimate(flops=2 * rows * shape[0] * shape[1] * count, bytes_accessed=15 * 1024 * 1024, transcendentals=0),
    )(owner, left, right, grad)


def combine_kernel(scale, mine_ref, theirs_ref, sq_ref, gbar_ref, sq_out):
    n_rows, cols = mine_ref.shape

    def slab(i, fold):
        rows = span(i, SLAB)
        mean = (mine_ref[rows, :] + theirs_ref[rows, :]) * scale
        gbar_ref[rows, :] = mean
        part = jnp.sum((mean * mean).reshape(SLAB // 8, 8, cols), axis=0)
        for j in range(cols // 128):
            fold = fold + part[:, j * 128:(j + 1) * 128]
        return fold

    fold = lax.fori_loop(0, n_rows // SLAB, slab, jnp.zeros((8, 128), F32))
    first = pl.program_id(0) == 0

    @pl.when(first)
    def _():
        sq_out[...] = sq_ref[...] + fold

    @pl.when(jnp.logical_not(first))
    def _():
        sq_out[...] += fold


def combine(scale, mine, theirs, squares):
    rows, cols = mine.shape
    steps = 2
    spec = pl.BlockSpec((rows // steps, cols), lambda i: (i, 0))
    small = pl.BlockSpec((8, 128), lambda i: (0, 0))
    return pl.pallas_call(
        functools.partial(combine_kernel, scale),
        name="combine",
        out_shape=(jax.ShapeDtypeStruct((rows, cols), F32), jax.ShapeDtypeStruct((8, 128), F32)),
        grid=(steps,),
        in_specs=[spec, spec, small],
        out_specs=(spec, small),
        compiler_params=pltpu.CompilerParams(vmem_limit_bytes=VMEM_LIMIT),
        cost_estimate=pl.CostEstimate(flops=4 * rows * cols, bytes_accessed=12 * rows * cols, transcendentals=0),
    )(mine, theirs, squares)


def update_kernel(n_pieces, n_alias, want_bf16, owner_ref, lr_ref, clip_ref, w_ref, m_ref, v_ref, *rest):
    g_refs = rest[:n_pieces]
    w_out, m_out, v_out, last_out = rest[n_pieces + n_alias:]
    clip, lr = clip_ref[0:1, 0:1], lr_ref[0]

    def run(g_ref, b_out):
        def slab(i, carry):
            rows = span(i, SLAB)
            w = w_ref[0, rows, :]
            q = clip * g_ref[rows, :]
            m_new = BETA1 * m_ref[0, rows, :] + (1.0 - BETA1) * q
            v_new = BETA2 * v_ref[0, rows, :] + (1.0 - BETA2) * q * q
            m_hat = m_new * (1.0 / (1.0 - BETA1 ** ADAM_STEP))
            v_hat = v_new * (1.0 / (1.0 - BETA2 ** ADAM_STEP))
            w_new = w - lr * (m_hat / (jnp.sqrt(v_hat) + ADAM_EPS) + WEIGHT_DECAY * w)
            w_out[0, rows, :], m_out[0, rows, :], v_out[0, rows, :] = w_new, m_new, v_new
            if b_out is not None:
                b_out[rows, :] = w_new.astype(BF16)
            return carry

        lax.fori_loop(0, g_ref.shape[0] // SLAB, slab, 0)

    if n_pieces == 1:
        run(g_refs[0], last_out if want_bf16 else None)
    else:
        for p in range(n_pieces):
            pl.when(pl.program_id(0) == p)(functools.partial(run, g_refs[p], None))
    if not want_bf16:
        last_out[...] = clip_ref[...]


def update_units(kind, first, owner, knobs, state, grads, chain, want_bf16):
    rows, cols = grads[0].shape
    n = len(grads)
    steps = 2 if n == 1 else 1
    block = rows // steps
    if kind == 0:
        spec = pl.BlockSpec((1, block, cols), lambda p, i, own: (0, own[0] * steps + i, first + p))
    else:
        spec = pl.BlockSpec((1, block, cols), lambda p, i, own: (0, (own[0] * PIECES + first + p) * steps + i, 0))

    def piece_spec(q):
        return pl.BlockSpec((block, cols), lambda p, i, own: (jnp.clip((p - q) * steps + i, 0, steps - 1), 0))

    full = jax.ShapeDtypeStruct(state[0].shape, F32)
    out_shape, out_specs = (full,) * 3, (spec,) * 3
    if want_bf16:
        out_shape += (jax.ShapeDtypeStruct((rows, cols), BF16),)
        out_specs += (piece_spec(0),)
    else:
        out_shape += (jax.ShapeDtypeStruct((8, 128), F32),)
        out_specs += (pl.BlockSpec((8, 128), lambda p, i, own: (0, 0)),)
    size = n * rows * cols
    return pl.pallas_call(
        functools.partial(update_kernel, n, len(chain), want_bf16),
        out_shape=out_shape,
        grid_spec=pltpu.PrefetchScalarGridSpec(
            num_scalar_prefetch=1,
            grid=(n, steps),
            in_specs=[pl.BlockSpec(memory_space=pltpu.SMEM), pl.BlockSpec(memory_space=pltpu.VMEM)] + [spec] * 3 + [piece_spec(q) for q in range(n)] + [ANY] * len(chain),
            out_specs=out_specs,
        ),
        input_output_aliases={6 + n + i: i for i in range(len(chain))},
        compiler_params=pltpu.CompilerParams(vmem_limit_bytes=UPDATE_VMEM),
        cost_estimate=pl.CostEstimate(flops=30 * size, bytes_accessed=28 * size, transcendentals=size),
    )(owner, *knobs, *state, *grads, *chain)


def norm_kernel(n_stages, n_rep, sq_ref, max_ref, clip_ref, slots, send_sem, recv_sem):
    n_dev = n_stages * n_rep
    me = lax.axis_index("data") * n_stages + lax.axis_index("stage")
    slots[me] = sq_ref[...]

    def place(d):
        q = lax.rem(me + d, n_dev)
        return {"data": q // n_stages, "stage": lax.rem(q, n_stages)}

    barrier = pltpu.get_barrier_semaphore()
    for d in range(1, n_dev):
        pl.semaphore_signal(barrier, inc=1, device_id=place(d), device_id_type=MESH_ID)
    pl.semaphore_wait(barrier, n_dev - 1)
    copies = []
    for d in range(1, n_dev):
        copies.append(pltpu.make_async_remote_copy(
            src_ref=sq_ref, dst_ref=slots.at[me], send_sem=send_sem.at[d - 1], recv_sem=recv_sem.at[d - 1],
            device_id=place(d), device_id_type=MESH_ID))
        copies[-1].start()
    for copy in copies:
        copy.wait()
    square = slots[0]
    for q in range(1, n_dev):
        square = square + slots[q]
    total = jnp.full(clip_ref.shape, jnp.sum(square), F32)
    clip_ref[...] = jnp.minimum(1.0, max_ref[0] / (jnp.sqrt(total) + NORM_EPS))


def clip_factor(n_stages, n_rep, squares, max_norm):
    n_dev = n_stages * n_rep
    return pl.pallas_call(
        functools.partial(norm_kernel, n_stages, n_rep),
        name="clip_factor",
        out_shape=jax.ShapeDtypeStruct((8, 128), F32),
        in_specs=[pl.BlockSpec(memory_space=pltpu.VMEM), pl.BlockSpec(memory_space=pltpu.SMEM)],
        out_specs=pl.BlockSpec(memory_space=pltpu.VMEM),
        scratch_shapes=[
            pltpu.VMEM((n_dev, 8, 128), F32),
            pltpu.SemaphoreType.DMA((n_dev - 1,)),
            pltpu.SemaphoreType.DMA((n_dev - 1,)),
        ],
        compiler_params=pltpu.CompilerParams(collective_id=2, has_side_effects=True),
        cost_estimate=pl.CostEstimate(flops=40000000, bytes_accessed=4096, transcendentals=0),
    )(squares, max_norm)


def fwd_kernel(n_stages, n_rep, batch_ref, *refs):
    n_w = 2 * PIECES * n_rep
    w_refs = refs[:n_w]
    out_ref, up_ref, down_ref, x_buf, acc_ref, pre_buf, w_sem, recv_sem, send_sem = refs[n_w:]
    stage = lax.axis_index("stage")
    me = lax.axis_index("data")
    last = n_stages - 1
    total = x_buf.shape[0]
    hidden = up_ref.shape[1]
    n_tiles = hidden // FWD_TILE
    n_chunks = (total - 2 * HEAD) // FWD_ROWS + 2
    final = n_chunks - 1

    def rows_of(c):
        return chunk_rows(c, total, FWD_ROWS)

    def batch_copy(c):
        return pltpu.make_async_copy(batch_ref.at[rows_of(c), :], x_buf.at[rows_of(c), :], recv_sem.at[c])

    copies = []
    for side in range(n_rep):
        owner = me if side == 0 else 1 - me
        for k in range(PIECES):
            u_src = w_refs[(2 * side) * PIECES + k]
            v_src = w_refs[(2 * side + 1) * PIECES + k]
            half_w, piece_n = u_src.shape
            piece_m = v_src.shape[0]
            u_dst = up_ref.at[span(owner, half_w), pl.ds(k * piece_n, piece_n)]
            v_dst = down_ref.at[span(owner * PIECES + k, piece_m), :]
            copies.append(pltpu.make_async_copy(u_src, u_dst, w_sem.at[len(copies)]))
            copies.append(pltpu.make_async_copy(v_src, v_dst, w_sem.at[len(copies)]))
    for copy in copies:
        copy.start()

    @pl.when(stage == 0)
    def _():
        def load(c, carry):
            batch_copy(c).start()
            return carry

        load(0, 0)
        lax.fori_loop(1, final, load, 0)
        load(final, 0)

    meet_neighbours(stage, n_stages)
    for copy in copies:
        copy.wait()

    def send_of(c):
        return pltpu.make_async_remote_copy(
            src_ref=out_ref.at[rows_of(c), :], dst_ref=x_buf.at[rows_of(c), :],
            send_sem=send_sem.at[c], recv_sem=recv_sem.at[c],
            device_id={"stage": stage + 1}, device_id_type=MESH_ID)

    def chunk(c, carry):
        rows = rows_of(c)
        size = pl.ds(0, HEAD if isinstance(c, int) else FWD_ROWS)
        batch_copy(c).wait()

        def products(j):
            pre_buf[j % 2, size, :] = dot_nn(x_buf[rows, :], up_ref[:, pl.ds(j * FWD_TILE, FWD_TILE)])

        def rest(j):
            hid = gelu_value(pre_buf[j % 2, size, :]).astype(BF16)
            part = dot_nn(hid, down_ref[pl.ds(j * FWD_TILE, FWD_TILE), :])
            if j == 0:
                acc_ref[size, :] = x_buf[rows, :].astype(F32) + part
            elif j < n_tiles - 1:
                acc_ref[size, :] += part
            else:
                out_ref[rows, :] = (acc_ref[size, :] + part).astype(BF16)

        products(0)
        for j in range(n_tiles):
            if j + 1 < n_tiles:
                products(j + 1)
            rest(j)

        @pl.when(stage < last)
        def _():
            send_of(c).start()

        return carry

    chunk(0, 0)
    lax.fori_loop(1, final, chunk, 0)
    chunk(final, 0)

    @pl.when(stage < last)
    def _():
        def finish(c, carry):
            send_of(c).wait_send()
            return carry

        finish(0, 0)
        lax.fori_loop(1, final, finish, 0)
        finish(final, 0)


def forward(n_stages, n_rep, next_batch, weights):
    n_micro, rows, width = next_batch.shape
    total = n_micro * rows
    hidden = PIECES * weights[0].shape[1]
    n_chunks = (total - 2 * HEAD) // FWD_ROWS + 2
    return pl.pallas_call(
        functools.partial(fwd_kernel, n_stages, n_rep),
        name="forward",
        out_shape=pltpu.VMEM((total, width), BF16),
        in_specs=[ANY] * (1 + len(weights)),
        out_specs=pl.BlockSpec(memory_space=pltpu.VMEM),
        scratch_shapes=[
            pltpu.VMEM((width, hidden), BF16),
            pltpu.VMEM((hidden, width), BF16),
            pltpu.VMEM((total, width), BF16),
            pltpu.VMEM((FWD_ROWS, width), F32),
            pltpu.VMEM((2, FWD_ROWS, FWD_TILE), F32),
            pltpu.SemaphoreType.DMA((len(weights),)),
            pltpu.SemaphoreType.DMA((n_chunks,)),
            pltpu.SemaphoreType.DMA((n_chunks,)),
        ],
        compiler_params=pltpu.CompilerParams(collective_id=1, has_side_effects=True, vmem_limit_bytes=FWD_VMEM),
        cost_estimate=pl.CostEstimate(flops=4 * n_micro * rows * width * hidden, bytes_accessed=6 * rows * hidden, transcendentals=n_micro * rows * hidden),
    )(next_batch.reshape(total, width), *weights)


def store_kernel(y_ref, out_ref, sem):
    half = y_ref.shape[0] // 2
    copies = [pltpu.make_async_copy(y_ref.at[span(i, half), :], out_ref.at[span(i, half), :], sem.at[i]) for i in range(2)]
    for copy in copies:
        copy.start()
    for copy in copies:
        copy.wait()


def store(y):
    return pl.pallas_call(
        store_kernel,
        name="store",
        out_shape=jax.ShapeDtypeStruct(y.shape, y.dtype),
        in_specs=[pl.BlockSpec(memory_space=pltpu.VMEM)],
        out_specs=ANY,
        scratch_shapes=[pltpu.SemaphoreType.DMA((2,))],
        compiler_params=pltpu.CompilerParams(vmem_limit_bytes=STORE_VMEM),
        cost_estimate=pl.CostEstimate(flops=4000000, bytes_accessed=2 * y.size, transcendentals=0),
    )(y)


def part_of(parts):
    return next(iter(parts.values()))


def solution(mesh):
    n_stages = mesh.shape["stage"]
    n_rep = mesh.shape["data"]
    swap = [(i, n_rep - 1 - i) for i in range(n_rep)]

    def exchange(x):
        return lax.ppermute(x, "data", swap)

    def local_step(master_up, master_down, mom1_up, mom1_down, mom2_up, mom2_down, grad_up, grad_down, stage_acts, loss_grad, next_batch, learn_rate, max_norm):
        me = lax.axis_index("data")
        mine = jnp.reshape(me, (1,)).astype(jnp.int32)
        other = 1 - mine
        hid, d_pre, g_own = backward(n_stages, stage_acts, loss_grad, master_up, master_down)

        units = [(kind, first + i) for kind, first, count in GROUPS for i in range(count)]

        def wgrad(group, owner):
            kind, first, count = group
            operands = (stage_acts, d_pre, grad_up) if kind == 0 else (hid, g_own, grad_down)
            parts = wgrad_units(kind, first, count, owner, *operands)
            return {(kind, first + i): parts[i] for i in range(count)}

        arrived, whose = {}, other
        for group in GROUPS:
            parts = wgrad(group, whose)
            for unit, part in parts.items():
                arrived[unit] = exchange(part)
            whose = lax.optimization_barrier((other, part_of(parts)))[0]
        gbar, squares = {}, jnp.zeros((8, 128), F32)
        own_part = {}
        for kind in (0, 1):
            own_part.update(wgrad((kind, 0, PIECES), mine))
        for unit in units:
            gbar[unit], squares = combine(1.0 / n_rep, own_part[unit], arrived[unit], squares)
        clip = clip_factor(n_stages, n_rep, squares, jnp.reshape(max_norm, (1,)))
        knobs = (jnp.reshape(learn_rate, (1,)), clip)
        gbar_other = {}
        for unit in F32_FIRST:
            half = gbar[unit].shape[0] // 2
            top = exchange(gbar[unit][:half])
            low = exchange(lax.optimization_barrier((gbar[unit][half:], clip))[0])
            gbar_other[unit] = jnp.concatenate([top, low], axis=0)
        state = ((master_up, mom1_up, mom2_up), (master_down, mom1_down, mom2_down))
        chain = [(), ()]

        def update(unit, owner, grad):
            res = update_units(unit[0], unit[1], owner, knobs, state[unit[0]], [grad], chain[unit[0]], True)
            chain[unit[0]] = res[:3]
            return res[3]

        def update_group(kind, first, stop, clip):
            grads = [gbar_other[kind, k] for k in range(first, stop)]
            res = update_units(kind, first, other, (knobs[0], clip), state[kind], grads, chain[kind], False)
            chain[kind] = res[:3]
            return res[3]

        late = [unit for unit in units if unit not in F32_FIRST]
        own_w, other_w = {}, {}
        for unit in late + list(F32_FIRST):
            own_w[unit] = update(unit, mine, gbar[unit])
            if unit in late:
                other_w[unit] = exchange(own_w[unit])
        for unit in late:
            ready = lax.optimization_barrier((gbar[unit], own_w[late[-1]]))[0]
            gbar_other[unit] = exchange(ready)
        for unit in F32_FIRST:
            other_w[unit] = update(unit, other, gbar_other[unit])
        weights = []
        for side in (own_w, other_w):
            for kind in (0, 1):
                weights += [side[kind, k] for k in range(PIECES)]
        stage_outs = store(forward(n_stages, n_rep, next_batch, weights)).reshape((1,) + next_batch.shape)
        for kind, first, stop in TAIL:
            clip = update_group(kind, first, stop, clip)
        (new_up, new_m1_up, new_m2_up), (new_down, new_m1_down, new_m2_down) = chain
        return (new_up, new_down, new_m1_up, new_m1_down, new_m2_up, new_m2_down, stage_outs)

    w_spec = P("stage", None, None)
    g_spec = P("data", "stage", None, None)
    in_specs = (w_spec,) * 6 + (g_spec, g_spec, P("stage", "data", None), P("data", None), P(None, "data", None), P(), P())
    out_specs = (w_spec,) * 6 + (P("stage", None, "data", None),)
    return jax.shard_map(local_step, mesh=mesh, in_specs=in_specs, out_specs=out_specs, check_vma=False)
```
